8 devices in a mesh: dp: 1 (over z), tp: 8 (over y, x, core).
Axes of the slice: x: 2, y: 2, z: 1, core: 2. Of those that a mesh axis runs over, the one named last changes fastest.
Arguments:
- x_in: float32 [16, 128, 3072], P('dp', 'tp')
- d_out: bfloat16 [16, 128, 3072], P('dp', 'tp')
- lengths: int32 [16], P('dp')
- w_qkv: bfloat16 [3, 3072, 3, 32, 96], P(None, None, None, 'tp')
- w_out: bfloat16 [3, 32, 96, 3072], P(None, 'tp')
- w_up: bfloat16 [3, 3072, 12288], P(None, None, 'tp')
- b_up: float32 [3, 12288], P(None, 'tp')
- w_down: bfloat16 [3, 12288, 3072], P(None, 'tp')
- vec_par: float32 [3, 6, 3072], replicated
Outputs:
- output 1: float32 [16, 128, 3072], P('dp', 'tp')
- output 2: float32 [16, 128, 3072], P('dp', 'tp')
- output 3: bfloat16 [3, 3072, 3, 32, 96], P('dp', None, None, 'tp')
- output 4: bfloat16 [3, 32, 96, 3072], P('dp', 'tp')
- output 5: bfloat16 [3, 3072, 12288], P('dp', None, 'tp')
- output 6: float32 [3, 12288], P('dp', 'tp')
- output 7: bfloat16 [3, 12288, 3072], P('dp', 'tp')
- output 8: float32 [3, 6, 3072], P('dp')
All inputs are finite; a program needn't handle non-finite values.
Results may differ from the reference program's by a relative error of at most 0.02.
Values are sent between devices in bfloat16 or wider.
A program may use at most 1 GiB of HBM per device.

```python
import functools
import jax
import jax.numpy as jnp
from jax import lax

BATCH_GROUP = 16
SEQ_LEN = 128
D_MODEL = 3072
NUM_HEADS = 32
HEAD_DIM = 96
FF_DIM = 12288
LAYERS = 3


def draw_lengths(key_len, key_perm):
    lengths = jax.random.randint(key_len, (BATCH_GROUP,), SEQ_LEN // 4, SEQ_LEN + 1, jnp.int32)
    perm_order = jax.random.permutation(key_perm, BATCH_GROUP)
    return lengths.at[perm_order[0]].set(SEQ_LEN).at[perm_order[1]].set(SEQ_LEN // 4)


def setup_inputs(seed: int = 0, part: int = 0) -> dict:
    shared_key = jax.random.key(seed)
    part_key = jax.random.fold_in(jax.random.key(seed + 1), part)
    key_qkv, key_out, key_up, key_bup, key_down, key_vec = jax.random.split(shared_key, 6)
    key_x, key_dy, key_len, key_perm = jax.random.split(part_key, 4)
    inner_dim = NUM_HEADS * HEAD_DIM
    w_qkv = (jax.random.normal(key_qkv, (LAYERS, D_MODEL, 3, NUM_HEADS, HEAD_DIM), jnp.float32) * (1.2 * D_MODEL ** -0.5)).astype(jnp.bfloat16)
    w_out = (jax.random.normal(key_out, (LAYERS, NUM_HEADS, HEAD_DIM, D_MODEL), jnp.float32) * (2.0 * inner_dim ** -0.5)).astype(jnp.bfloat16)
    w_up = (jax.random.normal(key_up, (LAYERS, D_MODEL, FF_DIM), jnp.float32) * D_MODEL ** -0.5).astype(jnp.bfloat16)
    b_up = jax.random.normal(key_bup, (LAYERS, FF_DIM), jnp.float32) * 0.5
    w_down = (jax.random.normal(key_down, (LAYERS, FF_DIM, D_MODEL), jnp.float32) * (2.0 * FF_DIM ** -0.5)).astype(jnp.bfloat16)
    row_scale = jnp.array([0.25, 0.5, 0.25, 0.5, 0.5, 0.5], jnp.float32)[None, :, None]
    row_base = jnp.array([1.0, 0.0, 1.0, 0.0, 0.0, 0.0], jnp.float32)[None, :, None]
    vec_par = jax.random.normal(key_vec, (LAYERS, 6, D_MODEL), jnp.float32) * row_scale + row_base
    x_in = jax.random.normal(key_x, (BATCH_GROUP, SEQ_LEN, D_MODEL), jnp.float32)
    d_out = jax.random.normal(key_dy, (BATCH_GROUP, SEQ_LEN, D_MODEL), jnp.float32).astype(jnp.bfloat16)
    lengths = draw_lengths(key_len, key_perm)
    return {'x_in': x_in, 'd_out': d_out, 'lengths': lengths, 'w_qkv': w_qkv, 'w_out': w_out, 'w_up': w_up, 'b_up': b_up, 'w_down': w_down, 'vec_par': vec_par}


def layer_norm(x_val, gain_vec, shift_vec):
    row_mean = jnp.mean(x_val, axis=-1, keepdims=True)
    centered = x_val - row_mean
    row_var = jnp.mean(centered * centered, axis=-1, keepdims=True)
    return centered * lax.rsqrt(row_var + 1e-5) * gain_vec + shift_vec


def attend_one(item_tuple):
    q_one, k_one, v_one, length = item_tuple
    scores = jnp.einsum('hqe,hke->hqk', q_one.astype(jnp.float32), k_one.astype(jnp.float32)) * HEAD_DIM ** -0.5
    positions = jnp.arange(SEQ_LEN)
    allowed = (positions[None, :] <= positions[:, None]) & (positions[None, :] < length)
    scores = jnp.where(allowed[None], scores, -1e30)
    attn_prob = jax.nn.softmax(scores, axis=-1).astype(jnp.bfloat16)
    context = jnp.einsum('hqk,hke->hqe', attn_prob.astype(jnp.float32), v_one.astype(jnp.float32))
    return context.astype(jnp.bfloat16)


def gpt_layer(x_val, layer_par, lengths):
    w_qkv, w_out, w_up, b_up, w_down, vec_layer = layer_par
    a_in = layer_norm(x_val, vec_layer[0], vec_layer[1]).astype(jnp.bfloat16)
    qkv_all = jnp.einsum('bsd,dthe->tbhse', a_in.astype(jnp.float32), w_qkv.astype(jnp.float32)).astype(jnp.bfloat16)
    context = lax.map(attend_one, (qkv_all[0], qkv_all[1], qkv_all[2], lengths))
    attn_out = jnp.einsum('bhse,hed->bsd', context.astype(jnp.float32), w_out.astype(jnp.float32)).astype(jnp.bfloat16)
    hidden = x_val + attn_out.astype(jnp.float32) + vec_layer[4]
    a_mid = layer_norm(hidden, vec_layer[2], vec_layer[3]).astype(jnp.bfloat16)
    pre_act = jnp.einsum('bsd,df->bsf', a_mid.astype(jnp.float32), w_up.astype(jnp.float32)) + b_up
    act_bf = jax.nn.gelu(pre_act, approximate=True).astype(jnp.bfloat16)
    mlp_out = jnp.einsum('bsf,fd->bsd', act_bf.astype(jnp.float32), w_down.astype(jnp.float32)).astype(jnp.bfloat16)
    return hidden + mlp_out.astype(jnp.float32) + vec_layer[5]


def forward_stack(x_in, w_qkv, w_out, w_up, b_up, w_down, vec_par, lengths):
    def scan_step(carry_x, layer_par):
        return gpt_layer(carry_x, layer_par, lengths), None
    return lax.scan(scan_step, x_in, (w_qkv, w_out, w_up, b_up, w_down, vec_par))[0]


def reference(x_in, d_out, lengths, w_qkv, w_out, w_up, b_up, w_down, vec_par):
    y_out, pullback = jax.vjp(functools.partial(forward_stack, lengths=lengths), x_in, w_qkv, w_out, w_up, b_up, w_down, vec_par)
    grad_list = pullback(d_out.astype(jnp.float32))
    return (y_out, grad_list[0], grad_list[1], grad_list[2], grad_list[3], grad_list[4], grad_list[5], grad_list[6])
```

```python
from types import SimpleNamespace

import jax
import jax.numpy as jnp
from jax import lax
from jax.experimental import pallas as pl
from jax.experimental.pallas import tpu as pltpu
from jax.sharding import PartitionSpec as P

TP, DP = "tp", "dp"
D = 3072
ROWS = 128
TOK = 2 * 8 * ROWS
HEADS, HD = 4, 96
SEQS = 4
BM, BN = 384, 512
BF, F32 = jnp.bfloat16, jnp.float32
ANY = pl.ANY
VMEM_LIMIT = 66_900_000
GELU_C = 0.7978845608028654
Q_ORDER = (3, 1, 2, 0)
FIRST, MID, TOP, LAST = range(4)
N_FIRST, N_LN, N_RES, N_BWD2, N_BWD1 = range(5)
QKV, UP, DACT, DCTX = range(4)
WIDTH = (1152, 1536, 1536, 384)


def dims(lhs, rhs, lc, rc):
    return lax.dot_general(lhs, rhs, (((lc,), (rc,)), ((), ())), preferred_element_type=F32)


def peers():
    me = lax.axis_index(TP)
    dp = lax.axis_index(DP)
    core = me + 1 - 2 * lax.rem(me, 2)
    x = me + 2 - 4 * lax.rem(lax.div(me, 2), 2)
    y = me + 4 - 8 * lax.div(me, 4)
    return (dp, core), (dp, x), (dp, y)


def say_here(devices):
    for dev in devices:
        pl.semaphore_signal(pltpu.get_barrier_semaphore(), inc=1, device_id=dev, device_id_type=pl.DeviceIdType.MESH)


def await_peers(n=3):
    pl.semaphore_wait(pltpu.get_barrier_semaphore(), n)


def remote(src, dst, send, recv, dev):
    return pltpu.make_async_remote_copy(src_ref=src, dst_ref=dst, send_sem=send, recv_sem=recv, device_id=dev, device_id_type=pl.DeviceIdType.MESH)


class Pieces:
    def __init__(self, src, dst, sem, n):
        self.src, self.dst, self.sem, self.n = src, dst, sem, n

    def start(self):
        src, dst = self.src, self.dst
        step = src.shape[-2] // self.n
        for i in range(self.n):
            at = pl.ds(i * step, step)
            if len(src.shape) == 3:
                for j in range(src.shape[0]):
                    pltpu.make_async_copy(src.at[j, at], dst.at[j, at], self.sem).start()
            else:
                pltpu.make_async_copy(src.at[at], dst.at[at], self.sem).start()
        return self

    def wait(self):
        pltpu.make_async_copy(self.src, self.dst, self.sem).wait()


def call(name, cid, body, ins, outs, scratch, small):
    names = [list(vars(a)) for a in (ins, outs, scratch)]

    def kernel(*refs):
        body(SimpleNamespace(**dict(zip(sum(names, []), refs))))

    def spec(n):
        return pl.BlockSpec(memory_space=pltpu.VMEM if n in small else ANY)

    res = pl.pallas_call(
        kernel,
        name=name,
        out_shape=list(vars(outs).values()),
        in_specs=[spec(n) for n in names[0]],
        out_specs=[spec(n) for n in names[1]],
        scratch_shapes=list(vars(scratch).values()),
        compiler_params=pltpu.CompilerParams(vmem_limit_bytes=VMEM_LIMIT, collective_id=cid, has_side_effects=True),
    )(*vars(ins).values())
    return SimpleNamespace(**dict(zip(names[1], res)))


def fused(name, cid, kind, norm, arrays, vec, rs=None, ag=None, fills=(), bm=384, plan=()):
    ins, outs, sc = SimpleNamespace(**arrays), SimpleNamespace(), SimpleNamespace()
    dma = pltpu.SemaphoreType.DMA
    n_in = 2 if norm in (N_BWD2, N_BWD1) else 1
    n_acc = {N_BWD2: 4, N_BWD1: 2}.get(norm, 0)
    if norm != N_FIRST:
        outs.out0 = jax.ShapeDtypeStruct((2, ROWS, D), F32)
        sc.nout = pltpu.VMEM((ROWS, D), F32)
    if norm == N_RES:
        outs.out1 = jax.ShapeDtypeStruct((2, ROWS, D), F32)
        sc.nout1 = pltpu.VMEM((ROWS, D), F32)
    sc.nin = pltpu.VMEM((n_in, ROWS, D), F32)
    sc.nsem = dma((4,))
    if n_acc:
        outs.vo = jax.ShapeDtypeStruct((8, D), F32)
        sc.acc = pltpu.VMEM((n_acc, 8, D), F32)
    if rs:
        k1 = rs[1]
        tile1 = D if k1 <= 384 else 1024
        tiles1 = D // tile1
        sc.w1 = pltpu.VMEM((D, k1) if rs[2] else (k1, D), BF)
        sc.lhs = pltpu.VMEM((2, 2, ROWS, k1), BF)
        sc.own = pltpu.VMEM((2, 4, ROWS, D), BF)
        sc.snd = pltpu.VMEM((4, ROWS, D), BF)
        sc.drx = pltpu.VMEM((2, 4, ROWS, D), BF)
        sc.hx = pltpu.VMEM((2, 64, D), BF)
        sc.hy = pltpu.VMEM((2, 64, D), BF)
        sc.rx = pltpu.VMEM((2, ROWS, D), BF)
        sc.ry = pltpu.VMEM((2, ROWS, D), BF)
        sc.w1_sem = dma((tiles1,))
        sc.lhs_sem = dma((2,))
        sc.rs_send = dma((2, 10))
        sc.rs_recv = dma((2, 10))
    if ag:
        what = ag[0]
        n2 = WIDTH[what]
        outs.full = jax.ShapeDtypeStruct((2, 8, ROWS, D), BF)
        outs.res = jax.ShapeDtypeStruct((2, 8, ROWS, n2), BF)
        sc.w2 = pltpu.VMEM((D, n2) if what == UP else (n2, D), BF)
        sc.g = pltpu.VMEM((2, ROWS, D), BF)
        sc.agin = pltpu.VMEM((2, 2, ROWS, D), BF)
        sc.w2_sem = dma
        sc.g_sem = dma((2,))
        sc.agin_sem = dma((2,))
        sc.ag_send = dma((2, 10))
        sc.ag_recv = dma((2, 10))
        sc.res_st = pltpu.VMEM((2, 2, ROWS, n2), BF)
        sc.res_sem = dma((2,))
        if what == UP:
            outs.pre = jax.ShapeDtypeStruct((2, 8, ROWS, n2), F32)
        if what == DACT:
            outs.bup = jax.ShapeDtypeStruct((1, n2), F32)
            sc.bacc = pltpu.VMEM((8, n2), F32)
        if what in (UP, DACT):
            sc.pre_st = pltpu.VMEM((2, 2, ROWS, n2), F32)
            sc.pre_sem = dma((2,))
    if fills:
        sc.f_lhs = pltpu.VMEM((TOK, bm), BF)
        sc.f_at = pltpu.VMEM((bm, TOK), BF)
        sc.f_rhs = pltpu.VMEM((2, TOK, BN), BF)
        sc.f_out = pltpu.VMEM((2, bm, BN), BF)
        sc.f_sem = dma((5,))
        outs.g0 = jax.ShapeDtypeStruct(fills[0], BF)
        outs.g1 = jax.ShapeDtypeStruct(fills[1], BF)

    def body(r):
        core, px, py = peers()

        def begin(src, dst, sem, n=4):
            return Pieces(src, dst, sem, n).start()

        def norm_load(h):
            return [begin(x.at[h], r.nin.at[i], r.nsem.at[i]) for i, x in enumerate((r.in0, r.in1) if n_in == 2 else (r.in0,))]

        def vrow(row):
            return r.vec[row[0], row[1] : row[1] + 1, :]

        out_copy = []

        def norm_half(h, loads):
            for c in loads:
                c.wait()
            while out_copy:
                out_copy.pop().wait()

            def rows(i, _):
                at = pl.ds(pl.multiple_of(i * 16, 16), 16)
                x = r.nin[0, at, :]
                if rs:
                    o = r.own[h, 0, at, :].astype(F32) + r.rx[h, at, :].astype(F32) + r.ry[h, at, :].astype(F32)
                    o = o.astype(BF).astype(F32)
                if norm in (N_LN, N_RES):
                    x = x + o + vrow(vec.bias)
                    r.nout[at, :] = x
                if norm == N_RES:
                    r.nout1[at, :] = r.g[h, at, :].astype(F32)
                    return 0
                mean = jnp.sum(x, axis=-1, keepdims=True) * (1.0 / D)
                cen = x - mean
                var = jnp.sum(cen * cen, axis=-1, keepdims=True) * (1.0 / D)
                rstd = lax.rsqrt(var + 1e-5)
                if norm in (N_FIRST, N_LN):
                    r.g[h, at, :] = (cen * rstd * vrow(vec.gain) + vrow(vec.shift)).astype(BF)
                    return 0
                xh = cen * rstd
                dxh = o * vrow(vec.gain)
                m1 = jnp.sum(dxh, axis=-1, keepdims=True) * (1.0 / D)
                m2 = jnp.sum(dxh * xh, axis=-1, keepdims=True) * (1.0 / D)
                base = r.nin[1, at, :]
                res = base + rstd * (dxh - m1 - xh * m2)
                r.nout[at, :] = res
                if ag:
                    r.g[h, at, :] = res.astype(BF)
                sums = [o * xh, o] + ([res, base] if norm == N_BWD2 else [])
                for j, s in enumerate(sums):
                    r.acc[j] += s[0:8] + s[8:16]
                return 0

            lax.fori_loop(0, ROWS // 16, rows, 0)
            if norm != N_FIRST:
                out_copy.append(begin(r.nout, r.out0.at[h], r.nsem.at[2]))
            if norm == N_RES:
                out_copy.append(begin(r.nout1, r.out1.at[h], r.nsem.at[3]))

        top, bot = pl.ds(0, 64), pl.ds(64, 64)
        if rs:
            seq = [(h, q) for h in (0, 1) for q in Q_ORDER]
            lhs_loads, rs_copy, w1_loads = {}, {}, []

            def w1_load():
                for n in range(tiles1):
                    at = pl.ds(n * tile1, tile1)
                    src, dst = r.wa.at[rs[0]], r.w1
                    src, dst = (src.at[at], dst.at[at]) if rs[2] else (src.at[:, at], dst.at[:, at])
                    w1_loads.append(begin(src, dst, r.w1_sem.at[n]))

            def lhs_load(i):
                h, q = seq[i]
                lhs_loads[i] = begin(r.lhs1.at[h, pl.ds(2 * q, 2)], r.lhs.at[i % 2], r.lhs_sem.at[i % 2])

            def rs_start(h, j, src, dst, dev):
                c = remote(src, dst, r.rs_send.at[h, j], r.rs_recv.at[h, j], dev)
                c.start()
                rs_copy[h, j] = c

            def partial(i, between=None):
                h, q = seq[i]
                lhs_loads[i].wait()
                if h == 1:
                    rs_copy[0, q].wait_send()

                def tile(n, _):
                    at = pl.ds(pl.multiple_of(n * tile1, tile1), tile1)
                    x = r.lhs[i % 2].reshape(2 * ROWS, k1)
                    y = dims(x, r.w1[at, :], 1, 1) if rs[2] else dims(x, r.w1[:, at], 1, 0)
                    y = y.astype(BF)
                    r.own[h, q, :, at] = y[0:ROWS]
                    r.snd[q, :, at] = y[ROWS:]
                    return 0

                if i == 0:
                    for n in range(tiles1):
                        w1_loads[n].wait()
                        tile(n, 0)
                    await_peers()
                else:
                    tile(0, 0)
                    if between:
                        between()
                    if tiles1 > 1:
                        lax.fori_loop(1, tiles1, tile, 0)
                if i + 2 < len(seq):
                    lhs_load(i + 2)
                rs_start(h, q, r.snd.at[q], r.drx.at[h, q], core)

            def add_into(dst, src, n):
                def rows(i, _):
                    at = pl.ds(pl.multiple_of(i * 16, 16), 16)
                    dst[at, :] = (dst[at, :].astype(F32) + src[at, :].astype(F32)).astype(BF)
                    return 0

                lax.fori_loop(0, n // 16, rows, 0)

            def merge(h, q):
                rs_copy[h, q].wait_recv()
                add_into(r.own.at[h, q], r.drx.at[h, q], ROWS)

            def first_sends(h, q):
                if q == 3:
                    rs_start(h, 4, r.own.at[h, 3, top], r.hx.at[h], px)
                    rs_start(h, 5, r.own.at[h, 3, bot], r.hy.at[h], py)
                if q == 1:
                    rs_start(h, 6, r.own.at[h, 1, top], r.rx.at[h, top], px)
                if q == 2:
                    rs_start(h, 7, r.own.at[h, 2, bot], r.ry.at[h, bot], py)

            def third_sends(h):
                rs_copy[h, 5].wait_recv()
                add_into(r.own.at[h, 1, bot], r.hy.at[h], 64)
                rs_start(h, 8, r.own.at[h, 1, bot], r.rx.at[h, bot], px)
                rs_copy[h, 4].wait_recv()
                add_into(r.own.at[h, 2, top], r.hx.at[h], 64)
                rs_start(h, 9, r.own.at[h, 2, top], r.ry.at[h, top], py)

            def rs_done(h):
                for j in (6, 7, 8, 9):
                    rs_copy[h, j].wait_recv()

            def step(i, send=True):
                def between():
                    h, q = seq[i - 1]
                    merge(h, q)
                    if send:
                        first_sends(h, q)

                partial(i, between if i % 4 else None)

        if ag:
            full = r.full
            ag_copy, g_copy, ready_loads, res_out, w2_ready, count = {}, {}, {}, {}, [], [0]

            def ag_start(h, j, src, dst, dev):
                c = remote(src, dst, r.ag_send.at[h, j], r.ag_recv.at[h, j], dev)
                c.start()
                ag_copy[h, j] = c

            def own_sends(h):
                g = r.g
                ag_start(h, 1, g.at[h, top], full.at[h, 2, top], px)
                ag_start(h, 3, g.at[h, bot], full.at[h, 4, bot], py)
                ag_start(h, 2, g.at[h, bot], full.at[h, 2, bot], px)
                ag_start(h, 4, g.at[h, top], full.at[h, 4, top], py)
                ag_start(h, 0, g.at[h], full.at[h, 1], core)
                g_copy[h] = begin(g.at[h], full.at[h, 0], r.g_sem.at[h])

            def forward(h):
                ag_copy[h, 1].wait_recv()
                ag_start(h, 5, full.at[h, 2, top], full.at[h, 6, top], py)
                ag_copy[h, 3].wait_recv()
                ag_start(h, 6, full.at[h, 4, bot], full.at[h, 6, bot], px)

            def cross(h):
                ag_copy[h, 2].wait_recv()
                ag_start(h, 7, full.at[h, 2], full.at[h, 3], core)
                ag_copy[h, 4].wait_recv()
                ag_start(h, 8, full.at[h, 4], full.at[h, 5], core)

            def cross_far(h):
                ag_copy[h, 5].wait_recv()
                ag_copy[h, 6].wait_recv()
                ag_start(h, 9, full.at[h, 6], full.at[h, 7], core)

            def ready(h, q):
                s = count[0] % 2
                count[0] += 1
                if q == 0:
                    g_copy.pop(h).wait()
                    ag_copy[h, 0].wait_recv()
                else:
                    ag_copy[h, {1: 7, 2: 8, 3: 9}[q]].wait_recv()
                pair = pl.ds(2 * q, 2)
                loads = [begin(full.at[h, pair], r.agin.at[s], r.agin_sem.at[s])]
                if what == DACT:
                    loads.append(begin(r.pre.at[h, pair], r.pre_st.at[s], r.pre_sem.at[s]))
                ready_loads[h, q] = (s, loads)

            def product(h, q):
                if (h, q) not in ready_loads:
                    ready(h, q)
                s, loads = ready_loads.pop((h, q))
                pair = pl.ds(2 * q, 2)
                if not w2_ready:
                    w2_copy.wait()
                    w2_ready.append(1)
                for c in res_out.pop(s, ()):
                    c.wait()
                for c in loads:
                    c.wait()
                nt = 384 if what in (QKV, DCTX) else 512

                def tile(n, _):
                    at = pl.ds(pl.multiple_of(n * nt, nt), nt)
                    x = r.agin[s].reshape(2 * ROWS, D)
                    y = dims(x, r.w2[:, at], 1, 0) if what == UP else dims(x, r.w2[at, :], 1, 1)
                    if what == UP:
                        u = y + r.b_up[ag[1] : ag[1] + 1, at]
                        r.pre_st[s, :, :, at] = u.reshape(2, ROWS, nt)
                        y = u * (0.5 * (1.0 + jnp.tanh(GELU_C * (u + 0.044715 * (u * u * u)))))
                    if what == DACT:
                        u = r.pre_st[s, :, :, at].reshape(2 * ROWS, nt)
                        y = y.astype(BF).astype(F32)
                        t = jnp.tanh(GELU_C * (u + 0.044715 * (u * u * u)))
                        slope = 0.5 * (1.0 + t) + (0.5 * GELU_C) * u * (1.0 - t * t) * (1.0 + (3 * 0.044715) * (u * u))
                        y = y * slope
                        r.bacc[:, at] += jnp.sum(y.reshape(2 * ROWS // 8, 8, nt), axis=0)
                    r.res_st[s, :, :, at] = y.astype(BF).reshape(2, ROWS, nt)
                    return 0

                if n2 == nt:
                    tile(0, 0)
                else:
                    lax.fori_loop(0, n2 // nt, tile, 0)
                res_out[s] = [begin(r.res_st.at[s], r.res.at[h, pair], r.res_sem.at[s])]
                if what == UP:
                    res_out[s].append(begin(r.pre_st.at[s], r.pre.at[h, pair], r.pre_sem.at[s]))

        todo = []
        if fills:
            jobs = ((r.f0l, r.f0r, r.g0), (r.f1l, r.f1r, r.g1))
            todo = [[job, f[0] // bm, f[1] // BN, 0] for job, f in zip(jobs, fills)]

        def fill(n):
            while n > 0 and todo:
                (lhs, rhs, out), blocks, tiles, done = todo[0]
                count_all = blocks * tiles

                def lhs_copy(b):
                    return Pieces(lhs.at[:, pl.ds(pl.multiple_of(b * bm, bm), bm)], r.f_lhs, r.f_sem.at[0], 8)

                def rhs_copy(u):
                    t, s = lax.rem(u, tiles), lax.rem(u, 2)
                    return Pieces(rhs.at[:, pl.ds(pl.multiple_of(t * BN, BN), BN)], r.f_rhs.at[s], r.f_sem.at[1 + s], 8)

                def put_copy(u):
                    b, t, s = lax.div(u, tiles), lax.rem(u, tiles), lax.rem(u, 2)
                    dst = out.at[pl.ds(pl.multiple_of(b * bm, bm), bm), pl.ds(pl.multiple_of(t * BN, BN), BN)]
                    return Pieces(r.f_out.at[s], dst, r.f_sem.at[3 + s], 3)

                if done == 0:
                    lhs_copy(jnp.int32(0)).start()
                    rhs_copy(jnp.int32(0)).start()
                upto = min(count_all, done + n)

                def unit(u, _):
                    b, t, s = lax.div(u, tiles), lax.rem(u, tiles), lax.rem(u, 2)

                    @pl.when(t == 0)
                    def _():
                        lhs_copy(b).wait()
                        for k in range(TOK // 256):
                            r.f_at[:, k * 256 : (k + 1) * 256] = r.f_lhs[k * 256 : (k + 1) * 256, :].T

                        @pl.when(b + 1 < blocks)
                        def _():
                            lhs_copy(b + 1).start()

                    rhs_copy(u).wait()

                    @pl.when(u + 1 < count_all)
                    def _():
                        rhs_copy(u + 1).start()

                    @pl.when(u >= 2)
                    def _():
                        put_copy(u - 2).wait()

                    r.f_out[s] = dims(r.f_at[...], r.f_rhs[s], 1, 0).astype(BF)
                    put_copy(u).start()
                    return 0

                lax.fori_loop(done, upto, unit, 0)
                n -= upto - done
                todo[0][3] = upto
                if upto == count_all:
                    for u in range(max(0, count_all - 2), count_all):
                        put_copy(jnp.int32(u)).wait()
                    todo.pop(0)

        steps = list(plan)

        def fill_next():
            if steps:
                fill(steps.pop(0))

        say_here((core, px, py))
        if rs:
            lhs_load(0)
            w1_load()
            lhs_load(1)
        if kind == TOP:
            srcs = [begin(r.src.at[h], r.g.at[h], r.g_sem.at[h]) for h in (0, 1)]
        loads = norm_load(0)
        if ag:
            w2_copy = begin(r.wb.at[ag[1]], r.w2, r.w2_sem, 8)
        for j in range(n_acc):
            r.acc[j] = jnp.zeros((8, D), F32)
        if ag and what == DACT:
            r.bacc[...] = jnp.zeros((8, n2), F32)

        def both_halves():
            for i in range(4):
                step(i)
            merge(0, 0)
            third_sends(0)
            for i in range(4, 8):
                step(i)
            merge(1, 0)
            fill_next()
            rs_done(0)
            norm_half(0, loads)

        if kind == FIRST:
            norm_half(0, loads)
            loads = norm_load(1)
            await_peers()
            own_sends(0)
            norm_half(1, loads)
            product(0, 0)
            forward(0)
            own_sends(1)
            ready(1, 0)
            cross(0)
            product(1, 0)
            ready(0, 1)
            ready(0, 2)
            product(0, 1)
            product(0, 2)
            cross_far(0)
            product(0, 3)
            forward(1)
            cross(1)
            ready(1, 1)
            ready(1, 2)
            product(1, 1)
            product(1, 2)
            cross_far(1)
            product(1, 3)
        elif kind == LAST:
            both_halves()
            loads = norm_load(1)
            fill_next()
            third_sends(1)
            fill(1 << 20)
            rs_done(1)
            norm_half(1, loads)
        elif kind == MID:
            both_halves()
            loads = norm_load(1)
            fill_next()
            third_sends(1)
            own_sends(0)
            fill_next()
            ready(0, 0)
            product(0, 0)
            fill_next()
            rs_done(1)
            norm_half(1, loads)
            fill_next()
            forward(0)
            own_sends(1)
            fill_next()
            ready(1, 0)
            product(1, 0)
            fill_next()
            cross(0)
            fill_next()
            ready(0, 1)
            ready(0, 2)
            product(0, 1)
            product(0, 2)
            cross_far(0)
            fill(1 << 20)
            product(0, 3)
            forward(1)
            cross(1)
            ready(1, 1)
            ready(1, 2)
            product(1, 1)
            product(1, 2)
            cross_far(1)
            product(1, 3)
        elif kind == TOP:
            for c in srcs:
                c.wait()
            partial(0)
            own_sends(0)
            step(1, False)
            step(2, False)
            step(3, False)
            forward(0)
            own_sends(1)
            merge(0, 0)
            ready(0, 0)
            product(0, 0)
            cross(0)
            ready(1, 0)
            product(1, 0)
            ready(0, 1)
            ready(0, 2)
            product(0, 1)
            product(0, 2)
            forward(1)
            cross_far(0)
            for q in (3, 1, 2):
                first_sends(0, q)
            partial(4)
            product(0, 3)
            cross(1)
            step(5, False)
            ready(1, 1)
            ready(1, 2)
            product(1, 1)
            cross_far(1)
            product(1, 2)
            third_sends(0)
            for q in (3, 1):
                if q == 1:
                    merge(1, 1)
                first_sends(1, q)
            partial(6)
            merge(1, 2)
            first_sends(1, 2)
            partial(7)
            merge(1, 0)
            ready(1, 3)
            rs_done(0)
            norm_half(0, loads)
            loads = norm_load(1)
            product(1, 3)
            third_sends(1)
            rs_done(1)
            norm_half(1, loads)

        for j in range(n_acc):
            r.vo[j : j + 1, :] = jnp.sum(r.acc[j], axis=0, keepdims=True)
        if n_acc:
            r.vo[n_acc:8, :] = jnp.zeros((8 - n_acc, D), F32)
        if ag and what == DACT:
            r.bup[...] = jnp.sum(r.bacc[...], axis=0, keepdims=True)
        for c in out_copy:
            c.wait()
        if rs:
            for (h, j), c in rs_copy.items():
                if not (h == 0 and j < 4):
                    c.wait_send()
        if ag:
            for c in ag_copy.values():
                c.wait_send()
            for cs in res_out.values():
                for c in cs:
                    c.wait()

    small = ["vec", "b_up", "vo", "bup"]
    return call(name, cid, body, ins, outs, sc, small)


def visible(me, length):
    row = lax.broadcasted_iota(jnp.int32, (ROWS, ROWS), 0)
    col = lax.broadcasted_iota(jnp.int32, (ROWS, ROWS), 1)
    row_pos = lax.bitwise_or(lax.shift_left(lax.bitwise_xor(lax.shift_right_logical(row, 4), me), 4), lax.bitwise_and(row, 15))
    col_pos = lax.bitwise_or(lax.shift_left(lax.bitwise_xor(lax.shift_right_logical(col, 4), me), 4), lax.bitwise_and(col, 15))
    return (col_pos <= row_pos) & (col_pos < length)


def head_parts(x, h):
    return x[:, h * HD : (h + 1) * HD], x[:, 384 + h * HD : 384 + (h + 1) * HD], x[:, 768 + h * HD : 768 + (h + 1) * HD]


def probs(q, k, mask):
    s = dims(q, k, 1, 1) * (HD**-0.5)
    s = jnp.where(mask, s, -1e30)
    e = jnp.exp(s - jnp.max(s, axis=-1, keepdims=True))
    return e * (1.0 / jnp.sum(e, axis=-1, keepdims=True))


def attn_fwd_kernel(info, qkv, ctx):
    for i in range(SEQS):
        mask = visible(info[16], info[pl.program_id(0) * SEQS + i])
        x = qkv[:, i].reshape(ROWS, 1152)
        parts = []
        for h in range(HEADS):
            q, k, v = head_parts(x, h)
            parts.append(dims(probs(q, k, mask).astype(BF), v, 1, 0).astype(BF))
        ctx[:, i] = jnp.concatenate(parts, axis=-1).reshape(8, 16, 384)


def attn_bwd_one(info, i, qkv, dctx, out):
    mask = visible(info[16], info[pl.program_id(0) * SEQS + i])
    x = qkv[:, i].reshape(ROWS, 1152)
    dc = dctx[:, i].reshape(ROWS, 384)
    dqs, dks, dvs = [], [], []
    for h in range(HEADS):
        q, k, v = head_parts(x, h)
        d = dc[:, h * HD : (h + 1) * HD]
        p = probs(q, k, mask)
        dp = dims(d, v, 1, 1).astype(BF).astype(F32)
        dvs.append(dims(p.astype(BF), d, 0, 0).astype(BF))
        ds = p * (dp - jnp.sum(dp * p, axis=-1, keepdims=True))
        ds = (ds * (HD**-0.5)).astype(BF)
        dqs.append(dims(ds, k, 1, 0).astype(BF))
        dks.append(dims(ds, q, 0, 0).astype(BF))
    out[:, i] = jnp.concatenate(dqs + dks + dvs, axis=-1).reshape(8, 16, 1152)


def seq_spec(n):
    return pl.BlockSpec((None, 8, SEQS, 16, n), lambda i, info: (i // (8 // SEQS), 0, i % (8 // SEQS), 0, 0))


def by_seq(a):
    return a.reshape(2, 8, 8, 16, a.shape[-1])


def attn_fwd(info, qkv):
    grid_spec = pltpu.PrefetchScalarGridSpec(num_scalar_prefetch=1, grid=(16 // SEQS,), in_specs=[seq_spec(1152)], out_specs=seq_spec(384))
    out = pl.pallas_call(attn_fwd_kernel, name="attn_fwd", out_shape=jax.ShapeDtypeStruct((2, 8, 8, 16, 384), BF), grid_spec=grid_spec)(info, by_seq(qkv))
    return out.reshape(2, 8, ROWS, 384)


def stacking(puts, stacks, n):
    used = sorted({p[1] for p in puts})
    shapes = [jax.ShapeDtypeStruct((n,) + next(p[0].shape for p in puts if p[1] == k), BF) for k in used]
    given = [k for k in used if stacks[k] is not None]
    return used, shapes, given


def attn_bwd(info, qkv, dctx, puts, stacks, n):
    used, shapes, given = stacking(puts, stacks, n)
    m = len(puts)

    def kernel(info, qkv, dctx, *refs):
        grads, refs = refs[:m], refs[m + len(given) :]
        out, outs, bounce, sem = refs[0], refs[1 : 1 + len(used)], refs[1 + len(used) : -1], refs[-1]
        step = pl.program_id(0)

        def load(i):
            return Pieces(grads[i], bounce[i], sem.at[0, i], 8)

        def put(i):
            return Pieces(bounce[i], outs[used.index(puts[i][1])].at[puts[i][2]], sem.at[1, i], 8)

        @pl.when(step == 0)
        def _():
            for i in range(m):
                load(i).start()

        for at, some in ((1, range(m // 2)), (2, range(m // 2, m))):

            @pl.when(step == at)
            def _(some=some):
                for i in some:
                    load(i).wait()
                    put(i).start()

        for i in range(SEQS):
            attn_bwd_one(info, i, qkv, dctx, out)

        @pl.when(step == 16 // SEQS - 1)
        def _():
            for i in range(m):
                put(i).wait()

    hbm = pl.BlockSpec(memory_space=ANY)
    grid_spec = pltpu.PrefetchScalarGridSpec(
        num_scalar_prefetch=1,
        grid=(16 // SEQS,),
        in_specs=[seq_spec(1152), seq_spec(384)] + [hbm] * (m + len(given)),
        out_specs=[seq_spec(1152)] + [hbm] * len(used),
        scratch_shapes=[pltpu.VMEM(p[0].shape, BF) for p in puts] + [pltpu.SemaphoreType.DMA((2, m))],
    )
    res = pl.pallas_call(
        kernel,
        name="attn_bwd",
        out_shape=[jax.ShapeDtypeStruct((2, 8, 8, 16, 1152), BF)] + shapes,
        grid_spec=grid_spec,
        input_output_aliases={3 + m + j: 1 + used.index(k) for j, k in enumerate(given)},
        compiler_params=pltpu.CompilerParams(vmem_limit_bytes=VMEM_LIMIT),
    )(info, by_seq(qkv), by_seq(dctx), *[p[0] for p in puts], *[stacks[k] for k in given])
    for k, a in zip(used, res[1:]):
        stacks[k] = a
    return res[0].reshape(2, 8, ROWS, 1152)


def put_last(puts, stacks):
    m = len(puts)

    def kernel(*refs):
        grads, outs, bounce, sem = refs[:m], refs[2 * m : 3 * m], refs[3 * m : -1], refs[-1]
        loads = [Pieces(grads[i], bounce[i], sem.at[0, i], 8).start() for i in range(m)]
        stores = []
        for i in range(m):
            loads[i].wait()
            stores.append(Pieces(bounce[i], outs[i].at[puts[i][2]], sem.at[1, i], 8).start())
        for c in stores:
            c.wait()

    hbm = pl.BlockSpec(memory_space=ANY)
    olds = [stacks[p[1]] for p in puts]
    res = pl.pallas_call(
        kernel,
        name="put_last",
        out_shape=[jax.ShapeDtypeStruct(a.shape, a.dtype) for a in olds],
        in_specs=[hbm] * (2 * m),
        out_specs=[hbm] * m,
        scratch_shapes=[pltpu.VMEM(p[0].shape, BF) for p in puts] + [pltpu.SemaphoreType.DMA((2, m))],
        input_output_aliases={m + i: i for i in range(m)},
        compiler_params=pltpu.CompilerParams(vmem_limit_bytes=VMEM_LIMIT),
    )(*[p[0] for p in puts], *olds)
    for p, a in zip(puts, res):
        stacks[p[1]] = a


def sum_rows(parts, cid):
    n, half = len(parts), D // 2
    rows = -(-6 * n // 8) * 8
    ins = SimpleNamespace()
    for l, (a, b) in enumerate(parts):
        setattr(ins, f"a{l}", a)
        setattr(ins, f"b{l}", b)

    def body(r):
        core, px, py = peers()
        say_here((core, px, py))
        me = lax.axis_index(TP)
        mine = pl.ds(pl.multiple_of(lax.rem(me, 2) * half, half), half)
        for l in range(n):
            r.v[6 * l : 6 * l + 2, :] = getattr(r, f"a{l}")[0:2, :]
            r.v[6 * l + 2 : 6 * l + 6, :] = getattr(r, f"b{l}")[0:4, :]
        if rows > 6 * n:
            r.v[6 * n :, :] = jnp.zeros((rows - 6 * n, D), F32)
        await_peers()
        c = remote(r.v, r.a, r.send.at[0], r.recv.at[0], core)
        c.start()
        c.wait()
        r.s[0] = r.v[:, mine] + r.a[:, mine]
        for i, dev in ((0, px), (1, py)):
            c = remote(r.s.at[i], r.b.at[i], r.send.at[1 + i], r.recv.at[1 + i], dev)
            c.start()
            c.wait()
            r.s[i + 1] = r.s[i] + r.b[i]
        c = remote(r.s.at[2], r.t.at[:, mine], r.send.at[3], r.recv.at[3], core)
        c.start()
        r.u[:, mine] = r.s[2]
        c.wait()
        first = lax.broadcasted_iota(jnp.int32, (1, D), 1) < half
        keep = first == (lax.rem(me, 2) == 0)
        for l in range(n):
            at = slice(6 * l, 6 * l + 6)
            r.o[l] = jnp.where(keep, r.u[at, :], r.t[at, :])

    dma = pltpu.SemaphoreType.DMA
    scratch = SimpleNamespace(
        v=pltpu.VMEM((rows, D), F32),
        a=pltpu.VMEM((rows, D), F32),
        s=pltpu.VMEM((3, rows, half), F32),
        b=pltpu.VMEM((2, rows, half), F32),
        t=pltpu.VMEM((rows, D), F32),
        u=pltpu.VMEM((rows, D), F32),
        send=dma((4,)),
        recv=dma((4,)),
    )
    outs = SimpleNamespace(o=jax.ShapeDtypeStruct((n, 6, D), F32))
    return call("sum_rows", cid, body, ins, outs, scratch, list(vars(ins)) + ["o"]).o


def group_body(x_loc, dy_loc, len_loc, wqkv, wout, wup, bup, wdown, vec):
    n = wqkv.shape[0]
    ids = iter(range(64))
    x = x_loc.reshape(2, ROWS, D)
    dy = dy_loc.reshape(2, ROWS, D)
    wq = jnp.transpose(wqkv, (0, 2, 3, 4, 1)).reshape(n, 1152, D)
    wo = wout.reshape(n, 384, D)
    info = jnp.concatenate([len_loc, lax.axis_index(TP).reshape(1).astype(jnp.int32)])

    def flat(a):
        return a.reshape(TOK, a.shape[-1])

    def ln(layer, row, bias=None):
        return SimpleNamespace(gain=(layer, row), shift=(layer, row + 1), bias=bias)

    saved = [SimpleNamespace() for _ in range(n)]
    r = fused("first", next(ids), FIRST, N_FIRST, dict(in0=x, wb=wq, vec=vec), ln(0, 0), ag=(QKV, 0))
    s = saved[0]
    s.x, s.a, s.qkv = x, r.full, r.res
    for l in range(n):
        s = saved[l]
        s.ctx = attn_fwd(info, s.qkv)
        arrays = dict(lhs1=s.ctx, wa=wo, wb=wup, in0=s.x, vec=vec, b_up=bup)
        r = fused(f"mlp_in_{l}", next(ids), MID, N_LN, arrays, ln(l, 2, (l, 4)), rs=(l, 384, False), ag=(UP, l))
        s.hid, s.m, s.act, s.pre = r.out0, r.full, r.res, r.pre
        if l + 1 < n:
            arrays = dict(lhs1=s.act, wa=wdown, wb=wq, in0=s.hid, vec=vec)
            r = fused(f"attn_in_{l + 1}", next(ids), MID, N_LN, arrays, ln(l + 1, 0, (l, 5)), rs=(l, 1536, False), ag=(QKV, l + 1))
            s = saved[l + 1]
            s.x, s.a, s.qkv = r.out0, r.full, r.res
    s = saved[n - 1]
    arrays = dict(lhs1=s.act, wa=wdown, wb=wdown, in0=s.hid, vec=vec, src=dy, pre=s.pre)
    r = fused("top", next(ids), TOP, N_RES, arrays, ln(0, 0, (n - 1, 5)), rs=(n - 1, 1536, False), ag=(DACT, n - 1))
    y, d_cur, d_full, d_pre = r.out0, r.out1, r.full, r.res
    g_bup, rows, puts, stacks = [r.bup], [], [], [None] * 4
    for l in reversed(range(n)):
        s = saved[l]
        arrays = dict(lhs1=d_pre, wa=wup, wb=wo, in0=s.hid, in1=d_cur, vec=vec, f0l=flat(s.act), f0r=flat(d_full), f1l=flat(s.m), f1r=flat(d_pre))
        r = fused(
            f"d_mlp_{l}", next(ids), MID, N_BWD2, arrays, ln(l, 2), rs=(l, 1536, True), ag=(DCTX, l),
            fills=((1536, D), (D, 1536)), bm=768, plan=(4, 2, 2, 7, 2, 1, 2, 2),
        )
        d_hid, d_attn, v3 = r.out0, r.full, r.vo
        puts += [(r.g0, 3, l), (r.g1, 2, l)]
        d_qkv = attn_bwd(info, s.qkv, r.res, puts, stacks, n)
        arrays = dict(lhs1=d_qkv, wa=wq, in0=s.x, in1=d_hid, vec=vec, f0l=flat(s.ctx), f0r=flat(d_attn), f1l=flat(d_qkv), f1r=flat(s.a))
        common = dict(rs=(l, 1152, False), fills=((384, D), (1152, D)))
        if l:
            arrays.update(wb=wdown, pre=saved[l - 1].pre)
            r = fused(f"d_attn_{l}", next(ids), MID, N_BWD1, arrays, ln(l, 0), ag=(DACT, l - 1), plan=(9, 4, 1, 7, 1, 1, 1), **common)
            g_bup.append(r.bup)
            d_full, d_pre = r.full, r.res
        else:
            r = fused(f"d_attn_{l}", next(ids), LAST, N_BWD1, arrays, ln(l, 0), plan=(9, 5), **common)
        puts = [(r.g0, 1, l), (r.g1, 0, l)]
        rows.append((r.vo, v3))
        d_cur = r.out0
    put_last(puts, stacks)
    g_vec = sum_rows(rows[::-1], next(ids))
    g_qkv = jnp.transpose(stacks[0].reshape(n, 3, HEADS, HD, D), (0, 4, 1, 2, 3))
    g_out = stacks[1].reshape(n, HEADS, HD, D)
    shape = x_loc.shape
    return y.reshape(shape), d_cur.reshape(shape), g_qkv, g_out, stacks[2], jnp.concatenate(g_bup[::-1]), stacks[3], g_vec


def solution(mesh):
    act_spec = P(DP, TP, None)
    in_specs = (act_spec, act_spec, P(DP), P(None, None, None, TP, None), P(None, TP, None, None), P(None, None, TP), P(None, TP), P(None, TP, None), P())
    out_specs = (act_spec, act_spec, P(DP, None, None, TP, None), P(DP, TP, None, None), P(DP, None, TP), P(DP, TP), P(DP, TP, None), P(DP, None, None))
    return jax.shard_map(group_body, mesh=mesh, in_specs=in_specs, out_specs=out_specs, check_vma=False)
```

```python
from functools import partial
from types import SimpleNamespace

import jax
import jax.numpy as jnp
from jax import lax
from jax.experimental import pallas as pl
from jax.experimental.pallas import tpu as pltpu
from jax.sharding import PartitionSpec as P

TP, DP = "tp", "dp"
D, FF, INNER, QKV_N = 3072, 1536, 384, 1152
ROWS, HALF_ROWS, GROUP = 128, 64, 16
LANES, SUBL = 128, 8
A, B = HALVES = range(2)
PEERS = 8
TOK = len(HALVES) * PEERS * ROWS
HEADS, HD = 4, 96
SEQS, ALL_SEQS = 4, 16
BM, BN, KT = 384, 512, 256
BF, F32 = jnp.bfloat16, jnp.float32
ANY = pl.ANY
VMEM_LIMIT = 66_900_000
GELU_C, GELU_D = 0.7978845608028654, 0.044715
EPS, NEG = 1e-5, -1e30
ONE, TWO, HALF = 1.0, 2, 0.5
OWN, XN, YN, FAR = PAIRS = range(4)
Q_ORDER = (FAR, XN, YN, OWN)
R_X, R_Y, R_FAR = 2, 4, 6
X_FAR, Y_FAR, X_RAW, Y_RAW, X_SUM, Y_SUM, N_RS = range(4, 11)
G_CORE, G_XT, G_XB, G_YB, G_YT, G_FT, G_FB, G_C3, G_C5, G_C7, N_AG = range(11)
CROSSING = {XN: G_C3, YN: G_C5, FAR: G_C7}
FIRST, MID, TOP, LAST = range(4)
N_FIRST, N_LN, N_RES, N_BWD2, N_BWD1 = range(5)
QKV, UP, DACT, DCTX = range(4)
WIDTH = (QKV_N, FF, FF, INNER)
ALL = 1 << 20


def dims(lhs, rhs, lc, rc):
    return lax.dot_general(lhs, rhs, (((lc,), (rc,)), ((), ())), preferred_element_type=F32)


def peers():
    me = lax.axis_index(TP)
    dp = lax.axis_index(DP)

    def flip(bit):
        return me + bit - TWO * bit * lax.rem(lax.div(me, bit), TWO)

    return [(dp, flip(1 << k)) for k in range(3)]


def say_here(devices):
    for dev in devices:
        pl.semaphore_signal(pltpu.get_barrier_semaphore(), inc=1, device_id=dev, device_id_type=pl.DeviceIdType.MESH)


def await_peers(n=3):
    pl.semaphore_wait(pltpu.get_barrier_semaphore(), n)


def remote(src, dst, send, recv, dev):
    return pltpu.make_async_remote_copy(src_ref=src, dst_ref=dst, send_sem=send, recv_sem=recv, device_id=dev, device_id_type=pl.DeviceIdType.MESH)


class Pieces:
    def __init__(self, src, dst, sem, n):
        self.src, self.dst, self.sem, self.n = src, dst, sem, n

    def start(self):
        src, dst = self.src, self.dst
        step = src.shape[-2] // self.n
        for i in range(self.n):
            at = pl.ds(i * step, step)
            if len(src.shape) == 3:
                for j in range(src.shape[0]):
                    pltpu.make_async_copy(src.at[j, at], dst.at[j, at], self.sem).start()
            else:
                pltpu.make_async_copy(src.at[at], dst.at[at], self.sem).start()
        return self

    def wait(self):
        pltpu.make_async_copy(self.src, self.dst, self.sem).wait()


def call(name, cid, body, ins, outs, scratch, small):
    names = [list(vars(a)) for a in (ins, outs, scratch)]

    def kernel(*refs):
        body(SimpleNamespace(**dict(zip(sum(names, []), refs))))

    def spec(n):
        return pl.BlockSpec(memory_space=pltpu.VMEM if n in small else ANY)

    res = pl.pallas_call(
        kernel,
        name=name,
        out_shape=list(vars(outs).values()),
        in_specs=[spec(n) for n in names[0]],
        out_specs=[spec(n) for n in names[1]],
        scratch_shapes=list(vars(scratch).values()),
        compiler_params=pltpu.CompilerParams(vmem_limit_bytes=VMEM_LIMIT, collective_id=cid, has_side_effects=True),
    )(*vars(ins).values())
    return SimpleNamespace(**dict(zip(names[1], res)))


def fused(name, cid, kind, norm, arrays, vec, rs=None, ag=None, fills=(), plan=()):
    ins, outs, sc = SimpleNamespace(**arrays), SimpleNamespace(), SimpleNamespace()
    dma = pltpu.SemaphoreType.DMA
    n_in = len([k for k in arrays if k in ("in0", "in1")])
    n_acc = {N_BWD2: 4, N_BWD1: TWO}.get(norm, 0)
    shard = jax.ShapeDtypeStruct((TWO, ROWS, D), F32)
    if norm != N_FIRST:
        outs.out0 = shard
        sc.nout = pltpu.VMEM((ROWS, D), F32)
    if norm == N_RES:
        outs.out1 = shard
        sc.nout1 = pltpu.VMEM((ROWS, D), F32)
    sc.nin = pltpu.VMEM((n_in, ROWS, D), F32)
    sc.nsem = dma((n_in + TWO,))
    if n_acc:
        outs.vo = jax.ShapeDtypeStruct((SUBL, D), F32)
        sc.acc = pltpu.VMEM((n_acc, SUBL, D), F32)
    if rs:
        k1 = rs[1]
        tile1 = 1024
        tiles1 = D // tile1
        halves = (TWO, ROWS, D)
        sc.w1 = pltpu.VMEM((D, k1) if rs[2] else (k1, D), BF)
        sc.lhs = pltpu.VMEM((TWO, TWO, ROWS, k1), BF)
        sc.own = pltpu.VMEM((TWO, len(PAIRS), ROWS, D), BF)
        sc.snd = pltpu.VMEM((len(PAIRS), ROWS, D), BF)
        sc.drx = pltpu.VMEM((TWO, len(PAIRS), ROWS, D), BF)
        sc.hx = pltpu.VMEM((TWO, HALF_ROWS, D), BF)
        sc.hy = pltpu.VMEM((TWO, HALF_ROWS, D), BF)
        sc.rx = pltpu.VMEM(halves, BF)
        sc.ry = pltpu.VMEM(halves, BF)
        sc.w1_sem = dma((tiles1,))
        sc.lhs_sem = dma((TWO,))
        sc.rs_send = dma((TWO, N_RS))
        sc.rs_recv = dma((TWO, N_RS))
        sc.far_send = dma((tiles1, len(PAIRS)))
        sc.far_recv = dma((tiles1, len(PAIRS)))
    if ag:
        what = ag[0]
        n2 = WIDTH[what]
        outs.full = jax.ShapeDtypeStruct((TWO, PEERS, ROWS, D), BF)
        outs.res = jax.ShapeDtypeStruct((TWO, PEERS, ROWS, n2), BF)
        pairs_of = (TWO, TWO, ROWS, n2)
        sc.w2 = pltpu.VMEM((D, n2) if what == UP else (n2, D), BF)
        sc.g = pltpu.VMEM((TWO, ROWS, D), BF)
        sc.agin = pltpu.VMEM((TWO, TWO, ROWS, D), BF)
        sc.last = pltpu.VMEM((TWO, ROWS, D), BF)
        sc.w2_sem = dma
        sc.g_sem = dma((TWO,))
        sc.agin_sem = dma((TWO,))
        sc.last_sem = dma((TWO,))
        sc.ag_send = dma((TWO, N_AG))
        sc.ag_recv = dma((TWO, N_AG))
        sc.res_st = pltpu.VMEM(pairs_of, BF)
        sc.res_sem = dma((TWO,))
        if what == UP:
            outs.pre = jax.ShapeDtypeStruct((TWO, PEERS, ROWS, n2), F32)
        if what == DACT:
            outs.bup = jax.ShapeDtypeStruct((1, n2), F32)
            sc.bacc = pltpu.VMEM((SUBL, n2), F32)
        if what in (UP, DACT):
            sc.pre_st = pltpu.VMEM(pairs_of, F32)
            sc.pre_sem = dma((TWO,))
    if fills:
        sub_most = max(f[2] for f in fills)
        sc.f_lhs = pltpu.VMEM((TOK, BM), BF)
        sc.f_at = pltpu.VMEM((sub_most, BM, TOK), BF)
        sc.f_rhs = pltpu.VMEM((TWO, TOK, BN), BF)
        sc.f_out = pltpu.VMEM((TWO, BM, BN), BF)
        sc.fl_sem = dma
        sc.fr_sem = dma((TWO,))
        sc.fo_sem = dma((TWO,))
        outs.g0 = jax.ShapeDtypeStruct(fills[0][:2], BF)
        outs.g1 = jax.ShapeDtypeStruct(fills[1][:2], BF)

    def body(r):
        core, px, py = peers()

        def begin(src, dst, sem, n=4):
            return Pieces(src, dst, sem, n).start()

        def norm_load(h):
            some = (r.in0, r.in1) if n_in == TWO else (r.in0,)
            return [begin(x.at[h], r.nin.at[i], r.nsem.at[i]) for i, x in enumerate(some)]

        def vrow(row):
            return r.vec[row[0], pl.ds(row[1], 1), :]

        out_copy = []

        def mean(x):
            return jnp.sum(x, axis=-1, keepdims=True) * (ONE / D)

        def norm_half(h, loads):
            for c in loads:
                c.wait()
            while out_copy:
                out_copy.pop().wait()

            def rows(i, carry):
                at = pl.ds(pl.multiple_of(i * GROUP, GROUP), GROUP)
                x = r.nin[0, at, :]
                if rs:
                    o = r.own[h, OWN, at, :].astype(F32) + r.rx[h, at, :].astype(F32) + r.ry[h, at, :].astype(F32)
                    o = o.astype(BF).astype(F32)
                if norm in (N_LN, N_RES):
                    x = x + o + vrow(vec.bias)
                    r.nout[at, :] = x
                if norm == N_RES:
                    r.nout1[at, :] = r.g[h, at, :].astype(F32)
                    return carry
                cen = x - mean(x)
                rstd = lax.rsqrt(mean(cen * cen) + EPS)
                if norm in (N_FIRST, N_LN):
                    r.g[h, at, :] = (cen * rstd * vrow(vec.gain) + vrow(vec.shift)).astype(BF)
                    return carry
                xh = cen * rstd
                dxh = o * vrow(vec.gain)
                base = r.nin[1, at, :]
                res = base + rstd * (dxh - mean(dxh) - xh * mean(dxh * xh))
                r.nout[at, :] = res
                if ag:
                    r.g[h, at, :] = res.astype(BF)
                sums = [o * xh, o] + ([res, base] if norm == N_BWD2 else [])
                for j, v in enumerate(sums):
                    r.acc[j] += v[:SUBL] + v[SUBL:]
                return carry

            lax.fori_loop(0, ROWS // GROUP, rows, 0)
            if norm != N_FIRST:
                out_copy.append(begin(r.nout, r.out0.at[h], r.nsem.at[n_in]))
            if norm == N_RES:
                out_copy.append(begin(r.nout1, r.out1.at[h], r.nsem.at[n_in + 1]))

        top, bot = pl.ds(0, HALF_ROWS), pl.ds(HALF_ROWS, HALF_ROWS)
        if rs:
            seq = [(h, q) for h in HALVES for q in Q_ORDER]
            lhs_loads, rs_copy, far_copy, w1_loads = {}, {}, {}, []
            own = r.own

            def w1_load():
                for n in range(tiles1):
                    at = pl.ds(n * tile1, tile1)
                    src, dst = r.wa.at[rs[0]], r.w1
                    src, dst = (src.at[at], dst.at[at]) if rs[2] else (src.at[:, at], dst.at[:, at])
                    w1_loads.append(begin(src, dst, r.w1_sem.at[n]))

            def lhs_load(i):
                h, q = seq[i]
                s = i % TWO
                lhs_loads[i] = begin(r.lhs1.at[h, pl.ds(TWO * q, TWO)], r.lhs.at[s], r.lhs_sem.at[s])

            def rs_start(h, j, src, dst, dev):
                c = remote(src, dst, r.rs_send.at[h, j], r.rs_recv.at[h, j], dev)
                c.start()
                rs_copy[h, j] = c

            def far_start(n, j, src, dst, dev):
                c = remote(src, dst, r.far_send.at[n, j], r.far_recv.at[n, j], dev)
                c.start()
                far_copy[n, j] = c

            def add_into(dst, src, n, at_cols=slice(None)):
                def rows(i, carry):
                    at = pl.ds(pl.multiple_of(i * GROUP, GROUP), GROUP)
                    dst[at, at_cols] = (dst[at, at_cols].astype(F32) + src[at, at_cols].astype(F32)).astype(BF)
                    return carry

                lax.fori_loop(0, n // GROUP, rows, 0)

            def far_merge(n, send):
                cols = pl.ds(n * tile1, tile1)
                far_copy[n, 0].wait_recv()
                add_into(own.at[A, FAR], r.drx.at[A, FAR], ROWS, cols)
                if send:
                    far_sends(n)

            def far_sends(n):
                cols = pl.ds(n * tile1, tile1)
                far_start(n, 1, own.at[A, FAR, top, cols], r.hx.at[A, :, cols], px)
                far_start(n, 2, own.at[A, FAR, bot, cols], r.hy.at[A, :, cols], py)

            def product_in(i, between=None, send=True):
                h, q = seq[i]
                s = i % TWO
                lhs_loads[i].wait()
                if i == len(PAIRS):
                    for n in range(tiles1):
                        far_copy[n, 0].wait_send()
                elif h == B:
                    rs_copy[A, q].wait_send()

                def tile(n, carry):
                    at = pl.ds(pl.multiple_of(n * tile1, tile1), tile1)
                    x = r.lhs[s].reshape(TWO * ROWS, k1)
                    y = dims(x, r.w1[at, :], 1, 1) if rs[2] else dims(x, r.w1[:, at], 1, 0)
                    y = y.astype(BF)
                    own[h, q, :, at] = y[:ROWS]
                    r.snd[q, :, at] = y[ROWS:]
                    return carry

                if i == 0:
                    for n in range(tiles1):
                        cols = pl.ds(n * tile1, tile1)
                        w1_loads[n].wait()
                        tile(n, 0)
                        if n == 0:
                            await_peers()
                        far_start(n, 0, r.snd.at[FAR, :, cols], r.drx.at[A, FAR, :, cols], core)
                        if n:
                            far_merge(n - 1, send)
                else:
                    tile(0, 0)
                    if between:
                        between()
                    lax.fori_loop(1, tiles1, tile, 0)
                if i + TWO < len(seq):
                    lhs_load(i + TWO)
                if i:
                    rs_start(h, q, r.snd.at[q], r.drx.at[h, q], core)

            def merge(h, q):
                rs_copy[h, q].wait_recv()
                add_into(own.at[h, q], r.drx.at[h, q], ROWS)

            def first_sends(h, q):
                if q == FAR:
                    rs_start(h, X_FAR, own.at[h, q, top], r.hx.at[h], px)
                    rs_start(h, Y_FAR, own.at[h, q, bot], r.hy.at[h], py)
                if q == XN:
                    rs_start(h, X_RAW, own.at[h, q, top], r.rx.at[h, top], px)
                if q == YN:
                    rs_start(h, Y_RAW, own.at[h, q, bot], r.ry.at[h, bot], py)

            def far_wait(h, j):
                if h == A:
                    for n in range(tiles1):
                        far_copy[n, 1 + j].wait_recv()
                else:
                    rs_copy[h, X_FAR + j].wait_recv()

            def third_sends(h):
                far_wait(h, 1)
                add_into(own.at[h, XN, bot], r.hy.at[h], HALF_ROWS)
                rs_start(h, X_SUM, own.at[h, XN, bot], r.rx.at[h, bot], px)
                far_wait(h, 0)
                add_into(own.at[h, YN, top], r.hx.at[h], HALF_ROWS)
                rs_start(h, Y_SUM, own.at[h, YN, top], r.ry.at[h, top], py)

            def rs_done(h):
                for j in (X_RAW, Y_RAW, X_SUM, Y_SUM):
                    rs_copy[h, j].wait_recv()

            def step(i, send=True):
                def between():
                    h, q = seq[i - 1]
                    if i == 1:
                        far_merge(tiles1 - 1, send)
                        return
                    merge(h, q)
                    if send:
                        first_sends(h, q)

                product_in(i, between if i % len(PAIRS) else None, send)

        if ag:
            full = r.full
            ag_copy, g_copy, ready_loads, res_out, w2_ready, last_copy = {}, {}, {}, {}, [], []

            def ag_start(h, j, src, dst, dev):
                c = remote(src, dst, r.ag_send.at[h, j], r.ag_recv.at[h, j], dev)
                c.start()
                ag_copy[h, j] = c

            def own_sends(h):
                g = r.g
                ag_start(h, G_XT, g.at[h, top], full.at[h, R_X, top], px)
                ag_start(h, G_YB, g.at[h, bot], full.at[h, R_Y, bot], py)
                ag_start(h, G_XB, g.at[h, bot], full.at[h, R_X, bot], px)
                ag_start(h, G_YT, g.at[h, top], full.at[h, R_Y, top], py)
                ag_start(h, G_CORE, g.at[h], full.at[h, 1], core)
                g_copy[h] = begin(g.at[h], full.at[h, 0], r.g_sem.at[h])

            def far_place(h, other):
                return full.at[h, R_FAR + other] if h == A else r.last.at[other]

            def forward(h):
                ag_copy[h, G_XT].wait_recv()
                ag_start(h, G_FT, full.at[h, R_X, top], far_place(h, 0).at[top], py)
                ag_copy[h, G_YB].wait_recv()
                ag_start(h, G_FB, full.at[h, R_Y, bot], far_place(h, 0).at[bot], px)

            def cross(h):
                ag_copy[h, G_XB].wait_recv()
                ag_start(h, G_C3, full.at[h, R_X], full.at[h, R_X + 1], core)
                ag_copy[h, G_YT].wait_recv()
                ag_start(h, G_C5, full.at[h, R_Y], full.at[h, R_Y + 1], core)

            def cross_far(h):
                ag_copy[h, G_FT].wait_recv()
                ag_copy[h, G_FB].wait_recv()
                ag_start(h, G_C7, far_place(h, 0), far_place(h, 1), core)
                if h == B:
                    last_copy.append(begin(r.last.at[0], full.at[h, R_FAR], r.last_sem.at[0]))

            def ready(h, q):
                s = (len(PAIRS) * h + (OWN, XN, YN, FAR).index(q)) % TWO
                pair = pl.ds(TWO * q, TWO)
                loads = []
                if what == DACT:
                    loads.append(begin(r.pre.at[h, pair], r.pre_st.at[s], r.pre_sem.at[s]))
                if q == OWN:
                    g_copy.pop(h).wait()
                    ag_copy[h, G_CORE].wait_recv()
                else:
                    ag_copy[h, CROSSING[q]].wait_recv()
                if (h, q) == (B, FAR):
                    last_copy.append(begin(r.last.at[1], full.at[h, R_FAR + 1], r.last_sem.at[1]))
                else:
                    loads.append(begin(full.at[h, pair], r.agin.at[s], r.agin_sem.at[s]))
                ready_loads[h, q] = (s, loads)

            def product(h, q):
                if (h, q) not in ready_loads:
                    ready(h, q)
                s, loads = ready_loads.pop((h, q))
                pair = pl.ds(TWO * q, TWO)
                if not w2_ready:
                    w2_copy.wait()
                    w2_ready.append(s)
                for c in res_out.pop(s, ()):
                    c.wait()
                for c in loads:
                    c.wait()
                nt = BM if what in (QKV, DCTX) else BN

                def tile(n, carry):
                    at = pl.ds(pl.multiple_of(n * nt, nt), nt)
                    x = r.last[...] if (h, q) == (B, FAR) else r.agin[s]
                    x = x.reshape(TWO * ROWS, D)
                    y = dims(x, r.w2[:, at], 1, 0) if what == UP else dims(x, r.w2[at, :], 1, 1)
                    if what == UP:
                        u = y + r.b_up[pl.ds(ag[1], 1), at]
                        r.pre_st[s, :, :, at] = u.reshape(TWO, ROWS, nt)
                        y = u * (HALF * (ONE + jnp.tanh(GELU_C * (u + GELU_D * (u * u * u)))))
                    if what == DACT:
                        u = r.pre_st[s, :, :, at].reshape(TWO * ROWS, nt)
                        y = y.astype(BF).astype(F32)
                        t = jnp.tanh(GELU_C * (u + GELU_D * (u * u * u)))
                        y = y * (HALF * (ONE + t) + (HALF * GELU_C) * u * (ONE - t * t) * (ONE + (3 * GELU_D) * (u * u)))
                        r.bacc[:, at] += jnp.sum(y.reshape(-1, SUBL, nt), axis=0)
                    r.res_st[s, :, :, at] = y.astype(BF).reshape(TWO, ROWS, nt)
                    return carry

                if n2 == nt:
                    tile(0, 0)
                else:
                    lax.fori_loop(0, n2 // nt, tile, 0)
                res_out[s] = [begin(r.res_st.at[s], r.res.at[h, pair], r.res_sem.at[s])]
                if what == UP:
                    res_out[s].append(begin(r.pre_st.at[s], r.pre.at[h, pair], r.pre_sem.at[s]))

        jobs = []
        if fills:
            refs = ((r.f0l, r.f0r, r.g0), (r.f1l, r.f1r, r.g1))
            jobs = [SimpleNamespace(lhs=f[0], rhs=f[1], out=f[2], blocks=c[0] // BM // c[2], tiles=c[1] // BN, sub=c[2], done=0) for f, c in zip(refs, fills)]

        def lhs_copy(j, k):
            return Pieces(j.lhs.at[:, pl.ds(pl.multiple_of(k * BM, BM), BM)], r.f_lhs, r.fl_sem, PEERS)

        def rhs_copy(j, v):
            s = lax.rem(v, TWO)
            return Pieces(j.rhs.at[:, pl.ds(pl.multiple_of(lax.rem(v, j.tiles) * BN, BN), BN)], r.f_rhs.at[s], r.fr_sem.at[s], PEERS)

        def put_copy(j, u):
            s, v = lax.rem(u, TWO), lax.div(u, j.sub)
            row = lax.div(v, j.tiles) * j.sub + lax.rem(u, j.sub)
            dst = j.out.at[pl.ds(pl.multiple_of(row * BM, BM), BM), pl.ds(pl.multiple_of(lax.rem(v, j.tiles) * BN, BN), BN)]
            return Pieces(r.f_out.at[s], dst, r.fo_sem.at[s], 3)

        def job_begin(j):
            lhs_copy(j, jnp.int32(0)).start()
            rhs_copy(j, jnp.int32(0)).start()

        def fill(n):
            while n > 0 and jobs:
                j = jobs[0]
                rhs_all = j.blocks * j.tiles
                count = rhs_all * j.sub

                def unit(u, carry):
                    v, b, s = lax.div(u, j.sub), lax.rem(u, j.sub), lax.rem(u, TWO)
                    vs, t = lax.rem(v, TWO), lax.rem(v, j.tiles)
                    k = lax.div(v, j.tiles) * j.sub + b

                    @pl.when(t == 0)
                    def _():
                        lhs_copy(j, k).wait()
                        for i in range(TOK // KT):
                            r.f_at[b, :, i * KT : (i + 1) * KT] = r.f_lhs[i * KT : (i + 1) * KT, :].T

                        @pl.when(k + 1 < j.blocks * j.sub)
                        def _():
                            lhs_copy(j, k + 1).start()

                    @pl.when(b == 0)
                    def _():
                        rhs_copy(j, v).wait()

                        @pl.when(v + 1 < rhs_all)
                        def _():
                            rhs_copy(j, v + 1).start()

                    @pl.when(u >= TWO)
                    def _():
                        put_copy(j, u - TWO).wait()

                    r.f_out[s] = dims(r.f_at[b], r.f_rhs[vs], 1, 0).astype(BF)
                    put_copy(j, u).start()
                    return carry

                upto = min(count, j.done + n)
                n -= upto - j.done
                lax.fori_loop(j.done, upto, unit, 0)
                j.done = upto
                if upto == count:
                    for u in (count - TWO, count - 1):
                        put_copy(j, jnp.int32(u)).wait()
                    jobs.pop(0)
                    if jobs:
                        job_begin(jobs[0])

        steps = list(plan)

        def fill_next():
            if steps:
                fill(steps.pop(0))

        say_here((core, px, py))
        if rs:
            lhs_load(0)
            w1_load()
            lhs_load(1)
        if kind == TOP:
            srcs = [begin(r.src.at[h], r.g.at[h], r.g_sem.at[h]) for h in HALVES]
        loads = norm_load(A)
        if ag:
            w2_copy = begin(r.wb.at[ag[1]], r.w2, r.w2_sem, PEERS)
        if jobs:
            job_begin(jobs[0])
        for j in range(n_acc):
            r.acc[j] = jnp.zeros((SUBL, D), F32)
        if ag and what == DACT:
            r.bacc[...] = jnp.zeros((SUBL, n2), F32)

        def both_halves():
            for i in range(len(PAIRS)):
                step(i)
            merge(A, OWN)
            third_sends(A)
            for i in range(len(PAIRS), len(seq)):
                step(i)
            merge(B, OWN)
            fill_next()
            rs_done(A)
            norm_half(A, loads)

        def products(h):
            cross(h)
            fill_next()
            ready(h, XN)
            ready(h, YN)
            product(h, XN)
            product(h, YN)
            fill_next()
            cross_far(h)

        if kind == FIRST:
            norm_half(A, loads)
            loads = norm_load(B)
            await_peers()
            own_sends(A)
            norm_half(B, loads)
            product(A, OWN)
            forward(A)
            own_sends(B)
            ready(B, OWN)
            product(B, OWN)
            products(A)
            product(A, FAR)
            forward(B)
            products(B)
            product(B, FAR)
        elif kind == LAST:
            both_halves()
            loads = norm_load(B)
            fill_next()
            third_sends(B)
            fill(ALL)
            rs_done(B)
            norm_half(B, loads)
        elif kind == MID:
            both_halves()
            loads = norm_load(B)
            fill_next()
            third_sends(B)
            own_sends(A)
            fill_next()
            product(A, OWN)
            fill_next()
            rs_done(B)
            norm_half(B, loads)
            fill_next()
            forward(A)
            own_sends(B)
            fill_next()
            product(B, OWN)
            fill_next()
            products(A)
            fill(ALL)
            product(A, FAR)
            forward(B)
            products(B)
            product(B, FAR)
        elif kind == TOP:
            for c in srcs:
                c.wait()
            product_in(0, send=False)
            own_sends(A)
            for i in range(1, len(PAIRS)):
                step(i, False)
            forward(A)
            own_sends(B)
            merge(A, OWN)
            product(A, OWN)
            ready(B, OWN)
            cross(A)
            product(B, OWN)
            ready(A, XN)
            ready(A, YN)
            product(A, XN)
            product(A, YN)
            forward(B)
            cross_far(A)
            for n in range(tiles1):
                far_sends(n)
            first_sends(A, XN)
            first_sends(A, YN)
            product_in(4)
            product(A, FAR)
            cross(B)
            step(5, False)
            ready(B, XN)
            ready(B, YN)
            product(B, XN)
            cross_far(B)
            product(B, YN)
            third_sends(A)
            first_sends(B, FAR)
            merge(B, XN)
            first_sends(B, XN)
            product_in(6)
            merge(B, YN)
            first_sends(B, YN)
            product_in(7)
            merge(B, OWN)
            rs_done(A)
            norm_half(A, loads)
            loads = norm_load(B)
            product(B, FAR)
            third_sends(B)
            rs_done(B)
            norm_half(B, loads)

        for j in range(n_acc):
            r.vo[pl.ds(j, 1), :] = jnp.sum(r.acc[j], axis=0, keepdims=True)
        if n_acc:
            r.vo[n_acc:, :] = jnp.zeros((SUBL - n_acc, D), F32)
        if ag and what == DACT:
            r.bup[...] = jnp.sum(r.bacc[...], axis=0, keepdims=True)
        for c in out_copy:
            c.wait()
        if rs:
            for (h, j), c in rs_copy.items():
                if h == B or j > OWN + YN + 1:
                    c.wait_send()
            for (n, j), c in far_copy.items():
                if j:
                    c.wait_send()
        if ag:
            for c in ag_copy.values():
                c.wait_send()
            for cs in res_out.values():
                for c in cs:
                    c.wait()
            for c in last_copy:
                c.wait()

    return call(name, cid, body, ins, outs, sc, ("vec", "b_up", "vo", "bup"))


def positions(me):
    def pos(axis):
        i = lax.broadcasted_iota(jnp.int32, (ROWS, ROWS), axis)
        return lax.bitwise_xor(lax.div(i, GROUP), me) * GROUP + lax.rem(i, GROUP)

    return pos(0), pos(1)


def heads_of(x, part, h):
    at = part * INNER + h * HD
    return x[:, at : at + HD]


def softmax(s):
    e = jnp.exp(s - jnp.max(s, axis=-1, keepdims=True))
    return e * (ONE / jnp.sum(e, axis=-1, keepdims=True))


def attn_fwd_kernel(group, info, qkv, ctx, s_ref, p_ref):
    row, col = positions(info[ALL_SEQS])
    for first in range(0, SEQS, group):
        some = [(i, h) for i in range(first, first + group) for h in range(HEADS)]
        xs = {i: qkv[:, i].reshape(ROWS, QKV_N) for i, _ in some}
        for n, (i, h) in enumerate(some):
            mask = (col <= row) & (col < info[pl.program_id(0) * SEQS + i])
            score = dims(heads_of(xs[i], 0, h), heads_of(xs[i], 1, h), 1, 1) * HD**-HALF
            s_ref[n] = jnp.where(mask, score, NEG)
        p_ref[...] = softmax(s_ref[...]).astype(BF)
        out = {i: [] for i in xs}
        for n, (i, h) in enumerate(some):
            out[i].append(dims(p_ref[n], heads_of(xs[i], TWO, h), 1, 0).astype(BF))
        for i, parts in out.items():
            ctx[:, i] = jnp.concatenate(parts, axis=-1).reshape(PEERS, GROUP, INNER)


def attn_bwd_steps(group, info, qkv, dctx, out, s_ref, dp_ref, p_ref, ds_ref):
    row, col = positions(info[ALL_SEQS])
    for first in range(0, SEQS, group):
        some = [(i, h) for i in range(first, first + group) for h in range(HEADS)]
        xs = {i: (qkv[:, i].reshape(ROWS, QKV_N), dctx[:, i].reshape(ROWS, INNER)) for i, _ in some}
        for n, (i, h) in enumerate(some):
            x, d = xs[i]
            mask = (col <= row) & (col < info[pl.program_id(0) * SEQS + i])
            score = dims(heads_of(x, 0, h), heads_of(x, 1, h), 1, 1) * HD**-HALF
            s_ref[n] = jnp.where(mask, score, NEG)
            dp_ref[n] = dims(heads_of(d, 0, h), heads_of(x, TWO, h), 1, 1).astype(BF)
        p = softmax(s_ref[...])
        dp = dp_ref[...].astype(F32)
        p_ref[...] = p.astype(BF)
        ds = p * (dp - jnp.sum(dp * p, axis=-1, keepdims=True))
        ds_ref[...] = (ds * HD**-HALF).astype(BF)
        grads = {i: ([], [], []) for i in xs}
        for n, (i, h) in enumerate(some):
            x, d = xs[i]
            dq, dk, dv = grads[i]
            dq.append(dims(ds_ref[n], heads_of(x, 1, h), 1, 0).astype(BF))
            dk.append(dims(ds_ref[n], heads_of(x, 0, h), 0, 0).astype(BF))
            dv.append(dims(p_ref[n], heads_of(d, 0, h), 0, 0).astype(BF))
        for i, parts in grads.items():
            out[:, i] = jnp.concatenate(sum(parts, []), axis=-1).reshape(PEERS, GROUP, QKV_N)


def seq_spec(n):
    per_half = PEERS // SEQS
    return pl.BlockSpec((None, PEERS, SEQS, GROUP, n), lambda i, info: (lax.div(i, per_half), 0, lax.rem(i, per_half), 0, 0))


def by_seq(a):
    return a.reshape(TWO, PEERS, PEERS, GROUP, a.shape[-1])


def seq_shape(n):
    return jax.ShapeDtypeStruct((TWO, PEERS, PEERS, GROUP, n), BF)


def attn_tiles(group, *types):
    return [pltpu.VMEM((group * HEADS, ROWS, ROWS), t) for t in types]


def attn_fwd(info, qkv, group):
    grid_spec = pltpu.PrefetchScalarGridSpec(
        num_scalar_prefetch=1, grid=(ALL_SEQS // SEQS,), in_specs=[seq_spec(QKV_N)], out_specs=seq_spec(INNER), scratch_shapes=attn_tiles(group, F32, BF)
    )
    out = pl.pallas_call(partial(attn_fwd_kernel, group), name="attn_fwd", out_shape=seq_shape(INNER), grid_spec=grid_spec)(info, by_seq(qkv))
    return out.reshape(TWO, PEERS, ROWS, INNER)


def stacking(puts, stacks, n):
    used = sorted({p[1] for p in puts})
    shapes = [jax.ShapeDtypeStruct((n,) + next(p[0].shape for p in puts if p[1] == k), BF) for k in used]
    given = [k for k in used if stacks[k] is not None]
    return used, shapes, given


def attn_bwd(info, qkv, dctx, puts, stacks, n, group):
    used, shapes, given = stacking(puts, stacks, n)
    m = len(puts)

    def kernel(info, qkv, dctx, *refs):
        grads, refs = refs[:m], refs[m + len(given) :]
        out, outs, refs = refs[0], refs[1 : 1 + len(used)], refs[1 + len(used) :]
        bounce, load_sem, put_sem, tiles = refs[:m], refs[m], refs[m + 1], refs[m + TWO :]
        step = pl.program_id(0)

        def load(i):
            return Pieces(grads[i], bounce[i], load_sem.at[i], PEERS)

        def put(i):
            return Pieces(bounce[i], outs[used.index(puts[i][1])].at[puts[i][TWO]], put_sem.at[i], PEERS)

        @pl.when(step == 0)
        def _():
            for i in range(m):
                load(i).start()

        for at, some in ((1, range(m // TWO)), (TWO, range(m // TWO, m))):

            @pl.when(step == at)
            def _(some=some):
                for i in some:
                    load(i).wait()
                    put(i).start()

        attn_bwd_steps(group, info, qkv, dctx, out, *tiles)

        @pl.when(step == ALL_SEQS // SEQS - 1)
        def _():
            for i in range(m):
                put(i).wait()

    hbm = pl.BlockSpec(memory_space=ANY)
    dma = pltpu.SemaphoreType.DMA
    grid_spec = pltpu.PrefetchScalarGridSpec(
        num_scalar_prefetch=1,
        grid=(ALL_SEQS // SEQS,),
        in_specs=[seq_spec(QKV_N), seq_spec(INNER)] + [hbm] * (m + len(given)),
        out_specs=[seq_spec(QKV_N)] + [hbm] * len(used),
        scratch_shapes=[pltpu.VMEM(p[0].shape, BF) for p in puts] + [dma((m,)), dma((m,))] + attn_tiles(group, F32, BF, BF, BF),
    )
    res = pl.pallas_call(
        kernel,
        name="attn_bwd",
        out_shape=[seq_shape(QKV_N)] + shapes,
        grid_spec=grid_spec,
        input_output_aliases={3 + m + j: 1 + used.index(k) for j, k in enumerate(given)},
        compiler_params=pltpu.CompilerParams(vmem_limit_bytes=VMEM_LIMIT),
    )(info, by_seq(qkv), by_seq(dctx), *[p[0] for p in puts], *[stacks[k] for k in given])
    for k, a in zip(used, res[1:]):
        stacks[k] = a
    return res[0].reshape(TWO, PEERS, ROWS, QKV_N)


def put_last(puts, stacks):
    m = len(puts)

    def kernel(*refs):
        grads, outs, refs = refs[:m], refs[m + m : m + m + m], refs[m + m + m :]
        bounce, load_sem, put_sem = refs[:m], refs[m], refs[m + 1]
        loads = [Pieces(grads[i], bounce[i], load_sem.at[i], PEERS).start() for i in range(m)]
        stores = []
        for i in range(m):
            loads[i].wait()
            stores.append(Pieces(bounce[i], outs[i].at[puts[i][TWO]], put_sem.at[i], PEERS).start())
        for c in stores:
            c.wait()

    hbm = pl.BlockSpec(memory_space=ANY)
    dma = pltpu.SemaphoreType.DMA
    olds = [stacks[p[1]] for p in puts]
    res = pl.pallas_call(
        kernel,
        name="put_last",
        out_shape=[jax.ShapeDtypeStruct(a.shape, a.dtype) for a in olds],
        in_specs=[hbm] * (m + m),
        out_specs=[hbm] * m,
        scratch_shapes=[pltpu.VMEM(p[0].shape, BF) for p in puts] + [dma((m,)), dma((m,))],
        input_output_aliases={m + i: i for i in range(m)},
        compiler_params=pltpu.CompilerParams(vmem_limit_bytes=VMEM_LIMIT),
    )(*[p[0] for p in puts], *olds)
    for p, a in zip(puts, res):
        stacks[p[1]] = a


def sum_rows(parts, cid):
    n, half = len(parts), D // TWO
    per = 6
    rows = -(-per * n // SUBL) * SUBL
    ins = SimpleNamespace()
    for l, (a, b) in enumerate(parts):
        setattr(ins, f"a{l}", a)
        setattr(ins, f"b{l}", b)

    def body(r):
        core, px, py = peers()
        say_here((core, px, py))
        odd = lax.rem(lax.axis_index(TP), TWO)
        mine = pl.ds(pl.multiple_of(odd * half, half), half)
        for l in range(n):
            at = per * l
            r.v[at : at + TWO, :] = getattr(r, f"a{l}")[:TWO, :]
            r.v[at + TWO : at + per, :] = getattr(r, f"b{l}")[: per - TWO, :]
        if rows > per * n:
            r.v[per * n :, :] = jnp.zeros((rows - per * n, D), F32)
        await_peers()

        def send(src, dst, i, dev):
            c = remote(src, dst, r.send.at[i], r.recv.at[i], dev)
            c.start()
            return c

        send(r.v, r.a, 0, core).wait()
        r.s[0] = r.v[:, mine] + r.a[:, mine]
        for i, dev in enumerate((px, py)):
            send(r.s.at[i], r.b.at[i], 1 + i, dev).wait()
            r.s[i + 1] = r.s[i] + r.b[i]
        c = send(r.s.at[TWO], r.t.at[:, mine], 3, core)
        r.u[:, mine] = r.s[TWO]
        c.wait()
        first = lax.broadcasted_iota(jnp.int32, (1, D), 1) < half
        keep = first == (odd == 0)
        for l in range(n):
            at = slice(per * l, per * (l + 1))
            r.o[l] = jnp.where(keep, r.u[at, :], r.t[at, :])

    dma = pltpu.SemaphoreType.DMA
    whole, part = pltpu.VMEM((rows, D), F32), (rows, half)
    scratch = SimpleNamespace(v=whole, a=whole, t=whole, u=whole, s=pltpu.VMEM((3,) + part, F32), b=pltpu.VMEM((TWO,) + part, F32), send=dma((4,)), recv=dma((4,)))
    outs = SimpleNamespace(o=jax.ShapeDtypeStruct((n, per, D), F32))
    return call("sum_rows", cid, body, ins, outs, scratch, list(vars(ins)) + ["o"]).o


def group_body(x_loc, dy_loc, len_loc, wqkv, wout, wup, bup, wdown, vec):
    n = wqkv.shape[0]
    ids = iter(range(ROWS))
    shape = x_loc.shape
    x = x_loc.reshape(TWO, ROWS, D)
    dy = dy_loc.reshape(TWO, ROWS, D)
    wq = jnp.transpose(wqkv, (0, 2, 3, 4, 1)).reshape(n, QKV_N, D)
    wo = wout.reshape(n, INNER, D)
    info = jnp.concatenate([len_loc, lax.axis_index(TP).reshape(1).astype(jnp.int32)])

    def flat(a):
        return a.reshape(TOK, a.shape[-1])

    def row(layer, i, bias=None):
        return SimpleNamespace(gain=(layer, i), shift=(layer, i + 1), bias=bias)

    ln2, bias1, bias2 = TWO, 4, 5
    groups = (TWO, 1, 4)
    saved = [SimpleNamespace() for _ in range(n)]
    r = fused("first", next(ids), FIRST, N_FIRST, dict(in0=x, wb=wq, vec=vec), row(0, 0), ag=(QKV, 0))
    s = saved[0]
    s.x, s.a, s.qkv = x, r.full, r.res
    for l in range(n):
        s = saved[l]
        s.ctx = attn_fwd(info, s.qkv, groups[l])
        arrays = dict(lhs1=s.ctx, wa=wo, wb=wup, in0=s.x, vec=vec, b_up=bup)
        r = fused(f"mlp_in_{l}", next(ids), MID, N_LN, arrays, row(l, ln2, (l, bias1)), rs=(l, INNER, False), ag=(UP, l))
        s.hid, s.m, s.act, s.pre = r.out0, r.full, r.res, r.pre
        if l + 1 < n:
            arrays = dict(lhs1=s.act, wa=wdown, wb=wq, in0=s.hid, vec=vec)
            r = fused(f"attn_in_{l + 1}", next(ids), MID, N_LN, arrays, row(l + 1, 0, (l, bias2)), rs=(l, FF, False), ag=(QKV, l + 1))
            s = saved[l + 1]
            s.x, s.a, s.qkv = r.out0, r.full, r.res
    s = saved[n - 1]
    arrays = dict(lhs1=s.act, wa=wdown, wb=wdown, in0=s.hid, vec=vec, src=dy, pre=s.pre)
    r = fused("top", next(ids), TOP, N_RES, arrays, row(0, 0, (n - 1, bias2)), rs=(n - 1, FF, False), ag=(DACT, n - 1))
    y, d_cur, d_full, d_pre = r.out0, r.out1, r.full, r.res
    g_bup, rows, puts, stacks = [r.bup], [], [], [None] * 4
    mlp_plans = ((10, 5, 0, 15, 5, 0, 6, 1, 5), (6, 3, 0, 10, 3, 0, 4, 1, 4), (8, 4, 0, 13, 4, 0, 5, 1, 5))
    attn_plans = ((6, 4), (4, 3, 0, 6, 2, 0, 1, 1, 2), (6, 4, 0, 8, 3, 0, 1, 1))
    groups = (4, TWO, 1)
    for l in reversed(range(n)):
        s = saved[l]
        arrays = dict(lhs1=d_pre, wa=wup, wb=wo, in0=s.hid, in1=d_cur, vec=vec, f0l=flat(s.act), f0r=flat(d_full), f1l=flat(s.m), f1r=flat(d_pre))
        fills = ((FF, D, 4), (D, FF, 4))
        r = fused(f"d_mlp_{l}", next(ids), MID, N_BWD2, arrays, row(l, ln2), rs=(l, FF, True), ag=(DCTX, l), fills=fills, plan=mlp_plans[l])
        d_hid, d_attn, v3 = r.out0, r.full, r.vo
        puts += [(r.g0, 3, l), (r.g1, 2, l)]
        d_qkv = attn_bwd(info, s.qkv, r.res, puts, stacks, n, groups[l])
        arrays = dict(lhs1=d_qkv, wa=wq, in0=s.x, in1=d_hid, vec=vec, f0l=flat(s.ctx), f0r=flat(d_attn), f1l=flat(d_qkv), f1r=flat(s.a))
        common = dict(rs=(l, QKV_N, False), fills=((INNER, D, 1), (QKV_N, D, 3)), plan=attn_plans[l])
        if l:
            arrays.update(wb=wdown, pre=saved[l - 1].pre)
            r = fused(f"d_attn_{l}", next(ids), MID, N_BWD1, arrays, row(l, 0), ag=(DACT, l - 1), **common)
            g_bup.append(r.bup)
            d_full, d_pre = r.full, r.res
        else:
            r = fused(f"d_attn_{l}", next(ids), LAST, N_BWD1, arrays, row(l, 0), **common)
        puts = [(r.g0, 1, l), (r.g1, 0, l)]
        rows.append((r.vo, v3))
        d_cur = r.out0
    put_last(puts, stacks)
    g_vec = sum_rows(rows[::-1], next(ids))
    g_qkv = jnp.transpose(stacks[0].reshape(n, 3, HEADS, HD, D), (0, 4, 1, 2, 3))
    g_out = stacks[1].reshape(n, HEADS, HD, D)
    return y.reshape(shape), d_cur.reshape(shape), g_qkv, g_out, stacks[2], jnp.concatenate(g_bup[::-1]), stacks[3], g_vec


def solution(mesh):
    act_spec = P(DP, TP, None)
    in_specs = (act_spec, act_spec, P(DP), P(None, None, None, TP, None), P(None, TP, None, None), P(None, None, TP), P(None, TP), P(None, TP, None), P())
    out_specs = (act_spec, act_spec, P(DP, None, None, TP, None), P(DP, TP, None, None), P(DP, None, TP), P(DP, TP), P(DP, TP, None), P(DP, None, None))
    return jax.shard_map(group_body, mesh=mesh, in_specs=in_specs, out_specs=out_specs, check_vma=False)
```

```python
from functools import partial
from types import SimpleNamespace

import jax
import jax.numpy as jnp
from jax import lax
from jax.experimental import pallas as pl
from jax.experimental.pallas import tpu as pltpu
from jax.sharding import PartitionSpec as P

TP, DP = "tp", "dp"
D, FF, INNER, QKV_N = 3072, 1536, 384, 1152
ROWS, HALF_ROWS, GROUP = 128, 64, 16
LANES, SUBL = 128, 8
A, B = HALVES = range(2)
PEERS = 8
TOK = len(HALVES) * PEERS * ROWS
HEADS, HD = 4, 96
SEQS, ALL_SEQS = 4, 16
BM, BN, KT = 384, 512, 256
BF, F32 = jnp.bfloat16, jnp.float32
ANY = pl.ANY
VMEM_LIMIT = 66_900_000
GELU_C, GELU_D = 0.7978845608028654, 0.044715
EPS, NEG = 1e-5, -1e30
ONE, TWO, HALF = 1.0, 2, 0.5
OWN, XN, YN, FAR = PAIRS = range(4)
Q_ORDER = (FAR, XN, YN, OWN)
R_X, R_Y, R_FAR = 2, 4, 6
X_FAR, Y_FAR, X_RAW, Y_RAW, X_SUM, Y_SUM, N_RS = range(4, 11)
G_CORE, G_XT, G_XB, G_YB, G_YT, G_FT, G_FB, G_C3, G_C5, G_C7, N_AG = range(11)
CROSSING = {XN: G_C3, YN: G_C5, FAR: G_C7}
FIRST, MID, TOP, LAST = range(4)
N_FIRST, N_LN, N_RES, N_BWD2, N_BWD1 = range(5)
QKV, UP, DACT, DCTX = range(4)
WIDTH = (QKV_N, FF, FF, INNER)
ALL = 1 << 20


def dims(lhs, rhs, lc, rc):
    return lax.dot_general(lhs, rhs, (((lc,), (rc,)), ((), ())), preferred_element_type=F32)


def peers():
    me = lax.axis_index(TP)
    dp = lax.axis_index(DP)

    def flip(bit):
        return me + bit - TWO * bit * lax.rem(lax.div(me, bit), TWO)

    return [(dp, flip(1 << k)) for k in range(3)]


def say_here(devices):
    for dev in devices:
        pl.semaphore_signal(pltpu.get_barrier_semaphore(), inc=1, device_id=dev, device_id_type=pl.DeviceIdType.MESH)


def await_peers(n=3):
    pl.semaphore_wait(pltpu.get_barrier_semaphore(), n)


def remote(src, dst, send, recv, dev):
    return pltpu.make_async_remote_copy(src_ref=src, dst_ref=dst, send_sem=send, recv_sem=recv, device_id=dev, device_id_type=pl.DeviceIdType.MESH)


class Pieces:
    def __init__(self, src, dst, sem, n):
        self.src, self.dst, self.sem, self.n = src, dst, sem, n

    def start(self):
        src, dst = self.src, self.dst
        step = src.shape[-2] // self.n
        for i in range(self.n):
            at = pl.ds(i * step, step)
            if len(src.shape) == 3:
                for j in range(src.shape[0]):
                    pltpu.make_async_copy(src.at[j, at], dst.at[j, at], self.sem).start()
            else:
                pltpu.make_async_copy(src.at[at], dst.at[at], self.sem).start()
        return self

    def wait(self):
        pltpu.make_async_copy(self.src, self.dst, self.sem).wait()


def call(name, cid, body, ins, outs, scratch, small):
    names = [list(vars(a)) for a in (ins, outs, scratch)]

    def kernel(*refs):
        body(SimpleNamespace(**dict(zip(sum(names, []), refs))))

    def spec(n):
        return pl.BlockSpec(memory_space=pltpu.VMEM if n in small else ANY)

    res = pl.pallas_call(
        kernel,
        name=name,
        out_shape=list(vars(outs).values()),
        in_specs=[spec(n) for n in names[0]],
        out_specs=[spec(n) for n in names[1]],
        scratch_shapes=list(vars(scratch).values()),
        compiler_params=pltpu.CompilerParams(vmem_limit_bytes=VMEM_LIMIT, collective_id=cid, has_side_effects=True),
    )(*vars(ins).values())
    return SimpleNamespace(**dict(zip(names[1], res)))


def fused(name, cid, kind, norm, arrays, vec, rs=None, ag=None, fills=(), bm=BM, flat_t=False, plan=()):
    ins, outs, sc = SimpleNamespace(**arrays), SimpleNamespace(), SimpleNamespace()
    dma = pltpu.SemaphoreType.DMA
    n_in = len([k for k in arrays if k in ("in0", "in1")])
    n_acc = {N_BWD2: 4, N_BWD1: TWO}.get(norm, 0)
    shard = jax.ShapeDtypeStruct((TWO, ROWS, D), F32)
    if norm != N_FIRST:
        outs.out0 = shard
        sc.nout = pltpu.VMEM((ROWS, D), F32)
    if norm == N_RES:
        outs.out1 = shard
        sc.nout1 = pltpu.VMEM((ROWS, D), F32)
    sc.nin = pltpu.VMEM((n_in, ROWS, D), F32)
    sc.nsem = dma((n_in + TWO,))
    if n_acc:
        outs.vo = jax.ShapeDtypeStruct((SUBL, D), F32)
        sc.acc = pltpu.VMEM((n_acc, SUBL, D), F32)
    if rs:
        k1 = rs[1]
        tile1 = 1024
        tiles1 = D // tile1
        halves = (TWO, ROWS, D)
        sc.w1 = pltpu.VMEM((D, k1) if rs[2] else (k1, D), BF)
        sc.lhs = pltpu.VMEM((TWO, TWO, ROWS, k1), BF)
        sc.own = pltpu.VMEM((TWO, len(PAIRS), ROWS, D), BF)
        sc.snd = pltpu.VMEM((len(PAIRS), ROWS, D), BF)
        sc.drx = pltpu.VMEM((TWO, len(PAIRS), ROWS, D), BF)
        sc.hx = pltpu.VMEM((TWO, HALF_ROWS, D), BF)
        sc.hy = pltpu.VMEM((TWO, HALF_ROWS, D), BF)
        sc.rx = pltpu.VMEM(halves, BF)
        sc.ry = pltpu.VMEM(halves, BF)
        sc.w1_sem = dma((tiles1,))
        sc.lhs_sem = dma((TWO,))
        sc.rs_send = dma((TWO, N_RS))
        sc.rs_recv = dma((TWO, N_RS))
        sc.far_send = dma((tiles1, len(PAIRS)))
        sc.far_recv = dma((tiles1, len(PAIRS)))
    if ag:
        what = ag[0]
        n2 = WIDTH[what]
        outs.full = jax.ShapeDtypeStruct((TWO, PEERS, ROWS, D), BF)
        outs.res = jax.ShapeDtypeStruct((TWO, PEERS, ROWS, n2), BF)
        pairs_of = (TWO, TWO, ROWS, n2)
        sc.w2 = pltpu.VMEM((D, n2) if what == UP else (n2, D), BF)
        sc.g = pltpu.VMEM((TWO, ROWS, D), BF)
        sc.agin = pltpu.VMEM((TWO, TWO, ROWS, D), BF)
        sc.last = pltpu.VMEM((TWO, ROWS, D), BF)
        sc.w2_sem = dma
        sc.g_sem = dma((TWO,))
        sc.agin_sem = dma((TWO,))
        sc.last_sem = dma((TWO,))
        sc.ag_send = dma((TWO, N_AG))
        sc.ag_recv = dma((TWO, N_AG))
        sc.res_st = pltpu.VMEM(pairs_of, BF)
        sc.res_sem = dma((TWO,))
        if what == UP:
            outs.slope = jax.ShapeDtypeStruct((TWO, PEERS, ROWS, n2), F32)
            outs.full_t = jax.ShapeDtypeStruct((D, TOK), BF)
            outs.res_t = jax.ShapeDtypeStruct((n2, TOK), BF)
            sc.full_ts = pltpu.VMEM((D, KT), BF)
            sc.res_ts = pltpu.VMEM((n2, KT), BF)
            sc.t_sem = dma((TWO,))
        if what == DACT:
            outs.bup = jax.ShapeDtypeStruct((1, n2), F32)
            sc.bacc = pltpu.VMEM((SUBL, n2), F32)
        if what in (UP, DACT):
            sc.slope_st = pltpu.VMEM(pairs_of, F32)
            sc.slope_sem = dma((TWO,))
    if fills:
        slots = TWO if flat_t else max(f[2] for f in fills)
        sc.f_at = pltpu.VMEM((slots, bm, TOK), BF)
        sc.f_rhs = pltpu.VMEM((TWO, TOK, BN), BF)
        sc.f_out = pltpu.VMEM((TWO, bm, BN), BF)
        if not flat_t:
            sc.f_lhs = pltpu.VMEM((TOK, bm), BF)
        sc.fl_sem = dma((slots,))
        sc.fr_sem = dma((TWO,))
        sc.fo_sem = dma((TWO,))
        outs.g0 = jax.ShapeDtypeStruct(fills[0][:2], BF)
        outs.g1 = jax.ShapeDtypeStruct(fills[1][:2], BF)

    def body(r):
        core, px, py = peers()

        def begin(src, dst, sem, n=4):
            return Pieces(src, dst, sem, n).start()

        def norm_load(h):
            some = (r.in0, r.in1) if n_in == TWO else (r.in0,)
            return [begin(x.at[h], r.nin.at[i], r.nsem.at[i]) for i, x in enumerate(some)]

        def vrow(row):
            return r.vec[row[0], pl.ds(row[1], 1), :]

        out_copy = []

        def mean(x):
            return jnp.sum(x, axis=-1, keepdims=True) * (ONE / D)

        def norm_half(h, loads):
            for c in loads:
                c.wait()
            while out_copy:
                out_copy.pop().wait()

            def rows(i, carry):
                at = pl.ds(pl.multiple_of(i * GROUP, GROUP), GROUP)
                x = r.nin[0, at, :]
                if rs:
                    o = r.own[h, OWN, at, :].astype(F32) + r.rx[h, at, :].astype(F32) + r.ry[h, at, :].astype(F32)
                    o = o.astype(BF).astype(F32)
                if norm in (N_LN, N_RES):
                    x = x + o + vrow(vec.bias)
                    r.nout[at, :] = x
                if norm == N_RES:
                    r.nout1[at, :] = r.g[h, at, :].astype(F32)
                    return carry
                cen = x - mean(x)
                rstd = lax.rsqrt(mean(cen * cen) + EPS)
                if norm in (N_FIRST, N_LN):
                    r.g[h, at, :] = (cen * rstd * vrow(vec.gain) + vrow(vec.shift)).astype(BF)
                    return carry
                xh = cen * rstd
                dxh = o * vrow(vec.gain)
                base = r.nin[1, at, :]
                res = base + rstd * (dxh - mean(dxh) - xh * mean(dxh * xh))
                r.nout[at, :] = res
                if ag:
                    r.g[h, at, :] = res.astype(BF)
                sums = [o * xh, o] + ([res, base] if norm == N_BWD2 else [])
                for j, v in enumerate(sums):
                    r.acc[j] += v[:SUBL] + v[SUBL:]
                return carry

            lax.fori_loop(0, ROWS // GROUP, rows, 0)
            if norm != N_FIRST:
                out_copy.append(begin(r.nout, r.out0.at[h], r.nsem.at[n_in]))
            if norm == N_RES:
                out_copy.append(begin(r.nout1, r.out1.at[h], r.nsem.at[n_in + 1]))

        top, bot = pl.ds(0, HALF_ROWS), pl.ds(HALF_ROWS, HALF_ROWS)
        if rs:
            seq = [(h, q) for h in HALVES for q in Q_ORDER]
            lhs_loads, rs_copy, far_copy, w1_loads = {}, {}, {}, []
            own = r.own

            def w1_load():
                for n in range(tiles1):
                    at = pl.ds(n * tile1, tile1)
                    src, dst = r.wa.at[rs[0]], r.w1
                    src, dst = (src.at[at], dst.at[at]) if rs[2] else (src.at[:, at], dst.at[:, at])
                    w1_loads.append(begin(src, dst, r.w1_sem.at[n]))

            def lhs_load(i):
                h, q = seq[i]
                s = i % TWO
                lhs_loads[i] = begin(r.lhs1.at[h, pl.ds(TWO * q, TWO)], r.lhs.at[s], r.lhs_sem.at[s])

            def rs_start(h, j, src, dst, dev):
                c = remote(src, dst, r.rs_send.at[h, j], r.rs_recv.at[h, j], dev)
                c.start()
                rs_copy[h, j] = c

            def far_start(n, j, src, dst, dev):
                c = remote(src, dst, r.far_send.at[n, j], r.far_recv.at[n, j], dev)
                c.start()
                far_copy[n, j] = c

            def add_into(dst, src, n, at_cols=slice(None)):
                def rows(i, carry):
                    at = pl.ds(pl.multiple_of(i * GROUP, GROUP), GROUP)
                    dst[at, at_cols] = (dst[at, at_cols].astype(F32) + src[at, at_cols].astype(F32)).astype(BF)
                    return carry

                lax.fori_loop(0, n // GROUP, rows, 0)

            def far_merge(n, send):
                cols = pl.ds(n * tile1, tile1)
                far_copy[n, 0].wait_recv()
                add_into(own.at[A, FAR], r.drx.at[A, FAR], ROWS, cols)
                if send:
                    far_sends(n)

            def far_sends(n):
                cols = pl.ds(n * tile1, tile1)
                far_start(n, 1, own.at[A, FAR, top, cols], r.hx.at[A, :, cols], px)
                far_start(n, 2, own.at[A, FAR, bot, cols], r.hy.at[A, :, cols], py)

            def product_in(i, between=None, send=True):
                h, q = seq[i]
                s = i % TWO
                lhs_loads[i].wait()
                if i == len(PAIRS):
                    for n in range(tiles1):
                        far_copy[n, 0].wait_send()
                elif h == B:
                    rs_copy[A, q].wait_send()

                def tile(n, carry):
                    at = pl.ds(pl.multiple_of(n * tile1, tile1), tile1)
                    x = r.lhs[s].reshape(TWO * ROWS, k1)
                    y = dims(x, r.w1[at, :], 1, 1) if rs[2] else dims(x, r.w1[:, at], 1, 0)
                    y = y.astype(BF)
                    own[h, q, :, at] = y[:ROWS]
                    r.snd[q, :, at] = y[ROWS:]
                    return carry

                if i == 0:
                    for n in range(tiles1):
                        cols = pl.ds(n * tile1, tile1)
                        w1_loads[n].wait()
                        tile(n, 0)
                        if n == 0:
                            await_peers()
                        far_start(n, 0, r.snd.at[FAR, :, cols], r.drx.at[A, FAR, :, cols], core)
                        if n:
                            far_merge(n - 1, send)
                else:
                    tile(0, 0)
                    if between:
                        between()
                    lax.fori_loop(1, tiles1, tile, 0)
                if i + TWO < len(seq):
                    lhs_load(i + TWO)
                if i:
                    rs_start(h, q, r.snd.at[q], r.drx.at[h, q], core)

            def merge(h, q):
                rs_copy[h, q].wait_recv()
                add_into(own.at[h, q], r.drx.at[h, q], ROWS)

            def first_sends(h, q):
                if q == FAR:
                    rs_start(h, X_FAR, own.at[h, q, top], r.hx.at[h], px)
                    rs_start(h, Y_FAR, own.at[h, q, bot], r.hy.at[h], py)
                if q == XN:
                    rs_start(h, X_RAW, own.at[h, q, top], r.rx.at[h, top], px)
                if q == YN:
                    rs_start(h, Y_RAW, own.at[h, q, bot], r.ry.at[h, bot], py)

            def far_wait(h, j):
                if h == A:
                    for n in range(tiles1):
                        far_copy[n, 1 + j].wait_recv()
                else:
                    rs_copy[h, X_FAR + j].wait_recv()

            def third_sends(h):
                far_wait(h, 1)
                add_into(own.at[h, XN, bot], r.hy.at[h], HALF_ROWS)
                rs_start(h, X_SUM, own.at[h, XN, bot], r.rx.at[h, bot], px)
                far_wait(h, 0)
                add_into(own.at[h, YN, top], r.hx.at[h], HALF_ROWS)
                rs_start(h, Y_SUM, own.at[h, YN, top], r.ry.at[h, top], py)

            def rs_done(h):
                for j in (X_RAW, Y_RAW, X_SUM, Y_SUM):
                    rs_copy[h, j].wait_recv()

            def step(i, send=True):
                def between():
                    h, q = seq[i - 1]
                    if i == 1:
                        far_merge(tiles1 - 1, send)
                        return
                    merge(h, q)
                    if send:
                        first_sends(h, q)

                product_in(i, between if i % len(PAIRS) else None, send)

        if ag:
            full = r.full
            ag_copy, g_copy, ready_loads, res_out, w2_ready, last_copy = {}, {}, {}, {}, [], []

            def ag_start(h, j, src, dst, dev):
                c = remote(src, dst, r.ag_send.at[h, j], r.ag_recv.at[h, j], dev)
                c.start()
                ag_copy[h, j] = c

            def own_sends(h):
                g = r.g
                ag_start(h, G_XT, g.at[h, top], full.at[h, R_X, top], px)
                ag_start(h, G_YB, g.at[h, bot], full.at[h, R_Y, bot], py)
                ag_start(h, G_XB, g.at[h, bot], full.at[h, R_X, bot], px)
                ag_start(h, G_YT, g.at[h, top], full.at[h, R_Y, top], py)
                ag_start(h, G_CORE, g.at[h], full.at[h, 1], core)
                g_copy[h] = begin(g.at[h], full.at[h, 0], r.g_sem.at[h])

            def far_place(h, other):
                return full.at[h, R_FAR + other] if h == A else r.last.at[other]

            def forward(h):
                ag_copy[h, G_XT].wait_recv()
                ag_start(h, G_FT, full.at[h, R_X, top], far_place(h, 0).at[top], py)
                ag_copy[h, G_YB].wait_recv()
                ag_start(h, G_FB, full.at[h, R_Y, bot], far_place(h, 0).at[bot], px)

            def cross(h):
                ag_copy[h, G_XB].wait_recv()
                ag_start(h, G_C3, full.at[h, R_X], full.at[h, R_X + 1], core)
                ag_copy[h, G_YT].wait_recv()
                ag_start(h, G_C5, full.at[h, R_Y], full.at[h, R_Y + 1], core)

            def cross_far(h):
                ag_copy[h, G_FT].wait_recv()
                ag_copy[h, G_FB].wait_recv()
                ag_start(h, G_C7, far_place(h, 0), far_place(h, 1), core)
                if h == B:
                    last_copy.append(begin(r.last.at[0], full.at[h, R_FAR], r.last_sem.at[0]))

            def ready(h, q):
                s = (len(PAIRS) * h + (OWN, XN, YN, FAR).index(q)) % TWO
                pair = pl.ds(TWO * q, TWO)
                loads = []
                if what == DACT:
                    loads.append(begin(r.slope.at[h, pair], r.slope_st.at[s], r.slope_sem.at[s]))
                if q == OWN:
                    g_copy.pop(h).wait()
                    ag_copy[h, G_CORE].wait_recv()
                else:
                    ag_copy[h, CROSSING[q]].wait_recv()
                if (h, q) == (B, FAR):
                    last_copy.append(begin(r.last.at[1], full.at[h, R_FAR + 1], r.last_sem.at[1]))
                else:
                    loads.append(begin(full.at[h, pair], r.agin.at[s], r.agin_sem.at[s]))
                ready_loads[h, q] = (s, loads)

            flipped = {}

            def flip(src, stage, dst, i):
                if i in flipped:
                    flipped[i].wait()

                def block(k, carry):
                    at = pl.ds(pl.multiple_of(k * KT, KT), KT)
                    stage[at, :] = src[:, :, at].reshape(KT, KT).T
                    return carry

                lax.fori_loop(0, stage.shape[0] // KT, block, 0)
                flipped[i] = begin(stage, dst, r.t_sem.at[i])

            def product(h, q):
                if (h, q) not in ready_loads:
                    ready(h, q)
                s, loads = ready_loads.pop((h, q))
                pair = pl.ds(TWO * q, TWO)
                if not w2_ready:
                    w2_copy.wait()
                    w2_ready.append(s)
                for c in res_out.pop(s, ()):
                    c.wait()
                for c in loads:
                    c.wait()
                nt = BM if what in (QKV, DCTX) else BN

                def tile(n, carry):
                    at = pl.ds(pl.multiple_of(n * nt, nt), nt)
                    x = r.last[...] if (h, q) == (B, FAR) else r.agin[s]
                    x = x.reshape(TWO * ROWS, D)
                    y = dims(x, r.w2[:, at], 1, 0) if what == UP else dims(x, r.w2[at, :], 1, 1)
                    if what == UP:
                        u = y + r.b_up[pl.ds(ag[1], 1), at]
                        t = jnp.tanh(GELU_C * (u + GELU_D * (u * u * u)))
                        slope = HALF * (ONE + t) + (HALF * GELU_C) * u * (ONE - t * t) * (ONE + (3 * GELU_D) * (u * u))
                        r.slope_st[s, :, :, at] = slope.reshape(TWO, ROWS, nt)
                        y = u * (HALF * (ONE + t))
                    if what == DACT:
                        y = y.astype(BF).astype(F32) * r.slope_st[s, :, :, at].reshape(TWO * ROWS, nt)
                        r.bacc[:, at] += jnp.sum(y.reshape(-1, SUBL, nt), axis=0)
                    r.res_st[s, :, :, at] = y.astype(BF).reshape(TWO, ROWS, nt)
                    return carry

                if n2 == nt:
                    tile(0, 0)
                else:
                    lax.fori_loop(0, n2 // nt, tile, 0)
                res_out[s] = [begin(r.res_st.at[s], r.res.at[h, pair], r.res_sem.at[s])]
                if what == UP:
                    res_out[s].append(begin(r.slope_st.at[s], r.slope.at[h, pair], r.slope_sem.at[s]))
                    cols = pl.ds((h * PEERS + TWO * q) * ROWS, KT)
                    gathered = r.last if (h, q) == (B, FAR) else r.agin.at[s]
                    flip(gathered, r.full_ts, r.full_t.at[:, cols], 0)
                    flip(r.res_st.at[s], r.res_ts, r.res_t.at[:, cols], 1)

        jobs = []
        if fills:
            refs = ((r.f0l, r.f0r, r.g0), (r.f1l, r.f1r, r.g1))
            jobs = [SimpleNamespace(lhs=f[0], rhs=f[1], out=f[2], blocks=c[0] // bm // c[2], tiles=c[1] // BN, sub=c[2], done=0) for f, c in zip(refs, fills)]

        def lhs_copy(j, k):
            at = pl.ds(pl.multiple_of(k * bm, bm), bm)
            if flat_t:
                s = lax.rem(k, TWO)
                return Pieces(j.lhs.at[at], r.f_at.at[s], r.fl_sem.at[s], PEERS)
            return Pieces(j.lhs.at[:, at], r.f_lhs, r.fl_sem.at[0], PEERS)

        def rhs_copy(j, v):
            s = lax.rem(v, TWO)
            return Pieces(j.rhs.at[:, pl.ds(pl.multiple_of(lax.rem(v, j.tiles) * BN, BN), BN)], r.f_rhs.at[s], r.fr_sem.at[s], PEERS)

        def put_copy(j, u):
            s, v = lax.rem(u, TWO), lax.div(u, j.sub)
            row = lax.div(v, j.tiles) * j.sub + lax.rem(u, j.sub)
            dst = j.out.at[pl.ds(pl.multiple_of(row * bm, bm), bm), pl.ds(pl.multiple_of(lax.rem(v, j.tiles) * BN, BN), BN)]
            return Pieces(r.f_out.at[s], dst, r.fo_sem.at[s], 3)

        def job_begin(j):
            lhs_copy(j, jnp.int32(0)).start()
            if flat_t:
                lhs_copy(j, jnp.int32(1)).start()
            rhs_copy(j, jnp.int32(0)).start()

        def fill(n):
            while n > 0 and jobs:
                j = jobs[0]
                rhs_all = j.blocks * j.tiles
                count = rhs_all * j.sub

                def unit(u, carry):
                    v, b, s = lax.div(u, j.sub), lax.rem(u, j.sub), lax.rem(u, TWO)
                    vs, t = lax.rem(v, TWO), lax.rem(v, j.tiles)
                    k = lax.div(v, j.tiles) * j.sub + b

                    @pl.when(t == 0)
                    def _():
                        lhs_copy(j, k).wait()
                        if flat_t:
                            return
                        for i in range(TOK // KT):
                            r.f_at[b, :, i * KT : (i + 1) * KT] = r.f_lhs[i * KT : (i + 1) * KT, :].T

                        @pl.when(k + 1 < j.blocks * j.sub)
                        def _():
                            lhs_copy(j, k + 1).start()

                    @pl.when(b == 0)
                    def _():
                        rhs_copy(j, v).wait()

                        @pl.when(v + 1 < rhs_all)
                        def _():
                            rhs_copy(j, v + 1).start()

                    @pl.when(u >= TWO)
                    def _():
                        put_copy(j, u - TWO).wait()

                    r.f_out[s] = dims(r.f_at[lax.rem(k, TWO) if flat_t else b], r.f_rhs[vs], 1, 0).astype(BF)
                    put_copy(j, u).start()
                    if flat_t:

                        @pl.when((t == j.tiles - 1) & (k + TWO < j.blocks * j.sub))
                        def _():
                            lhs_copy(j, k + TWO).start()

                    return carry

                upto = min(count, j.done + n)
                n -= upto - j.done
                lax.fori_loop(j.done, upto, unit, 0)
                j.done = upto
                if upto == count:
                    for u in (count - TWO, count - 1):
                        put_copy(j, jnp.int32(u)).wait()
                    jobs.pop(0)
                    if jobs:
                        job_begin(jobs[0])

        steps = list(plan)

        def fill_next():
            if steps:
                fill(steps.pop(0))

        say_here((core, px, py))
        if rs:
            lhs_load(0)
            w1_load()
            lhs_load(1)
        if kind == TOP:
            srcs = [begin(r.src.at[h], r.g.at[h], r.g_sem.at[h]) for h in HALVES]
        loads = norm_load(A)
        if ag:
            w2_copy = begin(r.wb.at[ag[1]], r.w2, r.w2_sem, PEERS)
        if jobs:
            job_begin(jobs[0])
        for j in range(n_acc):
            r.acc[j] = jnp.zeros((SUBL, D), F32)
        if ag and what == DACT:
            r.bacc[...] = jnp.zeros((SUBL, n2), F32)

        def both_halves():
            for i in range(len(PAIRS)):
                step(i)
            merge(A, OWN)
            third_sends(A)
            for i in range(len(PAIRS), len(seq)):
                step(i)
            merge(B, OWN)
            fill_next()
            rs_done(A)
            norm_half(A, loads)

        def products(h):
            cross(h)
            fill_next()
            ready(h, XN)
            ready(h, YN)
            product(h, XN)
            product(h, YN)
            fill_next()
            cross_far(h)

        if kind == FIRST:
            norm_half(A, loads)
            loads = norm_load(B)
            await_peers()
            own_sends(A)
            norm_half(B, loads)
            product(A, OWN)
            forward(A)
            own_sends(B)
            ready(B, OWN)
            product(B, OWN)
            products(A)
            product(A, FAR)
            forward(B)
            products(B)
            product(B, FAR)
        elif kind == LAST:
            both_halves()
            loads = norm_load(B)
            fill_next()
            third_sends(B)
            fill(ALL)
            rs_done(B)
            norm_half(B, loads)
        elif kind == MID:
            both_halves()
            loads = norm_load(B)
            fill_next()
            third_sends(B)
            own_sends(A)
            fill_next()
            product(A, OWN)
            fill_next()
            rs_done(B)
            norm_half(B, loads)
            fill_next()
            forward(A)
            own_sends(B)
            fill_next()
            product(B, OWN)
            fill_next()
            products(A)
            fill_next()
            product(A, FAR)
            forward(B)
            fill_next()
            products(B)
            fill(ALL)
            product(B, FAR)
        elif kind == TOP:
            for c in srcs:
                c.wait()
            product_in(0, send=False)
            own_sends(A)
            for i in range(1, len(PAIRS)):
                step(i, False)
            forward(A)
            own_sends(B)
            merge(A, OWN)
            product(A, OWN)
            ready(B, OWN)
            cross(A)
            product(B, OWN)
            ready(A, XN)
            ready(A, YN)
            product(A, XN)
            product(A, YN)
            forward(B)
            cross_far(A)
            for n in range(tiles1):
                far_sends(n)
            first_sends(A, XN)
            first_sends(A, YN)
            product_in(4)
            product(A, FAR)
            cross(B)
            step(5, False)
            ready(B, XN)
            ready(B, YN)
            product(B, XN)
            cross_far(B)
            product(B, YN)
            third_sends(A)
            first_sends(B, FAR)
            merge(B, XN)
            first_sends(B, XN)
            product_in(6)
            merge(B, YN)
            first_sends(B, YN)
            product_in(7)
            merge(B, OWN)
            rs_done(A)
            norm_half(A, loads)
            loads = norm_load(B)
            product(B, FAR)
            third_sends(B)
            rs_done(B)
            norm_half(B, loads)

        for j in range(n_acc):
            r.vo[pl.ds(j, 1), :] = jnp.sum(r.acc[j], axis=0, keepdims=True)
        if n_acc:
            r.vo[n_acc:, :] = jnp.zeros((SUBL - n_acc, D), F32)
        if ag and what == DACT:
            r.bup[...] = jnp.sum(r.bacc[...], axis=0, keepdims=True)
        for c in out_copy:
            c.wait()
        if rs:
            for (h, j), c in rs_copy.items():
                if h == B or j > OWN + YN + 1:
                    c.wait_send()
            for (n, j), c in far_copy.items():
                if j:
                    c.wait_send()
        if ag:
            for c in ag_copy.values():
                c.wait_send()
            for cs in res_out.values():
                for c in cs:
                    c.wait()
            for c in last_copy + list(flipped.values()):
                c.wait()

    return call(name, cid, body, ins, outs, sc, ("vec", "b_up", "vo", "bup"))


def positions(me):
    def pos(axis):
        i = lax.broadcasted_iota(jnp.int32, (ROWS, ROWS), axis)
        return lax.bitwise_xor(lax.div(i, GROUP), me) * GROUP + lax.rem(i, GROUP)

    return pos(0), pos(1)


def heads_of(x, part, h):
    at = part * INNER + h * HD
    return x[:, at : at + HD]


def softmax(s):
    e = jnp.exp(s - jnp.max(s, axis=-1, keepdims=True))
    return e * (ONE / jnp.sum(e, axis=-1, keepdims=True))


def attn_fwd_kernel(group, info, qkv, ctx, s_ref, p_ref):
    row, col = positions(info[ALL_SEQS])
    for first in range(0, SEQS, group):
        some = [(i, h) for i in range(first, first + group) for h in range(HEADS)]
        xs = {i: qkv[:, i].reshape(ROWS, QKV_N) for i, _ in some}
        for n, (i, h) in enumerate(some):
            mask = (col <= row) & (col < info[pl.program_id(0) * SEQS + i])
            score = dims(heads_of(xs[i], 0, h), heads_of(xs[i], 1, h), 1, 1) * HD**-HALF
            s_ref[n] = jnp.where(mask, score, NEG)
        p_ref[...] = softmax(s_ref[...]).astype(BF)
        out = {i: [] for i in xs}
        for n, (i, h) in enumerate(some):
            out[i].append(dims(p_ref[n], heads_of(xs[i], TWO, h), 1, 0).astype(BF))
        for i, parts in out.items():
            ctx[:, i] = jnp.concatenate(parts, axis=-1).reshape(PEERS, GROUP, INNER)


def attn_bwd_steps(group, info, qkv, dctx, out, s_ref, dp_ref, p_ref, ds_ref):
    row, col = positions(info[ALL_SEQS])
    for first in range(0, SEQS, group):
        some = [(i, h) for i in range(first, first + group) for h in range(HEADS)]
        xs = {i: (qkv[:, i].reshape(ROWS, QKV_N), dctx[:, i].reshape(ROWS, INNER)) for i, _ in some}
        for n, (i, h) in enumerate(some):
            x, d = xs[i]
            mask = (col <= row) & (col < info[pl.program_id(0) * SEQS + i])
            score = dims(heads_of(x, 0, h), heads_of(x, 1, h), 1, 1) * HD**-HALF
            s_ref[n] = jnp.where(mask, score, NEG)
            dp_ref[n] = dims(heads_of(d, 0, h), heads_of(x, TWO, h), 1, 1).astype(BF)
        p = softmax(s_ref[...])
        dp = dp_ref[...].astype(F32)
        p_ref[...] = p.astype(BF)
        ds = p * (dp - jnp.sum(dp * p, axis=-1, keepdims=True))
        ds_ref[...] = (ds * HD**-HALF).astype(BF)
        grads = {i: ([], [], []) for i in xs}
        for n, (i, h) in enumerate(some):
            x, d = xs[i]
            dq, dk, dv = grads[i]
            dq.append(dims(ds_ref[n], heads_of(x, 1, h), 1, 0).astype(BF))
            dk.append(dims(ds_ref[n], heads_of(x, 0, h), 0, 0).astype(BF))
            dv.append(dims(p_ref[n], heads_of(d, 0, h), 0, 0).astype(BF))
        for i, parts in grads.items():
            out[:, i] = jnp.concatenate(sum(parts, []), axis=-1).reshape(PEERS, GROUP, QKV_N)


def seq_spec(n):
    per_half = PEERS // SEQS
    return pl.BlockSpec((None, PEERS, SEQS, GROUP, n), lambda i, info: (lax.div(i, per_half), 0, lax.rem(i, per_half), 0, 0))


def by_seq(a):
    return a.reshape(TWO, PEERS, PEERS, GROUP, a.shape[-1])


def seq_shape(n):
    return jax.ShapeDtypeStruct((TWO, PEERS, PEERS, GROUP, n), BF)


def attn_tiles(group, *types):
    return [pltpu.VMEM((group * HEADS, ROWS, ROWS), t) for t in types]


def attn_fwd(info, qkv, group):
    grid_spec = pltpu.PrefetchScalarGridSpec(
        num_scalar_prefetch=1, grid=(ALL_SEQS // SEQS,), in_specs=[seq_spec(QKV_N)], out_specs=seq_spec(INNER), scratch_shapes=attn_tiles(group, F32, BF)
    )
    out = pl.pallas_call(partial(attn_fwd_kernel, group), name="attn_fwd", out_shape=seq_shape(INNER), grid_spec=grid_spec)(info, by_seq(qkv))
    return out.reshape(TWO, PEERS, ROWS, INNER)


def stacking(puts, stacks):
    used = sorted({p[1] for p in puts})
    first = [next(p for p in puts if p[1] == k) for k in used]
    shapes = [jax.ShapeDtypeStruct((p[3],) + p[0].shape, p[0].dtype) for p in first]
    given = [k for k in used if stacks[k] is not None]
    dma = pltpu.SemaphoreType.DMA
    scratch = [pltpu.VMEM(p[0].shape, p[0].dtype) for p in puts] + [dma((len(puts),)), dma((len(puts),))]
    return used, shapes, given, scratch


def attn_bwd(info, qkv, dctx, puts, stacks, group):
    used, shapes, given, scratch = stacking(puts, stacks)
    m = len(puts)

    def kernel(info, qkv, dctx, *refs):
        grads, refs = refs[:m], refs[m + len(given) :]
        out, outs, refs = refs[0], refs[1 : 1 + len(used)], refs[1 + len(used) :]
        bounce, load_sem, put_sem, tiles = refs[:m], refs[m], refs[m + 1], refs[m + TWO :]
        step = pl.program_id(0)

        def load(i):
            return Pieces(grads[i], bounce[i], load_sem.at[i], PEERS)

        def put(i):
            return Pieces(bounce[i], outs[used.index(puts[i][1])].at[puts[i][TWO]], put_sem.at[i], PEERS)

        @pl.when(step == 0)
        def _():
            for i in range(m):
                load(i).start()

        for at, some in ((1, range(m // TWO)), (TWO, range(m // TWO, m))):

            @pl.when(step == at)
            def _(some=some):
                for i in some:
                    load(i).wait()
                    put(i).start()

        attn_bwd_steps(group, info, qkv, dctx, out, *tiles)

        @pl.when(step == ALL_SEQS // SEQS - 1)
        def _():
            for i in range(m):
                put(i).wait()

    hbm = pl.BlockSpec(memory_space=ANY)
    grid_spec = pltpu.PrefetchScalarGridSpec(
        num_scalar_prefetch=1,
        grid=(ALL_SEQS // SEQS,),
        in_specs=[seq_spec(QKV_N), seq_spec(INNER)] + [hbm] * (m + len(given)),
        out_specs=[seq_spec(QKV_N)] + [hbm] * len(used),
        scratch_shapes=scratch + attn_tiles(group, F32, BF, BF, BF),
    )
    res = pl.pallas_call(
        kernel,
        name="attn_bwd",
        out_shape=[seq_shape(QKV_N)] + shapes,
        grid_spec=grid_spec,
        input_output_aliases={3 + m + j: 1 + used.index(k) for j, k in enumerate(given)},
        compiler_params=pltpu.CompilerParams(vmem_limit_bytes=VMEM_LIMIT),
    )(info, by_seq(qkv), by_seq(dctx), *[p[0] for p in puts], *[stacks[k] for k in given])
    for k, a in zip(used, res[1:]):
        stacks[k] = a
    return res[0].reshape(TWO, PEERS, ROWS, QKV_N)


def put_last(puts, stacks):
    used, shapes, given, scratch = stacking(puts, stacks)
    m = len(puts)

    def kernel(*refs):
        grads, refs = refs[:m], refs[m + len(given) :]
        outs, refs = refs[: len(used)], refs[len(used) :]
        bounce, load_sem, put_sem = refs[:m], refs[m], refs[m + 1]
        loads = [Pieces(grads[i], bounce[i], load_sem.at[i], PEERS).start() for i in range(m)]
        stores = []
        for i, p in enumerate(puts):
            loads[i].wait()
            stores.append(Pieces(bounce[i], outs[used.index(p[1])].at[p[TWO]], put_sem.at[i], PEERS).start())
        for c in stores:
            c.wait()

    hbm = pl.BlockSpec(memory_space=ANY)
    res = pl.pallas_call(
        kernel,
        name="put_last",
        out_shape=shapes,
        in_specs=[hbm] * (m + len(given)),
        out_specs=[hbm] * len(used),
        scratch_shapes=scratch,
        input_output_aliases={m + j: used.index(k) for j, k in enumerate(given)},
        compiler_params=pltpu.CompilerParams(vmem_limit_bytes=VMEM_LIMIT),
    )(*[p[0] for p in puts], *[stacks[k] for k in given])
    for k, a in zip(used, res):
        stacks[k] = a


def sum_rows(parts, cid):
    n, half = len(parts), D // TWO
    per = 6
    rows = -(-per * n // SUBL) * SUBL
    ins = SimpleNamespace()
    for l, (a, b) in enumerate(parts):
        setattr(ins, f"a{l}", a)
        setattr(ins, f"b{l}", b)

    def body(r):
        core, px, py = peers()
        say_here((core, px, py))
        odd = lax.rem(lax.axis_index(TP), TWO)
        mine = pl.ds(pl.multiple_of(odd * half, half), half)
        for l in range(n):
            at = per * l
            r.v[at : at + TWO, :] = getattr(r, f"a{l}")[:TWO, :]
            r.v[at + TWO : at + per, :] = getattr(r, f"b{l}")[: per - TWO, :]
        if rows > per * n:
            r.v[per * n :, :] = jnp.zeros((rows - per * n, D), F32)
        await_peers()

        def send(src, dst, i, dev):
            c = remote(src, dst, r.send.at[i], r.recv.at[i], dev)
            c.start()
            return c

        send(r.v, r.a, 0, core).wait()
        r.s[0] = r.v[:, mine] + r.a[:, mine]
        for i, dev in enumerate((px, py)):
            send(r.s.at[i], r.b.at[i], 1 + i, dev).wait()
            r.s[i + 1] = r.s[i] + r.b[i]
        c = send(r.s.at[TWO], r.t.at[:, mine], 3, core)
        r.u[:, mine] = r.s[TWO]
        c.wait()
        first = lax.broadcasted_iota(jnp.int32, (1, D), 1) < half
        keep = first == (odd == 0)
        for l in range(n):
            at = slice(per * l, per * (l + 1))
            r.o[l] = jnp.where(keep, r.u[at, :], r.t[at, :])

    dma = pltpu.SemaphoreType.DMA
    whole, part = pltpu.VMEM((rows, D), F32), (rows, half)
    scratch = SimpleNamespace(v=whole, a=whole, t=whole, u=whole, s=pltpu.VMEM((3,) + part, F32), b=pltpu.VMEM((TWO,) + part, F32), send=dma((4,)), recv=dma((4,)))
    outs = SimpleNamespace(o=jax.ShapeDtypeStruct((n, per, D), F32))
    return call("sum_rows", cid, body, ins, outs, scratch, list(vars(ins)) + ["o"]).o


def group_body(x_loc, dy_loc, len_loc, wqkv, wout, wup, bup, wdown, vec):
    n = wqkv.shape[0]
    ids = iter(range(ROWS))
    shape = x_loc.shape
    x = x_loc.reshape(TWO, ROWS, D)
    dy = dy_loc.reshape(TWO, ROWS, D)
    wq = jnp.transpose(wqkv, (0, 2, 3, 4, 1)).reshape(n, QKV_N, D)
    wo = wout.reshape(n, INNER, D)
    info = jnp.concatenate([len_loc, lax.axis_index(TP).reshape(1).astype(jnp.int32)])

    def flat(a):
        return a.reshape(TOK, a.shape[-1])

    def row(layer, i, bias=None):
        return SimpleNamespace(gain=(layer, i), shift=(layer, i + 1), bias=bias)

    ln2, bias1, bias2 = TWO, 4, 5
    saved = [SimpleNamespace() for _ in range(n)]
    r = fused("first", next(ids), FIRST, N_FIRST, dict(in0=x, wb=wq, vec=vec), row(0, 0), ag=(QKV, 0))
    s = saved[0]
    s.x, s.a, s.qkv = x, r.full, r.res
    for l in range(n):
        s = saved[l]
        s.ctx = attn_fwd(info, s.qkv, SEQS)
        arrays = dict(lhs1=s.ctx, wa=wo, wb=wup, in0=s.x, vec=vec, b_up=bup)
        r = fused(f"mlp_in_{l}", next(ids), MID, N_LN, arrays, row(l, ln2, (l, bias1)), rs=(l, INNER, False), ag=(UP, l))
        s.hid, s.act, s.slope, s.m_t, s.act_t = r.out0, r.res, r.slope, r.full_t, r.res_t
        if l + 1 < n:
            arrays = dict(lhs1=s.act, wa=wdown, wb=wq, in0=s.hid, vec=vec)
            r = fused(f"attn_in_{l + 1}", next(ids), MID, N_LN, arrays, row(l + 1, 0, (l, bias2)), rs=(l, FF, False), ag=(QKV, l + 1))
            s = saved[l + 1]
            s.x, s.a, s.qkv = r.out0, r.full, r.res
    s = saved[n - 1]
    arrays = dict(lhs1=s.act, wa=wdown, wb=wdown, in0=s.hid, vec=vec, src=dy, slope=s.slope)
    r = fused("top", next(ids), TOP, N_RES, arrays, row(0, 0, (n - 1, bias2)), rs=(n - 1, FF, False), ag=(DACT, n - 1))
    y, d_cur, d_full, d_pre = r.out0, r.out1, r.full, r.res
    g_bup, rows, puts, stacks = [r.bup], [], [(y.reshape(KT, D), 4, 0, 1)], [None] * 6
    mlp_plans = ((3, 2, 0, 6, 2, 0, 2, 0, 2, 2, 3, 0, 2), (2, 1, 0, 4, 1, 0, 2, 0, 2, 3, 4, 1, 2), (3, 1, 0, 5, 1, 0, 2, 0, 2, 2, 3, 0, 2))
    attn_plans = ((4, 3), (2, 1, 0, 4, 1, 0, 1, 1, 2, 2, 4, 1, 2), (3, 2, 0, 5, 1, 0, 1, 1, 1, 1, 3, 1, 2))
    for l in reversed(range(n)):
        s = saved[l]
        arrays = dict(lhs1=d_pre, wa=wup, wb=wo, in0=s.hid, in1=d_cur, vec=vec, f0l=s.act_t, f0r=flat(d_full), f1l=s.m_t, f1r=flat(d_pre))
        common = dict(fills=((FF, D, TWO), (D, FF, 1)), bm=BM + BM, flat_t=True, plan=mlp_plans[l])
        r = fused(f"d_mlp_{l}", next(ids), MID, N_BWD2, arrays, row(l, ln2), rs=(l, FF, True), ag=(DCTX, l), **common)
        d_hid, d_attn, v3 = r.out0, r.full, r.vo
        puts += [(r.g0, 3, l, n), (r.g1, TWO, l, n)]
        d_qkv = attn_bwd(info, s.qkv, r.res, puts, stacks, TWO if l else 1)
        arrays = dict(lhs1=d_qkv, wa=wq, in0=s.x, in1=d_hid, vec=vec, f0l=flat(s.ctx), f0r=flat(d_attn), f1l=flat(d_qkv), f1r=flat(s.a))
        common = dict(rs=(l, QKV_N, False), fills=((INNER, D, 1), (QKV_N, D, 3)), plan=attn_plans[l])
        if l:
            arrays.update(wb=wdown, slope=saved[l - 1].slope)
            r = fused(f"d_attn_{l}", next(ids), MID, N_BWD1, arrays, row(l, 0), ag=(DACT, l - 1), **common)
            g_bup.append(r.bup)
            d_full, d_pre = r.full, r.res
        else:
            r = fused(f"d_attn_{l}", next(ids), LAST, N_BWD1, arrays, row(l, 0), **common)
        puts = [(r.g0, 1, l, n), (r.g1, 0, l, n)]
        rows.append((r.vo, v3))
        d_cur = r.out0
    put_last(puts + [(d_cur.reshape(KT, D), 5, 0, 1)], stacks)
    g_vec = sum_rows(rows[::-1], next(ids))
    g_qkv = jnp.transpose(stacks[0].reshape(n, 3, HEADS, HD, D), (0, 4, 1, 2, 3))
    g_out = stacks[1].reshape(n, HEADS, HD, D)
    return stacks[4].reshape(shape), stacks[5].reshape(shape), g_qkv, g_out, stacks[2], jnp.concatenate(g_bup[::-1]), stacks[3], g_vec


def solution(mesh):
    act_spec = P(DP, TP, None)
    in_specs = (act_spec, act_spec, P(DP), P(None, None, None, TP, None), P(None, TP, None, None), P(None, None, TP), P(None, TP), P(None, TP, None), P())
    out_specs = (act_spec, act_spec, P(DP, None, None, TP, None), P(DP, TP, None, None), P(DP, None, TP), P(DP, TP), P(DP, TP, None), P(DP, None, None))
    return jax.shard_map(group_body, mesh=mesh, in_specs=in_specs, out_specs=out_specs, check_vma=False)
```

```python
from functools import partial
from types import SimpleNamespace

import jax
import jax.numpy as jnp
from jax import lax
from jax.experimental import pallas as pl
from jax.experimental.pallas import tpu as pltpu
from jax.sharding import PartitionSpec as P

TP, DP = "tp", "dp"
D, FF, INNER, QKV_N = 3072, 1536, 384, 1152
ROWS, HALF_ROWS, GROUP = 128, 64, 16
LANES, SUBL = 128, 8
A, B = HALVES = range(2)
PEERS = 8
TOK = len(HALVES) * PEERS * ROWS
HEADS, HD = 4, 96
SEQS, ALL_SEQS = 4, 16
BM, BN, KT = 384, 512, 256
BF, F32 = jnp.bfloat16, jnp.float32
ANY = pl.ANY
VMEM_LIMIT = 66_900_000
GELU_C, GELU_D = 0.7978845608028654, 0.044715
EPS, NEG = 1e-5, -1e30
ONE, TWO, HALF = 1.0, 2, 0.5
OWN, XN, YN, FAR = PAIRS = range(4)
Q_ORDER = (FAR, XN, YN, OWN)
R_X, R_Y, R_FAR = 2, 4, 6
X_FAR, Y_FAR, X_RAW, Y_RAW, X_SUM, Y_SUM, N_RS = range(4, 11)
G_CORE, G_XT, G_XB, G_YB, G_YT, G_FT, G_FB, G_C3, G_C5, G_C7, N_AG = range(11)
CROSSING = {XN: G_C3, YN: G_C5, FAR: G_C7}
FIRST, MID, TOP, LAST = range(4)
N_FIRST, N_LN, N_RES, N_BWD2, N_BWD1 = range(5)
QKV, UP, DACT, DCTX = range(4)
WIDTH = (QKV_N, FF, FF, INNER)
ALL = 1 << 20


def dims(lhs, rhs, lc, rc):
    return lax.dot_general(lhs, rhs, (((lc,), (rc,)), ((), ())), preferred_element_type=F32)


def peers():
    me = lax.axis_index(TP)
    dp = lax.axis_index(DP)

    def flip(bit):
        return me + bit - TWO * bit * lax.rem(lax.div(me, bit), TWO)

    return [(dp, flip(1 << k)) for k in range(3)]


def say_here(devices):
    for dev in devices:
        pl.semaphore_signal(pltpu.get_barrier_semaphore(), inc=1, device_id=dev, device_id_type=pl.DeviceIdType.MESH)


def await_peers(n=3):
    pl.semaphore_wait(pltpu.get_barrier_semaphore(), n)


def remote(src, dst, send, recv, dev):
    return pltpu.make_async_remote_copy(src_ref=src, dst_ref=dst, send_sem=send, recv_sem=recv, device_id=dev, device_id_type=pl.DeviceIdType.MESH)


class Pieces:
    def __init__(self, src, dst, sem, n):
        self.src, self.dst, self.sem, self.n = src, dst, sem, n

    def start(self):
        src, dst = self.src, self.dst
        step = src.shape[-2] // self.n
        for i in range(self.n):
            at = pl.ds(i * step, step)
            if len(src.shape) == 3:
                for j in range(src.shape[0]):
                    pltpu.make_async_copy(src.at[j, at], dst.at[j, at], self.sem).start()
            else:
                pltpu.make_async_copy(src.at[at], dst.at[at], self.sem).start()
        return self

    def wait(self):
        pltpu.make_async_copy(self.src, self.dst, self.sem).wait()


def call(name, cid, body, ins, outs, scratch, small):
    names = [list(vars(a)) for a in (ins, outs, scratch)]

    def kernel(*refs):
        body(SimpleNamespace(**dict(zip(sum(names, []), refs))))

    def spec(n):
        return pl.BlockSpec(memory_space=pltpu.VMEM if n in small else ANY)

    res = pl.pallas_call(
        kernel,
        name=name,
        out_shape=list(vars(outs).values()),
        in_specs=[spec(n) for n in names[0]],
        out_specs=[spec(n) for n in names[1]],
        scratch_shapes=list(vars(scratch).values()),
        compiler_params=pltpu.CompilerParams(vmem_limit_bytes=VMEM_LIMIT, collective_id=cid, has_side_effects=True),
    )(*vars(ins).values())
    return SimpleNamespace(**dict(zip(names[1], res)))


def config(norm, arrays, vec, rs=None, ag=None, fills=(), bm=BM, flat_t=False, plan=(), taken=()):
    return SimpleNamespace(norm=norm, arrays=arrays, vec=vec, rs=rs, ag=ag, fills=fills, bm=bm, flat_t=flat_t, plan=plan, taken=dict(taken))


def declare(c):
    outs, sc = SimpleNamespace(), SimpleNamespace()
    dma = pltpu.SemaphoreType.DMA
    n_in = TWO if c.norm in (N_BWD2, N_BWD1) else 1
    n_acc = {N_BWD2: 4, N_BWD1: TWO}.get(c.norm, 0)
    shard = jax.ShapeDtypeStruct((TWO, ROWS, D), F32)
    if c.norm != N_FIRST:
        outs.out0 = shard
        sc.nout = pltpu.VMEM((ROWS, D), F32)
    if c.norm == N_RES:
        outs.out1 = shard
        sc.nout1 = pltpu.VMEM((ROWS, D), F32)
    sc.nin = pltpu.VMEM((n_in, ROWS, D), F32)
    sc.nsem = dma((n_in + TWO,))
    if n_acc:
        outs.vo = jax.ShapeDtypeStruct((SUBL, D), F32)
        sc.acc = pltpu.VMEM((n_acc, SUBL, D), F32)
    if c.rs:
        k1 = c.rs[1]
        tile1 = 1024
        tiles1 = D // tile1
        halves = (TWO, ROWS, D)
        sc.w1 = pltpu.VMEM((D, k1) if c.rs[2] else (k1, D), BF)
        sc.lhs = pltpu.VMEM((TWO, TWO, ROWS, k1), BF)
        sc.own = pltpu.VMEM((TWO, len(PAIRS), ROWS, D), BF)
        sc.snd = pltpu.VMEM((len(PAIRS), ROWS, D), BF)
        sc.drx = pltpu.VMEM((TWO, len(PAIRS), ROWS, D), BF)
        sc.hx = pltpu.VMEM((TWO, HALF_ROWS, D), BF)
        sc.hy = pltpu.VMEM((TWO, HALF_ROWS, D), BF)
        sc.rx = pltpu.VMEM(halves, BF)
        sc.ry = pltpu.VMEM(halves, BF)
        sc.w1_sem = dma((tiles1,))
        sc.lhs_sem = dma((TWO,))
        sc.rs_send = dma((TWO, N_RS))
        sc.rs_recv = dma((TWO, N_RS))
        sc.far_send = dma((tiles1, len(PAIRS)))
        sc.far_recv = dma((tiles1, len(PAIRS)))
    if c.ag:
        what = c.ag[0]
        n2 = WIDTH[what]
        outs.full = jax.ShapeDtypeStruct((TWO, PEERS, ROWS, D), BF)
        outs.res = jax.ShapeDtypeStruct((TWO, PEERS, ROWS, n2), BF)
        pairs_of = (TWO, TWO, ROWS, n2)
        sc.w2 = pltpu.VMEM((D, n2) if what == UP else (n2, D), BF)
        sc.g = pltpu.VMEM((TWO, ROWS, D), BF)
        sc.agin = pltpu.VMEM((TWO, TWO, ROWS, D), BF)
        sc.last = pltpu.VMEM((TWO, ROWS, D), BF)
        sc.w2_sem = dma
        sc.g_sem = dma((TWO,))
        sc.agin_sem = dma((TWO,))
        sc.last_sem = dma((TWO,))
        sc.ag_send = dma((TWO, N_AG))
        sc.ag_recv = dma((TWO, N_AG))
        sc.res_st = pltpu.VMEM(pairs_of, BF)
        sc.res_sem = dma((TWO,))
        if what == UP:
            outs.slope = jax.ShapeDtypeStruct((TWO, PEERS, ROWS, n2), F32)
            outs.full_t = jax.ShapeDtypeStruct((D, TOK), BF)
            outs.res_t = jax.ShapeDtypeStruct((n2, TOK), BF)
            sc.full_ts = pltpu.VMEM((D, KT), BF)
            sc.res_ts = pltpu.VMEM((n2, KT), BF)
            sc.t_sem = dma((TWO,))
        if what == DACT:
            outs.bup = jax.ShapeDtypeStruct((1, n2), F32)
            sc.bacc = pltpu.VMEM((SUBL, n2), F32)
        if what in (UP, DACT):
            sc.slope_st = pltpu.VMEM(pairs_of, F32)
            sc.slope_sem = dma((TWO,))
    if c.fills:
        slots = TWO if c.flat_t else max(f[2] for f in c.fills)
        sc.f_at = pltpu.VMEM((slots, c.bm, TOK), BF)
        sc.f_rhs = pltpu.VMEM((TWO, TOK, BN), BF)
        sc.f_out = pltpu.VMEM((TWO, c.bm, BN), BF)
        if not c.flat_t:
            sc.f_lhs = pltpu.VMEM((TOK, c.bm), BF)
        sc.fl_sem = dma((slots,))
        sc.fr_sem = dma((TWO,))
        sc.fo_sem = dma((TWO,))
        outs.g0 = jax.ShapeDtypeStruct(c.fills[0][:2], BF)
        outs.g1 = jax.ShapeDtypeStruct(c.fills[1][:2], BF)
    return outs, sc


def stage(c, r):
    norm, vec, rs, ag, fills, bm, flat_t, plan = c.norm, c.vec, c.rs, c.ag, c.fills, c.bm, c.flat_t, c.plan
    n_in = TWO if norm in (N_BWD2, N_BWD1) else 1
    n_acc = {N_BWD2: 4, N_BWD1: TWO}.get(norm, 0)
    if rs:
        k1 = rs[1]
        tile1 = 1024
        tiles1 = D // tile1
    if ag:
        what = ag[0]
        n2 = WIDTH[what]
    core, px, py = peers()
    waiting = [1] if c.first else []
    late = () if c.first else (4, 5)

    def await_once():
        while waiting:
            waiting.pop()
            await_peers()

    def begin(src, dst, sem, n=4):
        return Pieces(src, dst, sem, n).start()

    def norm_load(h):
        some = (r.in0, r.in1) if n_in == TWO else (r.in0,)
        return [begin(x.at[h], r.nin.at[i], r.nsem.at[i]) for i, x in enumerate(some)]

    def vrow(row):
        return r.vec[row[0], pl.ds(row[1], 1), :]

    out_copy = []

    def mean(x):
        return jnp.sum(x, axis=-1, keepdims=True) * (ONE / D)

    def norm_half(h, loads):
        for c in loads:
            c.wait()
        while out_copy:
            out_copy.pop().wait()

        def rows(i, carry):
            at = pl.ds(pl.multiple_of(i * GROUP, GROUP), GROUP)
            x = r.nin[0, at, :]
            if rs:
                o = r.own[h, OWN, at, :].astype(F32) + r.rx[h, at, :].astype(F32) + r.ry[h, at, :].astype(F32)
                o = o.astype(BF).astype(F32)
            if norm in (N_LN, N_RES):
                x = x + o + vrow(vec.bias)
                r.nout[at, :] = x
            if norm == N_RES:
                r.nout1[at, :] = r.g[h, at, :].astype(F32)
                return carry
            cen = x - mean(x)
            rstd = lax.rsqrt(mean(cen * cen) + EPS)
            if norm in (N_FIRST, N_LN):
                r.g[h, at, :] = (cen * rstd * vrow(vec.gain) + vrow(vec.shift)).astype(BF)
                return carry
            xh = cen * rstd
            dxh = o * vrow(vec.gain)
            base = r.nin[1, at, :]
            res = base + rstd * (dxh - mean(dxh) - xh * mean(dxh * xh))
            r.nout[at, :] = res
            if ag:
                r.g[h, at, :] = res.astype(BF)
            sums = [o * xh, o] + ([res, base] if norm == N_BWD2 else [])
            for j, v in enumerate(sums):
                r.acc[j] += v[:SUBL] + v[SUBL:]
            return carry

        lax.fori_loop(0, ROWS // GROUP, rows, 0)
        if norm != N_FIRST:
            out_copy.append(begin(r.nout, r.out0.at[h], r.nsem.at[n_in]))
        if norm == N_RES:
            out_copy.append(begin(r.nout1, r.out1.at[h], r.nsem.at[n_in + 1]))

    top, bot = pl.ds(0, HALF_ROWS), pl.ds(HALF_ROWS, HALF_ROWS)
    if rs:
        seq = [(h, q) for h in HALVES for q in Q_ORDER]
        lhs_loads, rs_copy, far_copy, w1_loads = {}, {}, {}, []
        own = r.own

        def w1_load():
            for n in range(tiles1):
                at = pl.ds(n * tile1, tile1)
                src, dst = r.wa.at[rs[0]], r.w1
                src, dst = (src.at[at], dst.at[at]) if rs[2] else (src.at[:, at], dst.at[:, at])
                w1_loads.append(begin(src, dst, r.w1_sem.at[n]))

        def lhs_load(i):
            h, q = seq[i]
            s = i % TWO
            lhs_loads[i] = begin(r.lhs1.at[h, pl.ds(TWO * q, TWO)], r.lhs.at[s], r.lhs_sem.at[s])

        def lhs_late():
            for i in late:
                lhs_load(i)

        def rs_start(h, j, src, dst, dev):
            c = remote(src, dst, r.rs_send.at[h, j], r.rs_recv.at[h, j], dev)
            c.start()
            rs_copy[h, j] = c

        def far_start(n, j, src, dst, dev):
            c = remote(src, dst, r.far_send.at[n, j], r.far_recv.at[n, j], dev)
            c.start()
            far_copy[n, j] = c

        def add_into(dst, src, n, at_cols=slice(None)):
            def rows(i, carry):
                at = pl.ds(pl.multiple_of(i * GROUP, GROUP), GROUP)
                dst[at, at_cols] = (dst[at, at_cols].astype(F32) + src[at, at_cols].astype(F32)).astype(BF)
                return carry

            lax.fori_loop(0, n // GROUP, rows, 0)

        def far_merge(n, send):
            cols = pl.ds(n * tile1, tile1)
            far_copy[n, 0].wait_recv()
            add_into(own.at[A, FAR], r.drx.at[A, FAR], ROWS, cols)
            if send:
                far_sends(n)

        def far_sends(n):
            cols = pl.ds(n * tile1, tile1)
            far_start(n, 1, own.at[A, FAR, top, cols], r.hx.at[A, :, cols], px)
            far_start(n, 2, own.at[A, FAR, bot, cols], r.hy.at[A, :, cols], py)

        def product_in(i, between=None, send=True):
            h, q = seq[i]
            s = i % TWO
            lhs_loads[i].wait()
            if i == len(PAIRS):
                for n in range(tiles1):
                    far_copy[n, 0].wait_send()
            elif h == B:
                rs_copy[A, q].wait_send()

            def tile(n, carry):
                at = pl.ds(pl.multiple_of(n * tile1, tile1), tile1)
                x = r.lhs[s].reshape(TWO * ROWS, k1)
                y = dims(x, r.w1[at, :], 1, 1) if rs[2] else dims(x, r.w1[:, at], 1, 0)
                y = y.astype(BF)
                own[h, q, :, at] = y[:ROWS]
                r.snd[q, :, at] = y[ROWS:]
                return carry

            if i == 0:
                for n in range(tiles1):
                    cols = pl.ds(n * tile1, tile1)
                    w1_loads[n].wait()
                    tile(n, 0)
                    if n == 0:
                        await_once()
                    far_start(n, 0, r.snd.at[FAR, :, cols], r.drx.at[A, FAR, :, cols], core)
                    if n:
                        far_merge(n - 1, send)
            else:
                tile(0, 0)
                if between:
                    between()
                lax.fori_loop(1, tiles1, tile, 0)
            if i + TWO < len(seq) and i + TWO not in late:
                lhs_load(i + TWO)
            if i:
                rs_start(h, q, r.snd.at[q], r.drx.at[h, q], core)

        def merge(h, q):
            rs_copy[h, q].wait_recv()
            add_into(own.at[h, q], r.drx.at[h, q], ROWS)

        def first_sends(h, q):
            if q == FAR:
                rs_start(h, X_FAR, own.at[h, q, top], r.hx.at[h], px)
                rs_start(h, Y_FAR, own.at[h, q, bot], r.hy.at[h], py)
            if q == XN:
                rs_start(h, X_RAW, own.at[h, q, top], r.rx.at[h, top], px)
            if q == YN:
                rs_start(h, Y_RAW, own.at[h, q, bot], r.ry.at[h, bot], py)

        def far_wait(h, j):
            if h == A:
                for n in range(tiles1):
                    far_copy[n, 1 + j].wait_recv()
            else:
                rs_copy[h, X_FAR + j].wait_recv()

        def third_sends(h):
            far_wait(h, 1)
            add_into(own.at[h, XN, bot], r.hy.at[h], HALF_ROWS)
            rs_start(h, X_SUM, own.at[h, XN, bot], r.rx.at[h, bot], px)
            far_wait(h, 0)
            add_into(own.at[h, YN, top], r.hx.at[h], HALF_ROWS)
            rs_start(h, Y_SUM, own.at[h, YN, top], r.ry.at[h, top], py)

        def rs_done(h):
            for j in (X_RAW, Y_RAW, X_SUM, Y_SUM):
                rs_copy[h, j].wait_recv()

        def step(i, send=True):
            def between():
                h, q = seq[i - 1]
                if i == 1:
                    far_merge(tiles1 - 1, send)
                    return
                merge(h, q)
                if send:
                    first_sends(h, q)

            product_in(i, between if i % len(PAIRS) else None, send)

    if ag:
        full = r.full
        ag_copy, g_copy, ready_loads, res_out, w2_copy, last_copy = {}, {}, {}, {}, [], []

        def w2_load():
            w2_copy.append(begin(r.wb.at[ag[1]], r.w2, r.w2_sem, PEERS))

        def ag_start(h, j, src, dst, dev):
            c = remote(src, dst, r.ag_send.at[h, j], r.ag_recv.at[h, j], dev)
            c.start()
            ag_copy[h, j] = c

        def own_sends(h):
            g = r.g
            ag_start(h, G_XT, g.at[h, top], full.at[h, R_X, top], px)
            ag_start(h, G_YB, g.at[h, bot], full.at[h, R_Y, bot], py)
            ag_start(h, G_XB, g.at[h, bot], full.at[h, R_X, bot], px)
            ag_start(h, G_YT, g.at[h, top], full.at[h, R_Y, top], py)
            ag_start(h, G_CORE, g.at[h], full.at[h, 1], core)
            g_copy[h] = begin(g.at[h], full.at[h, 0], r.g_sem.at[h])

        def far_place(h, other):
            return full.at[h, R_FAR + other] if h == A else r.last.at[other]

        def forward(h):
            ag_copy[h, G_XT].wait_recv()
            ag_start(h, G_FT, full.at[h, R_X, top], far_place(h, 0).at[top], py)
            ag_copy[h, G_YB].wait_recv()
            ag_start(h, G_FB, full.at[h, R_Y, bot], far_place(h, 0).at[bot], px)

        def cross(h):
            ag_copy[h, G_XB].wait_recv()
            ag_start(h, G_C3, full.at[h, R_X], full.at[h, R_X + 1], core)
            ag_copy[h, G_YT].wait_recv()
            ag_start(h, G_C5, full.at[h, R_Y], full.at[h, R_Y + 1], core)

        def cross_far(h):
            ag_copy[h, G_FT].wait_recv()
            ag_copy[h, G_FB].wait_recv()
            ag_start(h, G_C7, far_place(h, 0), far_place(h, 1), core)
            if h == B:
                last_copy.append(begin(r.last.at[0], full.at[h, R_FAR], r.last_sem.at[0]))

        def ready(h, q):
            s = (len(PAIRS) * h + (OWN, XN, YN, FAR).index(q)) % TWO
            pair = pl.ds(TWO * q, TWO)
            loads = []
            if what == DACT:
                loads.append(begin(r.slope.at[h, pair], r.slope_st.at[s], r.slope_sem.at[s]))
            if q == OWN:
                g_copy.pop(h).wait()
                ag_copy[h, G_CORE].wait_recv()
            else:
                ag_copy[h, CROSSING[q]].wait_recv()
            if (h, q) == (B, FAR):
                last_copy.append(begin(r.last.at[1], full.at[h, R_FAR + 1], r.last_sem.at[1]))
            else:
                loads.append(begin(full.at[h, pair], r.agin.at[s], r.agin_sem.at[s]))
            ready_loads[h, q] = (s, loads)

        flipped = {}

        def flip(src, stage, dst, i):
            if i in flipped:
                flipped[i].wait()

            def block(k, carry):
                at = pl.ds(pl.multiple_of(k * KT, KT), KT)
                stage[at, :] = src[:, :, at].reshape(KT, KT).T
                return carry

            lax.fori_loop(0, stage.shape[0] // KT, block, 0)
            flipped[i] = begin(stage, dst, r.t_sem.at[i])

        to_flip = []

        def flip_all():
            while to_flip:
                flip(*to_flip.pop(0))

        def product(h, q):
            if (h, q) not in ready_loads:
                ready(h, q)
            s, loads = ready_loads.pop((h, q))
            pair = pl.ds(TWO * q, TWO)
            while w2_copy:
                w2_copy.pop().wait()
            for c in res_out.pop(s, ()):
                c.wait()
            for c in loads:
                c.wait()
            nt = BM if what in (QKV, DCTX) else BN

            def tile(n, carry):
                at = pl.ds(pl.multiple_of(n * nt, nt), nt)
                x = r.last[...] if (h, q) == (B, FAR) else r.agin[s]
                x = x.reshape(TWO * ROWS, D)
                y = dims(x, r.w2[:, at], 1, 0) if what == UP else dims(x, r.w2[at, :], 1, 1)
                if what == UP:
                    u = y + r.b_up[pl.ds(ag[1], 1), at]
                    t = jnp.tanh(GELU_C * (u + GELU_D * (u * u * u)))
                    slope = HALF * (ONE + t) + (HALF * GELU_C) * u * (ONE - t * t) * (ONE + (3 * GELU_D) * (u * u))
                    r.slope_st[s, :, :, at] = slope.reshape(TWO, ROWS, nt)
                    y = u * (HALF * (ONE + t))
                if what == DACT:
                    y = y.astype(BF).astype(F32) * r.slope_st[s, :, :, at].reshape(TWO * ROWS, nt)
                    r.bacc[:, at] += jnp.sum(y.reshape(-1, SUBL, nt), axis=0)
                r.res_st[s, :, :, at] = y.astype(BF).reshape(TWO, ROWS, nt)
                return carry

            if n2 == nt:
                tile(0, 0)
            else:
                lax.fori_loop(0, n2 // nt, tile, 0)
            res_out[s] = [begin(r.res_st.at[s], r.res.at[h, pair], r.res_sem.at[s])]
            if what == UP:
                res_out[s].append(begin(r.slope_st.at[s], r.slope.at[h, pair], r.slope_sem.at[s]))
                cols = pl.ds((h * PEERS + TWO * q) * ROWS, KT)
                gathered = r.last if (h, q) == (B, FAR) else r.agin.at[s]
                to_flip.append((gathered, r.full_ts, r.full_t.at[:, cols], 0))
                to_flip.append((r.res_st.at[s], r.res_ts, r.res_t.at[:, cols], 1))

    jobs = []
    if fills:
        refs = ((r.f0l, r.f0r, r.g0), (r.f1l, r.f1r, r.g1))
        jobs = [SimpleNamespace(lhs=f[0], rhs=f[1], out=f[2], blocks=c[0] // bm // c[2], tiles=c[1] // BN, sub=c[2], done=0) for f, c in zip(refs, fills)]

    def lhs_copy(j, k):
        at = pl.ds(pl.multiple_of(k * bm, bm), bm)
        if flat_t:
            s = lax.rem(k, TWO)
            return Pieces(j.lhs.at[at], r.f_at.at[s], r.fl_sem.at[s], PEERS)
        return Pieces(j.lhs.at[:, at], r.f_lhs, r.fl_sem.at[0], PEERS)

    def rhs_copy(j, v):
        s = lax.rem(v, TWO)
        return Pieces(j.rhs.at[:, pl.ds(pl.multiple_of(lax.rem(v, j.tiles) * BN, BN), BN)], r.f_rhs.at[s], r.fr_sem.at[s], PEERS)

    def put_copy(j, u):
        s, v = lax.rem(u, TWO), lax.div(u, j.sub)
        row = lax.div(v, j.tiles) * j.sub + lax.rem(u, j.sub)
        dst = j.out.at[pl.ds(pl.multiple_of(row * bm, bm), bm), pl.ds(pl.multiple_of(lax.rem(v, j.tiles) * BN, BN), BN)]
        return Pieces(r.f_out.at[s], dst, r.fo_sem.at[s], 3)

    def job_begin(j):
        lhs_copy(j, jnp.int32(0)).start()
        if flat_t:
            lhs_copy(j, jnp.int32(1)).start()
        rhs_copy(j, jnp.int32(0)).start()

    def fill(n):
        while n > 0 and jobs:
            j = jobs[0]
            rhs_all = j.blocks * j.tiles
            count = rhs_all * j.sub

            def unit(u, carry):
                v, b, s = lax.div(u, j.sub), lax.rem(u, j.sub), lax.rem(u, TWO)
                vs, t = lax.rem(v, TWO), lax.rem(v, j.tiles)
                k = lax.div(v, j.tiles) * j.sub + b

                @pl.when(t == 0)
                def _():
                    lhs_copy(j, k).wait()
                    if flat_t:
                        return
                    for i in range(TOK // KT):
                        r.f_at[b, :, i * KT : (i + 1) * KT] = r.f_lhs[i * KT : (i + 1) * KT, :].T

                    @pl.when(k + 1 < j.blocks * j.sub)
                    def _():
                        lhs_copy(j, k + 1).start()

                @pl.when(b == 0)
                def _():
                    rhs_copy(j, v).wait()

                    @pl.when(v + 1 < rhs_all)
                    def _():
                        rhs_copy(j, v + 1).start()

                @pl.when(u >= TWO)
                def _():
                    put_copy(j, u - TWO).wait()

                r.f_out[s] = dims(r.f_at[lax.rem(k, TWO) if flat_t else b], r.f_rhs[vs], 1, 0).astype(BF)
                put_copy(j, u).start()
                if flat_t:

                    @pl.when((t == j.tiles - 1) & (k + TWO < j.blocks * j.sub))
                    def _():
                        lhs_copy(j, k + TWO).start()

                return carry

            upto = min(count, j.done + n)
            n -= upto - j.done
            lax.fori_loop(j.done, upto, unit, 0)
            j.done = upto
            if upto == count:
                for u in (count - TWO, count - 1):
                    put_copy(j, jnp.int32(u)).wait()
                jobs.pop(0)
                if jobs:
                    job_begin(jobs[0])

    steps = list(plan)

    def fill_next():
        if steps:
            fill(steps.pop(0))

    def prologue():
        if rs:
            lhs_load(0)
            w1_load()
            lhs_load(1)
        if ag:
            w2_load()
        if jobs:
            job_begin(jobs[0])

    def clear():
        for j in range(n_acc):
            r.acc[j] = jnp.zeros((SUBL, D), F32)
        if ag and what == DACT:
            r.bacc[...] = jnp.zeros((SUBL, n2), F32)

    def rs_sent():
        for (h, j), x in rs_copy.items():
            if h == B or j > 3:
                x.wait_send()
        for (n, j), x in far_copy.items():
            if j:
                x.wait_send()
        rs_copy.clear()
        far_copy.clear()

    def rows_out():
        while out_copy:
            out_copy.pop().wait()

    def res_done():
        for s in list(res_out):
            for x in res_out.pop(s):
                x.wait()

    def end():
        for j in range(n_acc):
            r.vo[pl.ds(j, 1), :] = jnp.sum(r.acc[j], axis=0, keepdims=True)
        if n_acc:
            r.vo[n_acc:, :] = jnp.zeros((SUBL - n_acc, D), F32)
        if ag and what == DACT:
            r.bup[...] = jnp.sum(r.bacc[...], axis=0, keepdims=True)
        rows_out()
        if rs:
            rs_sent()
        if ag:
            for x in ag_copy.values():
                x.wait_send()
            res_done()
            for x in last_copy + list(flipped.values()):
                x.wait()

    return SimpleNamespace(**locals())


SHARED = ("own", "snd", "drx", "hx", "hy", "rx", "ry", "nin", "nout", "g", "agin", "last")


def fused(name, cid, kind, *stages):
    ins, outs, scratch, small, views = SimpleNamespace(), SimpleNamespace(), SimpleNamespace(), [], []
    for i, c in enumerate(stages):
        c.first = i == 0
        c_outs, c_sc = declare(c)
        view = {}
        for group, names in ((ins, c.arrays), (outs, vars(c_outs)), (scratch, vars(c_sc))):
            for n, x in names.items():
                view[n] = f"{n}{0 if group is scratch and n in SHARED else i}"
                setattr(group, view[n], x)
                if group is not scratch and n in ("vec", "b_up", "vo", "bup"):
                    small.append(view[n])
        view.update({n: f"{prev}{i - 1}" for n, prev in c.taken.items()})
        views.append(view)
    if len(stages) > 1:
        del scratch.w10
        views[0]["w1"] = views[1]["w2"]

    def body(refs):
        refs = vars(refs)
        st = [stage(c, SimpleNamespace(**{n: refs[x] for n, x in v.items()})) for c, v in zip(stages, views)]
        if len(st) > 1:
            st[0].r.w1 = st[0].r.w1.at[pl.ds(0, stages[0].rs[1])]
        say_here(peers())
        PROGRAMS[kind](*st)

    res = call(name, cid, body, ins, outs, scratch, small)
    return [SimpleNamespace(**{n: getattr(res, x) for n, x in v.items() if hasattr(res, x) and n not in c.taken}) for c, v in zip(stages, views)]


def both_halves(s, loads):
    for i in range(len(PAIRS)):
        s.step(i)
    s.merge(A, OWN)
    s.third_sends(A)
    second_half(s, loads)


def second_half(s, loads):
    for i in range(len(PAIRS), len(s.seq)):
        s.step(i)
    s.merge(B, OWN)
    s.fill_next()
    s.rs_done(A)
    s.norm_half(A, loads)


def products(s, h):
    s.cross(h)
    s.fill_next()
    s.ready(h, XN)
    s.ready(h, YN)
    s.product(h, XN)
    if h == A:
        s.flip_all()
    s.product(h, YN)
    if h == A:
        s.flip_all()
    s.fill_next()
    s.cross_far(h)


def first_program(s):
    s.prologue()
    loads = s.norm_load(A)
    s.norm_half(A, loads)
    loads = s.norm_load(B)
    s.await_once()
    s.own_sends(A)
    s.norm_half(B, loads)
    s.product(A, OWN)
    s.forward(A)
    s.own_sends(B)
    s.ready(B, OWN)
    s.product(B, OWN)
    products(s, A)
    s.product(A, FAR)
    s.forward(B)
    products(s, B)
    s.product(B, FAR)
    s.end()


def last_program(s):
    s.prologue()
    loads = s.norm_load(A)
    s.clear()
    both_halves(s, loads)
    loads = s.norm_load(B)
    s.fill_next()
    s.third_sends(B)
    s.fill(ALL)
    s.rs_done(B)
    s.norm_half(B, loads)
    s.end()


def to_forward(s, next_loads=None):
    loads = s.norm_load(B)
    s.fill_next()
    s.third_sends(B)
    s.own_sends(A)
    s.fill_next()
    s.product(A, OWN)
    s.flip_all()
    s.fill_next()
    s.rs_done(B)
    s.norm_half(B, loads)
    if next_loads:
        next_loads()
    s.fill_next()
    s.forward(A)
    s.own_sends(B)
    s.fill_next()
    s.product(B, OWN)
    s.flip_all()
    s.fill_next()
    products(s, A)
    s.fill_next()
    s.product(A, FAR)
    s.flip_all()
    s.forward(B)


def to_end(s):
    s.fill_next()
    products(s, B)
    s.fill(ALL)
    s.flip_all()
    s.product(B, FAR)
    s.flip_all()
    s.end()


def mid_program(s, z=None):
    s.prologue()
    loads = s.norm_load(A)
    s.clear()
    both_halves(s, loads)
    if z is None:
        to_forward(s)
        to_end(s)
        return

    def next_loads():
        z.w1_load()
        z.w2_load()

    to_forward(s, next_loads)
    s.res_done()
    s.rows_out()
    s.rs_sent()
    z.lhs_load(0)
    z.lhs_load(1)
    loads = z.norm_load(A)
    z.step(0)
    z.step(1)
    s.cross(B)
    z.step(TWO)
    z.step(3)
    s.ready(B, XN)
    s.ready(B, YN)
    z.merge(A, OWN)
    s.cross_far(B)
    s.product(B, XN)
    s.product(B, YN)
    s.flip_all()
    s.product(B, FAR)
    z.third_sends(A)
    s.flip_all()
    s.res_done()
    z.lhs_late()
    for i in range(len(PAIRS), len(z.seq)):
        z.step(i)
    z.merge(B, OWN)
    z.rs_done(A)
    s.end()
    z.norm_half(A, loads)
    to_forward(z)
    to_end(z)


def top_program(s):
    s.prologue()
    loads = s.norm_load(A)
    srcs = [s.begin(s.r.src.at[h], s.r.g.at[h], s.r.g_sem.at[h]) for h in HALVES]
    s.clear()
    for x in srcs:
        x.wait()
    s.await_once()
    s.own_sends(A)
    for i in range(len(PAIRS)):
        s.step(i, False)
        if i == TWO:
            s.forward(A)
            s.own_sends(B)
    s.merge(A, OWN)
    s.product(A, OWN)
    s.ready(B, OWN)
    s.cross(A)
    s.product(B, OWN)
    s.ready(A, XN)
    s.ready(A, YN)
    s.product(A, XN)
    s.product(A, YN)
    s.forward(B)
    s.cross_far(A)
    for n in range(s.tiles1):
        s.far_sends(n)
    s.first_sends(A, XN)
    s.first_sends(A, YN)
    s.product_in(4)
    s.product(A, FAR)
    s.cross(B)
    s.step(5, False)
    s.ready(B, XN)
    s.ready(B, YN)
    s.product(B, XN)
    s.cross_far(B)
    s.product(B, YN)
    s.third_sends(A)
    s.first_sends(B, FAR)
    s.merge(B, XN)
    s.first_sends(B, XN)
    s.product_in(6)
    s.merge(B, YN)
    s.first_sends(B, YN)
    s.product_in(7)
    s.merge(B, OWN)
    s.rs_done(A)
    s.norm_half(A, loads)
    loads = s.norm_load(B)
    s.product(B, FAR)
    s.third_sends(B)
    s.rs_done(B)
    s.norm_half(B, loads)
    s.end()


PROGRAMS = (first_program, mid_program, top_program, last_program)


def positions(me):
    def pos(axis):
        i = lax.broadcasted_iota(jnp.int32, (ROWS, ROWS), axis)
        return lax.bitwise_xor(lax.div(i, GROUP), me) * GROUP + lax.rem(i, GROUP)

    return pos(0), pos(1)


def heads_of(x, part, h):
    at = part * INNER + h * HD
    return x[:, at : at + HD]


def softmax(s):
    e = jnp.exp(s - jnp.max(s, axis=-1, keepdims=True))
    return e * (ONE / jnp.sum(e, axis=-1, keepdims=True))


def attn_fwd_kernel(group, info, qkv, ctx, s_ref, p_ref):
    row, col = positions(info[ALL_SEQS])
    for first in range(0, SEQS, group):
        some = [(i, h) for i in range(first, first + group) for h in range(HEADS)]
        xs = {i: qkv[:, i].reshape(ROWS, QKV_N) for i, _ in some}
        for n, (i, h) in enumerate(some):
            mask = (col <= row) & (col < info[pl.program_id(0) * SEQS + i])
            score = dims(heads_of(xs[i], 0, h), heads_of(xs[i], 1, h), 1, 1) * HD**-HALF
            s_ref[n] = jnp.where(mask, score, NEG)
        p_ref[...] = softmax(s_ref[...]).astype(BF)
        out = {i: [] for i in xs}
        for n, (i, h) in enumerate(some):
            out[i].append(dims(p_ref[n], heads_of(xs[i], TWO, h), 1, 0).astype(BF))
        for i, parts in out.items():
            ctx[:, i] = jnp.concatenate(parts, axis=-1).reshape(PEERS, GROUP, INNER)


def attn_bwd_steps(group, info, qkv, dctx, out, s_ref, dp_ref, p_ref, ds_ref):
    row, col = positions(info[ALL_SEQS])
    for first in range(0, SEQS, group):
        some = [(i, h) for i in range(first, first + group) for h in range(HEADS)]
        xs = {i: (qkv[:, i].reshape(ROWS, QKV_N), dctx[:, i].reshape(ROWS, INNER)) for i, _ in some}
        for n, (i, h) in enumerate(some):
            x, d = xs[i]
            mask = (col <= row) & (col < info[pl.program_id(0) * SEQS + i])
            score = dims(heads_of(x, 0, h), heads_of(x, 1, h), 1, 1) * HD**-HALF
            s_ref[n] = jnp.where(mask, score, NEG)
            dp_ref[n] = dims(heads_of(d, 0, h), heads_of(x, TWO, h), 1, 1).astype(BF)
        p = softmax(s_ref[...])
        dp = dp_ref[...].astype(F32)
        p_ref[...] = p.astype(BF)
        ds = p * (dp - jnp.sum(dp * p, axis=-1, keepdims=True))
        ds_ref[...] = (ds * HD**-HALF).astype(BF)
        grads = {i: ([], [], []) for i in xs}
        for n, (i, h) in enumerate(some):
            x, d = xs[i]
            dq, dk, dv = grads[i]
            dq.append(dims(ds_ref[n], heads_of(x, 1, h), 1, 0).astype(BF))
            dk.append(dims(ds_ref[n], heads_of(x, 0, h), 0, 0).astype(BF))
            dv.append(dims(p_ref[n], heads_of(d, 0, h), 0, 0).astype(BF))
        for i, parts in grads.items():
            out[:, i] = jnp.concatenate(sum(parts, []), axis=-1).reshape(PEERS, GROUP, QKV_N)


def seq_spec(n):
    per_half = PEERS // SEQS
    return pl.BlockSpec((None, PEERS, SEQS, GROUP, n), lambda i, info: (lax.div(i, per_half), 0, lax.rem(i, per_half), 0, 0))


def by_seq(a):
    return a.reshape(TWO, PEERS, PEERS, GROUP, a.shape[-1])


def seq_shape(n):
    return jax.ShapeDtypeStruct((TWO, PEERS, PEERS, GROUP, n), BF)


def attn_tiles(group, *types):
    return [pltpu.VMEM((group * HEADS, ROWS, ROWS), t) for t in types]


def attn_fwd(info, qkv, group):
    grid_spec = pltpu.PrefetchScalarGridSpec(
        num_scalar_prefetch=1, grid=(ALL_SEQS // SEQS,), in_specs=[seq_spec(QKV_N)], out_specs=seq_spec(INNER), scratch_shapes=attn_tiles(group, F32, BF)
    )
    out = pl.pallas_call(partial(attn_fwd_kernel, group), name="attn_fwd", out_shape=seq_shape(INNER), grid_spec=grid_spec)(info, by_seq(qkv))
    return out.reshape(TWO, PEERS, ROWS, INNER)


def stacking(puts, stacks):
    used = sorted({p[1] for p in puts})
    first = [next(p for p in puts if p[1] == k) for k in used]
    shapes = [jax.ShapeDtypeStruct((p[3],) + p[0].shape, p[0].dtype) for p in first]
    given = [k for k in used if stacks[k] is not None]
    dma = pltpu.SemaphoreType.DMA
    scratch = [pltpu.VMEM(p[0].shape, p[0].dtype) for p in puts] + [dma((len(puts),)), dma((len(puts),))]
    return used, shapes, given, scratch


def attn_bwd(info, qkv, dctx, puts, stacks, group):
    used, shapes, given, scratch = stacking(puts, stacks)
    m = len(puts)

    def kernel(info, qkv, dctx, *refs):
        grads, refs = refs[:m], refs[m + len(given) :]
        out, outs, refs = refs[0], refs[1 : 1 + len(used)], refs[1 + len(used) :]
        bounce, load_sem, put_sem, tiles = refs[:m], refs[m], refs[m + 1], refs[m + TWO :]
        step = pl.program_id(0)

        def load(i):
            return Pieces(grads[i], bounce[i], load_sem.at[i], PEERS)

        def put(i):
            return Pieces(bounce[i], outs[used.index(puts[i][1])].at[puts[i][TWO]], put_sem.at[i], PEERS)

        @pl.when(step == 0)
        def _():
            for i in range(m):
                load(i).start()

        for at, some in ((1, range(m // TWO)), (TWO, range(m // TWO, m))):

            @pl.when(step == at)
            def _(some=some):
                for i in some:
                    load(i).wait()
                    put(i).start()

        attn_bwd_steps(group, info, qkv, dctx, out, *tiles)

        @pl.when(step == ALL_SEQS // SEQS - 1)
        def _():
            for i in range(m):
                put(i).wait()

    hbm = pl.BlockSpec(memory_space=ANY)
    grid_spec = pltpu.PrefetchScalarGridSpec(
        num_scalar_prefetch=1,
        grid=(ALL_SEQS // SEQS,),
        in_specs=[seq_spec(QKV_N), seq_spec(INNER)] + [hbm] * (m + len(given)),
        out_specs=[seq_spec(QKV_N)] + [hbm] * len(used),
        scratch_shapes=scratch + attn_tiles(group, F32, BF, BF, BF),
    )
    res = pl.pallas_call(
        kernel,
        name="attn_bwd",
        out_shape=[seq_shape(QKV_N)] + shapes,
        grid_spec=grid_spec,
        input_output_aliases={3 + m + j: 1 + used.index(k) for j, k in enumerate(given)},
        compiler_params=pltpu.CompilerParams(vmem_limit_bytes=VMEM_LIMIT),
    )(info, by_seq(qkv), by_seq(dctx), *[p[0] for p in puts], *[stacks[k] for k in given])
    for k, a in zip(used, res[1:]):
        stacks[k] = a
    return res[0].reshape(TWO, PEERS, ROWS, QKV_N)


def put_last(puts, stacks):
    used, shapes, given, scratch = stacking(puts, stacks)
    m = len(puts)

    def kernel(*refs):
        grads, refs = refs[:m], refs[m + len(given) :]
        outs, refs = refs[: len(used)], refs[len(used) :]
        bounce, load_sem, put_sem = refs[:m], refs[m], refs[m + 1]
        loads = [Pieces(grads[i], bounce[i], load_sem.at[i], PEERS).start() for i in range(m)]
        stores = []
        for i, p in enumerate(puts):
            loads[i].wait()
            stores.append(Pieces(bounce[i], outs[used.index(p[1])].at[p[TWO]], put_sem.at[i], PEERS).start())
        for c in stores:
            c.wait()

    hbm = pl.BlockSpec(memory_space=ANY)
    res = pl.pallas_call(
        kernel,
        name="put_last",
        out_shape=shapes,
        in_specs=[hbm] * (m + len(given)),
        out_specs=[hbm] * len(used),
        scratch_shapes=scratch,
        input_output_aliases={m + j: used.index(k) for j, k in enumerate(given)},
        compiler_params=pltpu.CompilerParams(vmem_limit_bytes=VMEM_LIMIT),
    )(*[p[0] for p in puts], *[stacks[k] for k in given])
    for k, a in zip(used, res):
        stacks[k] = a


def sum_rows(parts, cid):
    n, half = len(parts), D // TWO
    per = 6
    rows = -(-per * n // SUBL) * SUBL
    ins = SimpleNamespace()
    for l, (a, b) in enumerate(parts):
        setattr(ins, f"a{l}", a)
        setattr(ins, f"b{l}", b)

    def body(r):
        core, px, py = peers()
        say_here((core, px, py))
        odd = lax.rem(lax.axis_index(TP), TWO)
        mine = pl.ds(pl.multiple_of(odd * half, half), half)
        for l in range(n):
            at = per * l
            r.v[at : at + TWO, :] = getattr(r, f"a{l}")[:TWO, :]
            r.v[at + TWO : at + per, :] = getattr(r, f"b{l}")[: per - TWO, :]
        if rows > per * n:
            r.v[per * n :, :] = jnp.zeros((rows - per * n, D), F32)
        await_peers()

        def send(src, dst, i, dev):
            c = remote(src, dst, r.send.at[i], r.recv.at[i], dev)
            c.start()
            return c

        send(r.v, r.a, 0, core).wait()
        r.s[0] = r.v[:, mine] + r.a[:, mine]
        for i, dev in enumerate((px, py)):
            send(r.s.at[i], r.b.at[i], 1 + i, dev).wait()
            r.s[i + 1] = r.s[i] + r.b[i]
        c = send(r.s.at[TWO], r.t.at[:, mine], 3, core)
        r.u[:, mine] = r.s[TWO]
        c.wait()
        first = lax.broadcasted_iota(jnp.int32, (1, D), 1) < half
        keep = first == (odd == 0)
        for l in range(n):
            at = slice(per * l, per * (l + 1))
            r.o[l] = jnp.where(keep, r.u[at, :], r.t[at, :])

    dma = pltpu.SemaphoreType.DMA
    whole, part = pltpu.VMEM((rows, D), F32), (rows, half)
    scratch = SimpleNamespace(v=whole, a=whole, t=whole, u=whole, s=pltpu.VMEM((3,) + part, F32), b=pltpu.VMEM((TWO,) + part, F32), send=dma((4,)), recv=dma((4,)))
    outs = SimpleNamespace(o=jax.ShapeDtypeStruct((n, per, D), F32))
    return call("sum_rows", cid, body, ins, outs, scratch, list(vars(ins)) + ["o"]).o


def group_body(x_loc, dy_loc, len_loc, wqkv, wout, wup, bup, wdown, vec):
    n = wqkv.shape[0]
    ids = iter(range(ROWS))
    shape = x_loc.shape
    x = x_loc.reshape(TWO, ROWS, D)
    dy = dy_loc.reshape(TWO, ROWS, D)
    wq = jnp.transpose(wqkv, (0, 2, 3, 4, 1)).reshape(n, QKV_N, D)
    wo = wout.reshape(n, INNER, D)
    info = jnp.concatenate([len_loc, lax.axis_index(TP).reshape(1).astype(jnp.int32)])

    def flat(a):
        return a.reshape(TOK, a.shape[-1])

    def row(layer, i, bias=None):
        return SimpleNamespace(gain=(layer, i), shift=(layer, i + 1), bias=bias)

    ln2, bias1, bias2 = TWO, 4, 5
    saved = [SimpleNamespace() for _ in range(n)]
    (r,) = fused("first", next(ids), FIRST, config(N_FIRST, dict(in0=x, wb=wq, vec=vec), row(0, 0), ag=(QKV, 0)))
    s = saved[0]
    s.x, s.a, s.qkv = x, r.full, r.res
    for l in range(n):
        s = saved[l]
        s.ctx = attn_fwd(info, s.qkv, SEQS)
        arrays = dict(lhs1=s.ctx, wa=wo, wb=wup, in0=s.x, vec=vec, b_up=bup)
        stages = [config(N_LN, arrays, row(l, ln2, (l, bias1)), rs=(l, INNER, False), ag=(UP, l))]
        if l + 1 < n:
            taken = (("lhs1", "res"), ("in0", "out0"))
            arrays = dict(wa=wdown, wb=wq, vec=vec)
            stages.append(config(N_LN, arrays, row(l + 1, 0, (l, bias2)), rs=(l, FF, False), ag=(QKV, l + 1), taken=taken))
        r, *more = fused(f"fwd_{l}", next(ids), MID, *stages)
        s.hid, s.act, s.slope, s.m_t, s.act_t = r.out0, r.res, r.slope, r.full_t, r.res_t
        for r in more:
            s = saved[l + 1]
            s.x, s.a, s.qkv = r.out0, r.full, r.res
    s = saved[n - 1]
    arrays = dict(lhs1=s.act, wa=wdown, wb=wdown, in0=s.hid, vec=vec, src=dy, slope=s.slope)
    (r,) = fused("top", next(ids), TOP, config(N_RES, arrays, row(0, 0, (n - 1, bias2)), rs=(n - 1, FF, False), ag=(DACT, n - 1)))
    y, d_cur, d_full, d_pre = r.out0, r.out1, r.full, r.res
    g_bup, rows, puts, stacks = [r.bup], [], [(y.reshape(KT, D), 4, 0, 1)], [None] * 6
    mlp_plans = ((3, 1, 0, 4, 1, 0, 2, 0, 2, 2, 3, 0, 2), (3, 1, 0, 6, 1, 0, 2, 0, 2, 2, 3, 0, 2), (3, 1, 0, 5, 1, 0, 2, 0, 2, 2, 2, 0, 1))
    attn_plans = ((2, 2), (2, 1, 0, 4, 1, 0, 1, 1, 1, 1, 4, 1, 2), (4, 2, 0, 6, 2, 0, 1, 1, 1, 1, 2, 1, 1))
    for l in reversed(range(n)):
        s = saved[l]
        arrays = dict(lhs1=d_pre, wa=wup, wb=wo, in0=s.hid, in1=d_cur, vec=vec, f0l=s.act_t, f0r=flat(d_full), f1l=s.m_t, f1r=flat(d_pre))
        common = dict(fills=((FF, D, TWO), (D, FF, 1)), bm=BM + BM, flat_t=True, plan=mlp_plans[l])
        (r,) = fused(f"d_mlp_{l}", next(ids), MID, config(N_BWD2, arrays, row(l, ln2), rs=(l, FF, True), ag=(DCTX, l), **common))
        d_hid, d_attn, v3 = r.out0, r.full, r.vo
        puts += [(r.g0, 3, l, n), (r.g1, TWO, l, n)]
        d_qkv = attn_bwd(info, s.qkv, r.res, puts, stacks, TWO if l else 1)
        arrays = dict(lhs1=d_qkv, wa=wq, in0=s.x, in1=d_hid, vec=vec, f0l=flat(s.ctx), f0r=flat(d_attn), f1l=flat(d_qkv), f1r=flat(s.a))
        common = dict(rs=(l, QKV_N, False), fills=((INNER, D, 1), (QKV_N, D, 3)), plan=attn_plans[l])
        if l:
            arrays.update(wb=wdown, slope=saved[l - 1].slope)
            common.update(ag=(DACT, l - 1))
        (r,) = fused(f"d_attn_{l}", next(ids), MID if l else LAST, config(N_BWD1, arrays, row(l, 0), **common))
        if l:
            g_bup.append(r.bup)
            d_full, d_pre = r.full, r.res
        puts = [(r.g0, 1, l, n), (r.g1, 0, l, n)]
        rows.append((r.vo, v3))
        d_cur = r.out0
    put_last(puts + [(d_cur.reshape(KT, D), 5, 0, 1)], stacks)
    g_vec = sum_rows(rows[::-1], next(ids))
    g_qkv = jnp.transpose(stacks[0].reshape(n, 3, HEADS, HD, D), (0, 4, 1, 2, 3))
    g_out = stacks[1].reshape(n, HEADS, HD, D)
    return stacks[4].reshape(shape), stacks[5].reshape(shape), g_qkv, g_out, stacks[2], jnp.concatenate(g_bup[::-1]), stacks[3], g_vec


def solution(mesh):
    act_spec = P(DP, TP, None)
    in_specs = (act_spec, act_spec, P(DP), P(None, None, None, TP, None), P(None, TP, None, None), P(None, None, TP), P(None, TP), P(None, TP, None), P())
    out_specs = (act_spec, act_spec, P(DP, None, None, TP, None), P(DP, TP, None, None), P(DP, None, TP), P(DP, TP), P(DP, TP, None), P(DP, None, None))
    return jax.shard_map(group_body, mesh=mesh, in_specs=in_specs, out_specs=out_specs, check_vma=False)
```

```python
from functools import partial
from types import SimpleNamespace

import jax
import jax.numpy as jnp
from jax import lax
from jax.experimental import pallas as pl
from jax.experimental.pallas import tpu as pltpu
from jax.sharding import PartitionSpec as P

TP, DP = "tp", "dp"
D, FF, INNER, QKV_N = 3072, 1536, 384, 1152
ROWS, HALF_ROWS, GROUP = 128, 64, 16
LANES, SUBL = 128, 8
A, B = HALVES = range(2)
PEERS = 8
TOK = len(HALVES) * PEERS * ROWS
HEADS, HD = 4, 96
SEQS, ALL_SEQS = 4, 16
BM, BN, KT = 384, 512, 256
BF, F32 = jnp.bfloat16, jnp.float32
ANY = pl.ANY
VMEM_LIMIT = 66_900_000
GELU_C, GELU_D = 0.7978845608028654, 0.044715
EPS, NEG = 1e-5, -1e30
ONE, TWO, HALF = 1.0, 2, 0.5
OWN, XN, YN, FAR = PAIRS = range(4)
Q_ORDER = (FAR, XN, YN, OWN)
R_X, R_Y, R_FAR = 2, 4, 6
X_FAR, Y_FAR, X_RAW, Y_RAW, X_SUM, Y_SUM, N_RS = range(4, 11)
G_CORE, G_XT, G_XB, G_YB, G_YT, G_FT, G_FB, G_C3, G_C5, G_C7, N_AG = range(11)
CROSSING = {XN: G_C3, YN: G_C5, FAR: G_C7}
FIRST, MID, TOP, LAST = range(4)
N_FIRST, N_LN, N_RES, N_BWD2, N_BWD1 = range(5)
QKV, UP, DACT, DCTX = range(4)
WIDTH = (QKV_N, FF, FF, INNER)
PER = 6
ALL = 1 << 20


def dims(lhs, rhs, lc, rc):
    return lax.dot_general(lhs, rhs, (((lc,), (rc,)), ((), ())), preferred_element_type=F32)


def peers():
    me = lax.axis_index(TP)
    dp = lax.axis_index(DP)

    def flip(bit):
        return me + bit - TWO * bit * lax.rem(lax.div(me, bit), TWO)

    return [(dp, flip(1 << k)) for k in range(3)]


def say_here(devices):
    for dev in devices:
        pl.semaphore_signal(pltpu.get_barrier_semaphore(), inc=1, device_id=dev, device_id_type=pl.DeviceIdType.MESH)


def await_peers(n=3):
    pl.semaphore_wait(pltpu.get_barrier_semaphore(), n)


def remote(src, dst, send, recv, dev):
    return pltpu.make_async_remote_copy(src_ref=src, dst_ref=dst, send_sem=send, recv_sem=recv, device_id=dev, device_id_type=pl.DeviceIdType.MESH)


class Pieces:
    def __init__(self, src, dst, sem, n):
        self.src, self.dst, self.sem, self.n = src, dst, sem, n

    def start(self):
        src, dst = self.src, self.dst
        step = src.shape[-2] // self.n
        for i in range(self.n):
            at = pl.ds(i * step, step)
            if len(src.shape) == 3:
                for j in range(src.shape[0]):
                    pltpu.make_async_copy(src.at[j, at], dst.at[j, at], self.sem).start()
            else:
                pltpu.make_async_copy(src.at[at], dst.at[at], self.sem).start()
        return self

    def wait(self):
        pltpu.make_async_copy(self.src, self.dst, self.sem).wait()


def call(name, cid, body, ins, outs, scratch, small):
    names = [list(vars(a)) for a in (ins, outs, scratch)]

    def kernel(*refs):
        body(SimpleNamespace(**dict(zip(sum(names, []), refs))))

    def spec(n):
        return pl.BlockSpec(memory_space=pltpu.VMEM if n in small else ANY)

    res = pl.pallas_call(
        kernel,
        name=name,
        out_shape=list(vars(outs).values()),
        in_specs=[spec(n) for n in names[0]],
        out_specs=[spec(n) for n in names[1]],
        scratch_shapes=list(vars(scratch).values()),
        compiler_params=pltpu.CompilerParams(vmem_limit_bytes=VMEM_LIMIT, collective_id=cid, has_side_effects=True),
    )(*vars(ins).values())
    return SimpleNamespace(**dict(zip(names[1], res)))


def config(norm, arrays, vec, rs=None, ag=None, fills=(), bm=BM, flat_t=False, plan=(), taken=(), layers=0):
    return SimpleNamespace(norm=norm, arrays=arrays, vec=vec, rs=rs, ag=ag, fills=fills, bm=bm, flat_t=flat_t, plan=plan, taken=dict(taken), layers=layers)


def declare(c):
    outs, sc = SimpleNamespace(), SimpleNamespace()
    dma = pltpu.SemaphoreType.DMA
    n_in = TWO if c.norm in (N_BWD2, N_BWD1) else 1
    n_acc = {N_BWD2: 4, N_BWD1: TWO}.get(c.norm, 0)
    shard = jax.ShapeDtypeStruct((TWO, ROWS, D), F32)
    if c.norm != N_FIRST:
        outs.out0 = shard
        sc.nout = pltpu.VMEM((ROWS, D), F32)
    if c.norm == N_RES:
        outs.out1 = shard
        sc.nout1 = pltpu.VMEM((ROWS, D), F32)
    sc.nin = pltpu.VMEM((n_in, ROWS, D), F32)
    sc.nsem = dma((n_in + TWO,))
    if n_acc:
        outs.vo = jax.ShapeDtypeStruct((SUBL, D), F32)
        sc.acc = pltpu.VMEM((n_acc, SUBL, D), F32)
    if c.rs:
        k1 = c.rs[1]
        tile1 = 1024
        tiles1 = D // tile1
        halves = (TWO, ROWS, D)
        sc.w1 = pltpu.VMEM((D, k1) if c.rs[2] else (k1, D), BF)
        sc.lhs = pltpu.VMEM((TWO, TWO, ROWS, k1), BF)
        sc.own = pltpu.VMEM((TWO, len(PAIRS), ROWS, D), BF)
        sc.snd = pltpu.VMEM((len(PAIRS), ROWS, D), BF)
        sc.drx = pltpu.VMEM((TWO, len(PAIRS), ROWS, D), BF)
        sc.hx = pltpu.VMEM((TWO, HALF_ROWS, D), BF)
        sc.hy = pltpu.VMEM((TWO, HALF_ROWS, D), BF)
        sc.rx = pltpu.VMEM(halves, BF)
        sc.ry = pltpu.VMEM(halves, BF)
        sc.w1_sem = dma((tiles1,))
        sc.lhs_sem = dma((TWO,))
        sc.rs_send = dma((TWO, N_RS))
        sc.rs_recv = dma((TWO, N_RS))
        sc.far_send = dma((tiles1, len(PAIRS)))
        sc.far_recv = dma((tiles1, len(PAIRS)))
    if c.ag:
        what = c.ag[0]
        n2 = WIDTH[what]
        outs.full = jax.ShapeDtypeStruct((TWO, PEERS, ROWS, D), BF)
        outs.res = jax.ShapeDtypeStruct((TWO, PEERS, ROWS, n2), BF)
        pairs_of = (TWO, TWO, ROWS, n2)
        sc.w2 = pltpu.VMEM((D, n2) if what == UP else (n2, D), BF)
        sc.g = pltpu.VMEM((TWO, ROWS, D), BF)
        sc.agin = pltpu.VMEM((TWO, TWO, ROWS, D), BF)
        sc.last = pltpu.VMEM((TWO, ROWS, D), BF)
        sc.w2_sem = dma
        sc.g_sem = dma((TWO,))
        sc.agin_sem = dma((TWO,))
        sc.last_sem = dma((TWO,))
        sc.ag_send = dma((TWO, N_AG))
        sc.ag_recv = dma((TWO, N_AG))
        sc.res_st = pltpu.VMEM(pairs_of, BF)
        sc.res_sem = dma((TWO,))
        if what == UP:
            outs.slope = jax.ShapeDtypeStruct((TWO, PEERS, ROWS, n2), F32)
            outs.full_t = jax.ShapeDtypeStruct((D, TOK), BF)
            outs.res_t = jax.ShapeDtypeStruct((n2, TOK), BF)
            sc.full_ts = pltpu.VMEM((D, KT), BF)
            sc.res_ts = pltpu.VMEM((n2, KT), BF)
            sc.t_sem = dma((TWO,))
        if what == DACT:
            outs.bup = jax.ShapeDtypeStruct((1, n2), F32)
            sc.bacc = pltpu.VMEM((SUBL, n2), F32)
        if what in (UP, DACT):
            sc.slope_st = pltpu.VMEM(pairs_of, F32)
            sc.slope_sem = dma((TWO,))
    if c.fills:
        slots = TWO if c.flat_t else max(f[2] for f in c.fills)
        sc.f_at = pltpu.VMEM((slots, c.bm, TOK), BF)
        ahead = 3 if c.flat_t or not c.ag else TWO
        sc.f_rhs = pltpu.VMEM((ahead, TOK, BN), BF)
        sc.f_out = pltpu.VMEM((TWO, c.bm, BN), BF)
        if not c.flat_t:
            sc.f_lhs = pltpu.VMEM((TOK, c.bm), BF)
        sc.fl_sem = dma((slots,))
        sc.fr_sem = dma((ahead,))
        sc.fo_sem = dma((TWO,))
        outs.g0 = jax.ShapeDtypeStruct(c.fills[0][:2], BF)
        outs.g1 = jax.ShapeDtypeStruct(c.fills[1][:2], BF)
    if c.layers:
        outs.row_o = jax.ShapeDtypeStruct((c.layers, PER, D), F32)
        rows = -(-PER * c.layers // SUBL) * SUBL
        for k, n in (("e", rows), ("l", SUBL)):
            half = (n, D // TWO)
            parts = dict(v=pltpu.VMEM((n, D), F32), a=pltpu.VMEM((n, D), F32), t=pltpu.VMEM((n, D), F32), s=pltpu.VMEM((3,) + half, F32), b=pltpu.VMEM((TWO,) + half, F32))
            parts.update(send=dma((4,)), recv=dma((4,)))
            for p, x in parts.items():
                setattr(sc, k + p, x)
    return outs, sc


def stage(c, r):
    norm, vec, rs, ag, fills, bm, flat_t, plan = c.norm, c.vec, c.rs, c.ag, c.fills, c.bm, c.flat_t, c.plan
    n_in = TWO if norm in (N_BWD2, N_BWD1) else 1
    n_acc = {N_BWD2: 4, N_BWD1: TWO}.get(norm, 0)
    if rs:
        k1 = rs[1]
        tile1 = 1024
        tiles1 = D // tile1
    if ag:
        what = ag[0]
        n2 = WIDTH[what]
    core, px, py = peers()
    waiting = [1] if c.first else []
    late = () if c.first else (4, 5)

    def await_once():
        while waiting:
            waiting.pop()
            await_peers()

    def begin(src, dst, sem, n=4):
        return Pieces(src, dst, sem, n).start()

    def norm_load(h):
        some = (r.in0, r.in1) if n_in == TWO else (r.in0,)
        return [begin(x.at[h], r.nin.at[i], r.nsem.at[i]) for i, x in enumerate(some)]

    def vrow(row):
        return r.vec[row[0], pl.ds(row[1], 1), :]

    out_copy = []

    def mean(x):
        return jnp.sum(x, axis=-1, keepdims=True) * (ONE / D)

    def norm_half(h, loads):
        for c in loads:
            c.wait()
        while out_copy:
            out_copy.pop().wait()

        def rows(i, carry):
            at = pl.ds(pl.multiple_of(i * GROUP, GROUP), GROUP)
            x = r.nin[0, at, :]
            if rs:
                o = r.own[h, OWN, at, :].astype(F32) + r.rx[h, at, :].astype(F32) + r.ry[h, at, :].astype(F32)
                o = o.astype(BF).astype(F32)
            if norm in (N_LN, N_RES):
                x = x + o + vrow(vec.bias)
                r.nout[at, :] = x
            if norm == N_RES:
                r.nout1[at, :] = r.g[h, at, :].astype(F32)
                return carry
            cen = x - mean(x)
            rstd = lax.rsqrt(mean(cen * cen) + EPS)
            if norm in (N_FIRST, N_LN):
                r.g[h, at, :] = (cen * rstd * vrow(vec.gain) + vrow(vec.shift)).astype(BF)
                return carry
            xh = cen * rstd
            dxh = o * vrow(vec.gain)
            base = r.nin[1, at, :]
            res = base + rstd * (dxh - mean(dxh) - xh * mean(dxh * xh))
            r.nout[at, :] = res
            if ag:
                r.g[h, at, :] = res.astype(BF)
            sums = [o * xh, o] + ([res, base] if norm == N_BWD2 else [])
            for j, v in enumerate(sums):
                r.acc[j] += v[:SUBL] + v[SUBL:]
            return carry

        lax.fori_loop(0, ROWS // GROUP, rows, 0)
        if norm != N_FIRST:
            out_copy.append(begin(r.nout, r.out0.at[h], r.nsem.at[n_in]))
        if norm == N_RES:
            out_copy.append(begin(r.nout1, r.out1.at[h], r.nsem.at[n_in + 1]))

    top, bot = pl.ds(0, HALF_ROWS), pl.ds(HALF_ROWS, HALF_ROWS)
    if rs:
        seq = [(h, q) for h in HALVES for q in Q_ORDER]
        lhs_loads, rs_copy, far_copy, w1_loads = {}, {}, {}, []
        own = r.own

        def w1_load():
            for n in range(tiles1):
                at = pl.ds(n * tile1, tile1)
                src, dst = r.wa.at[rs[0]], r.w1
                src, dst = (src.at[at], dst.at[at]) if rs[2] else (src.at[:, at], dst.at[:, at])
                w1_loads.append(begin(src, dst, r.w1_sem.at[n]))

        def lhs_load(i):
            h, q = seq[i]
            s = i % TWO
            lhs_loads[i] = begin(r.lhs1.at[h, pl.ds(TWO * q, TWO)], r.lhs.at[s], r.lhs_sem.at[s])

        def lhs_late():
            for i in late:
                lhs_load(i)

        def rs_start(h, j, src, dst, dev):
            c = remote(src, dst, r.rs_send.at[h, j], r.rs_recv.at[h, j], dev)
            c.start()
            rs_copy[h, j] = c

        def far_start(n, j, src, dst, dev):
            c = remote(src, dst, r.far_send.at[n, j], r.far_recv.at[n, j], dev)
            c.start()
            far_copy[n, j] = c

        def add_into(dst, src, n, at_cols=slice(None)):
            def rows(i, carry):
                at = pl.ds(pl.multiple_of(i * GROUP, GROUP), GROUP)
                dst[at, at_cols] = (dst[at, at_cols].astype(F32) + src[at, at_cols].astype(F32)).astype(BF)
                return carry

            lax.fori_loop(0, n // GROUP, rows, 0)

        def far_merge(n, send):
            cols = pl.ds(n * tile1, tile1)
            far_copy[n, 0].wait_recv()
            add_into(own.at[A, FAR], r.drx.at[A, FAR], ROWS, cols)
            if send:
                far_sends(n)

        def far_sends(n):
            cols = pl.ds(n * tile1, tile1)
            far_start(n, 1, own.at[A, FAR, top, cols], r.hx.at[A, :, cols], px)
            far_start(n, 2, own.at[A, FAR, bot, cols], r.hy.at[A, :, cols], py)

        def product_in(i, between=None, send=True):
            h, q = seq[i]
            s = i % TWO
            lhs_loads[i].wait()
            if i == len(PAIRS):
                for n in range(tiles1):
                    far_copy[n, 0].wait_send()
            elif h == B:
                rs_copy[A, q].wait_send()

            def tile(n, carry):
                at = pl.ds(pl.multiple_of(n * tile1, tile1), tile1)
                x = r.lhs[s].reshape(TWO * ROWS, k1)
                y = dims(x, r.w1[at, :], 1, 1) if rs[2] else dims(x, r.w1[:, at], 1, 0)
                y = y.astype(BF)
                own[h, q, :, at] = y[:ROWS]
                r.snd[q, :, at] = y[ROWS:]
                return carry

            if i == 0:
                for n in range(tiles1):
                    cols = pl.ds(n * tile1, tile1)
                    w1_loads[n].wait()
                    tile(n, 0)
                    if n == 0:
                        await_once()
                    far_start(n, 0, r.snd.at[FAR, :, cols], r.drx.at[A, FAR, :, cols], core)
                    if n:
                        far_merge(n - 1, send)
            else:
                tile(0, 0)
                if between:
                    between()
                lax.fori_loop(1, tiles1, tile, 0)
            if i + TWO < len(seq) and i + TWO not in late:
                lhs_load(i + TWO)
            if i:
                rs_start(h, q, r.snd.at[q], r.drx.at[h, q], core)

        def merge(h, q):
            rs_copy[h, q].wait_recv()
            add_into(own.at[h, q], r.drx.at[h, q], ROWS)

        def first_sends(h, q):
            if q == FAR:
                rs_start(h, X_FAR, own.at[h, q, top], r.hx.at[h], px)
                rs_start(h, Y_FAR, own.at[h, q, bot], r.hy.at[h], py)
            if q == XN:
                rs_start(h, X_RAW, own.at[h, q, top], r.rx.at[h, top], px)
            if q == YN:
                rs_start(h, Y_RAW, own.at[h, q, bot], r.ry.at[h, bot], py)

        def far_wait(h, j):
            if h == A:
                for n in range(tiles1):
                    far_copy[n, 1 + j].wait_recv()
            else:
                rs_copy[h, X_FAR + j].wait_recv()

        def third_sends(h):
            far_wait(h, 1)
            add_into(own.at[h, XN, bot], r.hy.at[h], HALF_ROWS)
            rs_start(h, X_SUM, own.at[h, XN, bot], r.rx.at[h, bot], px)
            far_wait(h, 0)
            add_into(own.at[h, YN, top], r.hx.at[h], HALF_ROWS)
            rs_start(h, Y_SUM, own.at[h, YN, top], r.ry.at[h, top], py)

        def rs_done(h):
            for j in (X_RAW, Y_RAW, X_SUM, Y_SUM):
                rs_copy[h, j].wait_recv()

        def step(i, send=True):
            def between():
                h, q = seq[i - 1]
                if i == 1:
                    far_merge(tiles1 - 1, send)
                    return
                merge(h, q)
                if send:
                    first_sends(h, q)

            product_in(i, between if i % len(PAIRS) else None, send)

    if ag:
        full = r.full
        ag_copy, g_copy, ready_loads, res_out, w2_copy, last_copy = {}, {}, {}, {}, [], []

        def w2_load():
            w2_copy.append(begin(r.wb.at[ag[1]], r.w2, r.w2_sem, PEERS))

        def ag_start(h, j, src, dst, dev):
            c = remote(src, dst, r.ag_send.at[h, j], r.ag_recv.at[h, j], dev)
            c.start()
            ag_copy[h, j] = c

        def own_sends(h):
            g = r.g
            ag_start(h, G_XT, g.at[h, top], full.at[h, R_X, top], px)
            ag_start(h, G_YB, g.at[h, bot], full.at[h, R_Y, bot], py)
            ag_start(h, G_XB, g.at[h, bot], full.at[h, R_X, bot], px)
            ag_start(h, G_YT, g.at[h, top], full.at[h, R_Y, top], py)
            ag_start(h, G_CORE, g.at[h], full.at[h, 1], core)
            g_copy[h] = begin(g.at[h], full.at[h, 0], r.g_sem.at[h])

        def far_place(h, other):
            return full.at[h, R_FAR + other] if h == A else r.last.at[other]

        def forward(h):
            ag_copy[h, G_XT].wait_recv()
            ag_start(h, G_FT, full.at[h, R_X, top], far_place(h, 0).at[top], py)
            ag_copy[h, G_YB].wait_recv()
            ag_start(h, G_FB, full.at[h, R_Y, bot], far_place(h, 0).at[bot], px)

        def cross(h):
            ag_copy[h, G_XB].wait_recv()
            ag_start(h, G_C3, full.at[h, R_X], full.at[h, R_X + 1], core)
            ag_copy[h, G_YT].wait_recv()
            ag_start(h, G_C5, full.at[h, R_Y], full.at[h, R_Y + 1], core)

        def cross_far(h):
            ag_copy[h, G_FT].wait_recv()
            ag_copy[h, G_FB].wait_recv()
            ag_start(h, G_C7, far_place(h, 0), far_place(h, 1), core)
            if h == B:
                last_copy.append(begin(r.last.at[0], full.at[h, R_FAR], r.last_sem.at[0]))

        def ready(h, q):
            s = (len(PAIRS) * h + (OWN, XN, YN, FAR).index(q)) % TWO
            pair = pl.ds(TWO * q, TWO)
            loads = []
            if what == DACT:
                loads.append(begin(r.slope.at[h, pair], r.slope_st.at[s], r.slope_sem.at[s]))
            if q == OWN:
                g_copy.pop(h).wait()
                ag_copy[h, G_CORE].wait_recv()
            else:
                ag_copy[h, CROSSING[q]].wait_recv()
            if (h, q) == (B, FAR):
                last_copy.append(begin(r.last.at[1], full.at[h, R_FAR + 1], r.last_sem.at[1]))
            else:
                loads.append(begin(full.at[h, pair], r.agin.at[s], r.agin_sem.at[s]))
            ready_loads[h, q] = (s, loads)

        flipped = {}

        def flip(src, stage, dst, i):
            if i in flipped:
                flipped[i].wait()

            def block(k, carry):
                at = pl.ds(pl.multiple_of(k * KT, KT), KT)
                stage[at, :] = src[:, :, at].reshape(KT, KT).T
                return carry

            lax.fori_loop(0, stage.shape[0] // KT, block, 0)
            flipped[i] = begin(stage, dst, r.t_sem.at[i])

        to_flip = []

        def flip_all():
            while to_flip:
                flip(*to_flip.pop(0))

        def product(h, q):
            if (h, q) not in ready_loads:
                ready(h, q)
            s, loads = ready_loads.pop((h, q))
            pair = pl.ds(TWO * q, TWO)
            while w2_copy:
                w2_copy.pop().wait()
            for c in res_out.pop(s, ()):
                c.wait()
            for c in loads:
                c.wait()
            nt = BM if what in (QKV, DCTX) else BN

            def tile(n, carry):
                at = pl.ds(pl.multiple_of(n * nt, nt), nt)
                x = r.last[...] if (h, q) == (B, FAR) else r.agin[s]
                x = x.reshape(TWO * ROWS, D)
                y = dims(x, r.w2[:, at], 1, 0) if what == UP else dims(x, r.w2[at, :], 1, 1)
                if what == UP:
                    u = y + r.b_up[pl.ds(ag[1], 1), at]
                    t = jnp.tanh(GELU_C * (u + GELU_D * (u * u * u)))
                    slope = HALF * (ONE + t) + (HALF * GELU_C) * u * (ONE - t * t) * (ONE + (3 * GELU_D) * (u * u))
                    r.slope_st[s, :, :, at] = slope.reshape(TWO, ROWS, nt)
                    y = u * (HALF * (ONE + t))
                if what == DACT:
                    y = y.astype(BF).astype(F32) * r.slope_st[s, :, :, at].reshape(TWO * ROWS, nt)
                    r.bacc[:, at] += jnp.sum(y.reshape(-1, SUBL, nt), axis=0)
                r.res_st[s, :, :, at] = y.astype(BF).reshape(TWO, ROWS, nt)
                return carry

            if n2 == nt:
                tile(0, 0)
            else:
                lax.fori_loop(0, n2 // nt, tile, 0)
            res_out[s] = [begin(r.res_st.at[s], r.res.at[h, pair], r.res_sem.at[s])]
            if what == UP:
                res_out[s].append(begin(r.slope_st.at[s], r.slope.at[h, pair], r.slope_sem.at[s]))
                cols = pl.ds((h * PEERS + TWO * q) * ROWS, KT)
                gathered = r.last if (h, q) == (B, FAR) else r.agin.at[s]
                to_flip.append((gathered, r.full_ts, r.full_t.at[:, cols], 0))
                to_flip.append((r.res_st.at[s], r.res_ts, r.res_t.at[:, cols], 1))

    jobs = []
    if fills:
        refs = ((r.f0l, r.f0r, r.g0), (r.f1l, r.f1r, r.g1))
        jobs = [SimpleNamespace(lhs=f[0], rhs=f[1], out=f[2], blocks=c[0] // bm // c[2], tiles=c[1] // BN, sub=c[2], done=0) for f, c in zip(refs, fills)]
        slots = r.f_rhs.shape[0]
        for j in jobs:
            j.fetches = j.tiles if j.tiles <= slots else j.blocks * j.tiles

    def lhs_copy(j, k):
        at = pl.ds(pl.multiple_of(k * bm, bm), bm)
        if flat_t:
            s = lax.rem(k, TWO)
            return Pieces(j.lhs.at[at], r.f_at.at[s], r.fl_sem.at[s], PEERS)
        return Pieces(j.lhs.at[:, at], r.f_lhs, r.fl_sem.at[0], PEERS)

    def rhs_copy(j, v):
        s = lax.rem(v, slots)
        return Pieces(j.rhs.at[:, pl.ds(pl.multiple_of(lax.rem(v, j.tiles) * BN, BN), BN)], r.f_rhs.at[s], r.fr_sem.at[s], PEERS)

    def put_copy(j, u):
        s, v = lax.rem(u, TWO), lax.div(u, j.sub)
        row = lax.div(v, j.tiles) * j.sub + lax.rem(u, j.sub)
        dst = j.out.at[pl.ds(pl.multiple_of(row * bm, bm), bm), pl.ds(pl.multiple_of(lax.rem(v, j.tiles) * BN, BN), BN)]
        return Pieces(r.f_out.at[s], dst, r.fo_sem.at[s], 3)

    def job_begin(j):
        lhs_copy(j, jnp.int32(0)).start()
        if flat_t:
            lhs_copy(j, jnp.int32(1)).start()
        for v in range(slots - 1):
            rhs_copy(j, jnp.int32(v)).start()

    def fill(n):
        while n > 0 and jobs:
            j = jobs[0]
            rhs_all = j.blocks * j.tiles
            count = rhs_all * j.sub

            def unit(u, carry):
                v, b, s = lax.div(u, j.sub), lax.rem(u, j.sub), lax.rem(u, TWO)
                vs, t = lax.rem(v, slots), lax.rem(v, j.tiles)
                k = lax.div(v, j.tiles) * j.sub + b

                @pl.when(t == 0)
                def _():
                    lhs_copy(j, k).wait()
                    if flat_t:
                        return
                    for i in range(TOK // KT):
                        r.f_at[b, :, i * KT : (i + 1) * KT] = r.f_lhs[i * KT : (i + 1) * KT, :].T

                    @pl.when(k + 1 < j.blocks * j.sub)
                    def _():
                        lhs_copy(j, k + 1).start()

                @pl.when((b == 0) & (v < j.fetches))
                def _():
                    rhs_copy(j, v).wait()

                    @pl.when(v + (slots - 1) < j.fetches)
                    def _():
                        rhs_copy(j, v + (slots - 1)).start()

                @pl.when(u >= TWO)
                def _():
                    put_copy(j, u - TWO).wait()

                r.f_out[s] = dims(r.f_at[lax.rem(k, TWO) if flat_t else b], r.f_rhs[vs], 1, 0).astype(BF)
                put_copy(j, u).start()
                if flat_t:

                    @pl.when((t == j.tiles - 1) & (k + TWO < j.blocks * j.sub))
                    def _():
                        lhs_copy(j, k + TWO).start()

                return carry

            upto = min(count, j.done + n)
            n -= upto - j.done
            lax.fori_loop(j.done, upto, unit, 0)
            j.done = upto
            if upto == count:
                for u in (count - TWO, count - 1):
                    put_copy(j, jnp.int32(u)).wait()
                jobs.pop(0)
                if jobs:
                    job_begin(jobs[0])

    steps = list(plan)

    def fill_next():
        if steps:
            fill(steps.pop(0))

    def prologue():
        if rs:
            lhs_load(0)
            w1_load()
            lhs_load(1)
        if ag:
            w2_load()
        if jobs:
            job_begin(jobs[0])

    def clear():
        for j in range(n_acc):
            r.acc[j] = jnp.zeros((SUBL, D), F32)
        if ag and what == DACT:
            r.bacc[...] = jnp.zeros((SUBL, n2), F32)

    def rs_sent():
        for (h, j), x in rs_copy.items():
            if h == B or j > 3:
                x.wait_send()
        for (n, j), x in far_copy.items():
            if j:
                x.wait_send()
        rs_copy.clear()
        far_copy.clear()

    def rows_out():
        while out_copy:
            out_copy.pop().wait()

    def res_done():
        for s in list(res_out):
            for x in res_out.pop(s):
                x.wait()

    def end():
        for j in range(n_acc):
            r.vo[pl.ds(j, 1), :] = jnp.sum(r.acc[j], axis=0, keepdims=True)
        if n_acc:
            r.vo[n_acc:, :] = jnp.zeros((SUBL - n_acc, D), F32)
        if ag and what == DACT:
            r.bup[...] = jnp.sum(r.bacc[...], axis=0, keepdims=True)
        rows_out()
        if rs:
            rs_sent()
        if ag:
            for x in ag_copy.values():
                x.wait_send()
            res_done()
            for x in last_copy + list(flipped.values()):
                x.wait()

    return SimpleNamespace(**locals())


SHARED = ("own", "snd", "drx", "hx", "hy", "rx", "ry", "nin", "nout", "agin")


def fused(name, cid, kind, *stages):
    ins, outs, scratch, small, views = SimpleNamespace(), SimpleNamespace(), SimpleNamespace(), [], []
    shared = SHARED + (("res_st", "slope_st") if kind == TOP else ("g", "last"))
    for i, c in enumerate(stages):
        c.first = i == 0
        c_outs, c_sc = declare(c)
        view = {}
        for group, names in ((ins, c.arrays), (outs, vars(c_outs)), (scratch, vars(c_sc))):
            for n, x in names.items():
                view[n] = f"{n}{0 if group is scratch and n in shared else i}"
                setattr(group, view[n], x)
                if group is not scratch and (n in ("vec", "b_up", "vo", "bup") or n.startswith("row_")):
                    small.append(view[n])
        view.update({n: f"{prev}{i - 1}" for n, prev in c.taken.items()})
        views.append(view)
    if kind == TOP:
        del scratch.w21
        views[1]["w2"] = views[1]["w1"]
    elif len(stages) > 1:
        del scratch.w10
        views[0]["w1"] = views[1]["w2"]

    def body(refs):
        refs = vars(refs)
        st = [stage(c, SimpleNamespace(**{n: refs[x] for n, x in v.items()})) for c, v in zip(stages, views)]
        if kind == MID and len(st) > 1:
            st[0].r.w1 = st[0].r.w1.at[pl.ds(0, stages[0].rs[1])]
        say_here(peers())
        PROGRAMS[kind](*st)

    res = call(name, cid, body, ins, outs, scratch, small)
    return [SimpleNamespace(**{n: getattr(res, x) for n, x in v.items() if hasattr(res, x) and n not in c.taken}) for c, v in zip(stages, views)]


def both_halves(s, loads):
    for i in range(len(PAIRS)):
        s.step(i)
    s.merge(A, OWN)
    s.third_sends(A)
    second_half(s, loads)


def second_half(s, loads):
    for i in range(len(PAIRS), len(s.seq)):
        s.step(i)
    s.merge(B, OWN)
    s.fill_next()
    s.rs_done(A)
    s.norm_half(A, loads)


def products(s, h):
    s.cross(h)
    s.fill_next()
    s.ready(h, XN)
    s.ready(h, YN)
    s.product(h, XN)
    if h == A:
        s.flip_all()
    s.product(h, YN)
    if h == A:
        s.flip_all()
    s.fill_next()
    s.cross_far(h)


def first_program(s):
    s.prologue()
    loads = s.norm_load(A)
    s.norm_half(A, loads)
    loads = s.norm_load(B)
    s.await_once()
    s.own_sends(A)
    s.norm_half(B, loads)
    s.product(A, OWN)
    s.forward(A)
    s.own_sends(B)
    s.ready(B, OWN)
    s.product(B, OWN)
    products(s, A)
    s.product(A, FAR)
    s.forward(B)
    products(s, B)
    s.product(B, FAR)
    s.end()


def sum_steps(v, a, t, s, b, send, recv):
    core, px, py = peers()
    half = D // TWO
    mine = pl.ds(pl.multiple_of(lax.rem(lax.axis_index(TP), TWO) * half, half), half)
    copies = []

    def go(src, dst, i, dev):
        x = remote(src, dst, send.at[i], recv.at[i], dev)
        x.start()
        copies.append(x)

    def one():
        go(v, a, 0, core)

    def two():
        copies.pop().wait()
        s[0] = v[:, mine] + a[:, mine]
        go(s.at[0], b.at[0], 1, px)

    def three():
        copies.pop().wait()
        s[1] = s[0] + b[0]
        go(s.at[1], b.at[1], TWO, py)

    def four():
        copies.pop().wait()
        s[TWO] = s[1] + b[1]
        t[:, mine] = s[TWO]
        go(s.at[TWO], t.at[:, mine], 3, core)

    def five():
        copies.pop().wait()

    return one, two, three, four, five


def last_program(s):
    r = s.r
    s.prologue()
    loads = s.norm_load(A)
    s.clear()
    layers = range(s.c.layers)
    r.ev[...] = jnp.zeros(r.ev.shape, F32)
    for l in layers:
        at = PER * l
        if l:
            r.ev[at : at + TWO, :] = getattr(r, f"row_a{l}")[:TWO, :]
        r.ev[at + TWO : at + PER, :] = getattr(r, f"row_b{l}")[: PER - TWO, :]
    early = sum_steps(r.ev, r.ea, r.et, r.es, r.eb, r.esend, r.erecv)
    late = sum_steps(r.lv, r.la, r.lt, r.ls, r.lb, r.lsend, r.lrecv)
    for i in range(len(PAIRS)):
        s.step(i)
        early[i]()
    s.merge(A, OWN)
    s.third_sends(A)
    second_half(s, loads)
    early[-1]()
    loads = s.norm_load(B)
    s.fill_next()
    s.third_sends(B)
    s.fill(ALL)
    s.rs_done(B)
    s.norm_half(B, loads)
    r.lv[...] = jnp.zeros(r.lv.shape, F32)
    for j in range(TWO):
        r.lv[pl.ds(j, 1), :] = jnp.sum(r.acc[j], axis=0, keepdims=True)
    for x in late:
        x()
    for l in layers:
        r.row_o[l] = r.et[PER * l : PER * (l + 1), :]
    r.row_o[0, :TWO, :] = r.lt[:TWO, :]
    s.end()


def to_forward(s, next_loads=None):
    loads = s.norm_load(B)
    s.fill_next()
    s.third_sends(B)
    s.own_sends(A)
    s.fill_next()
    s.product(A, OWN)
    s.flip_all()
    s.fill_next()
    s.rs_done(B)
    s.norm_half(B, loads)
    if next_loads:
        next_loads()
    s.fill_next()
    s.forward(A)
    s.own_sends(B)
    s.fill_next()
    s.product(B, OWN)
    s.flip_all()
    s.fill_next()
    products(s, A)
    s.fill_next()
    s.product(A, FAR)
    s.flip_all()
    s.forward(B)


def to_end(s):
    s.fill_next()
    products(s, B)
    s.fill(ALL)
    s.flip_all()
    s.product(B, FAR)
    s.flip_all()
    s.end()


def mid_program(s, z=None):
    s.prologue()
    loads = s.norm_load(A)
    s.clear()
    both_halves(s, loads)
    if z is None:
        to_forward(s)
        to_end(s)
        return

    def next_loads():
        z.w1_load()
        z.w2_load()

    to_forward(s, next_loads)
    s.res_done()
    s.rows_out()
    s.rs_sent()
    z.lhs_load(0)
    z.lhs_load(1)
    loads = z.norm_load(A)
    z.step(0)
    z.step(1)
    s.cross(B)
    z.step(TWO)
    z.step(3)
    s.ready(B, XN)
    s.ready(B, YN)
    z.merge(A, OWN)
    s.cross_far(B)
    s.product(B, XN)
    s.product(B, YN)
    s.flip_all()
    s.product(B, FAR)
    z.third_sends(A)
    s.flip_all()
    s.res_done()
    z.lhs_late()
    for i in range(len(PAIRS), len(z.seq)):
        z.step(i)
    z.merge(B, OWN)
    z.rs_done(A)
    s.end()
    z.norm_half(A, loads)
    to_forward(z)
    to_end(z)


def top_program(s, z):
    s.prologue()
    loads = s.norm_load(A)
    z.clear()
    both_halves(s, loads)
    srcs = []

    def next_loads():
        z.w1_load()
        srcs.extend(z.begin(z.r.src.at[h], z.r.g.at[h], z.r.g_sem.at[h]) for h in HALVES)

    to_forward(s, next_loads)
    for x in srcs:
        x.wait()
    z.own_sends(A)
    s.res_done()
    s.rows_out()
    s.rs_sent()
    z.lhs_load(0)
    z.lhs_load(1)
    loads = z.norm_load(A)
    z.step(0, False)
    z.step(1, False)
    s.cross(B)
    z.step(TWO, False)
    z.step(3, False)
    s.ready(B, XN)
    s.ready(B, YN)
    z.merge(A, OWN)
    s.cross_far(B)
    s.product(B, XN)
    s.product(B, YN)
    s.flip_all()
    z.forward(A)
    s.product(B, FAR)
    s.flip_all()
    s.end()
    z.own_sends(B)
    z.lhs_late()
    z.product(A, OWN)
    z.ready(B, OWN)
    z.cross(A)
    z.product(B, OWN)
    z.ready(A, XN)
    z.ready(A, YN)
    z.product(A, XN)
    z.product(A, YN)
    z.forward(B)
    z.cross_far(A)
    for n in range(z.tiles1):
        z.far_sends(n)
    z.first_sends(A, XN)
    z.first_sends(A, YN)
    z.product_in(4)
    z.product(A, FAR)
    z.cross(B)
    z.step(5, False)
    z.ready(B, XN)
    z.ready(B, YN)
    z.product(B, XN)
    z.cross_far(B)
    z.product(B, YN)
    z.third_sends(A)
    z.first_sends(B, FAR)
    z.merge(B, XN)
    z.first_sends(B, XN)
    z.product_in(6)
    z.merge(B, YN)
    z.first_sends(B, YN)
    z.product_in(7)
    z.merge(B, OWN)
    z.rs_done(A)
    z.norm_half(A, loads)
    loads = z.norm_load(B)
    z.product(B, FAR)
    z.third_sends(B)
    z.rs_done(B)
    z.norm_half(B, loads)
    z.end()


PROGRAMS = (first_program, mid_program, top_program, last_program)


def positions(me):
    def pos(axis):
        i = lax.broadcasted_iota(jnp.int32, (ROWS, ROWS), axis)
        return lax.bitwise_xor(lax.div(i, GROUP), me) * GROUP + lax.rem(i, GROUP)

    return pos(0), pos(1)


def heads_of(x, part, h):
    at = part * INNER + h * HD
    return x[:, at : at + HD]


def softmax(s):
    e = jnp.exp(s - jnp.max(s, axis=-1, keepdims=True))
    return e * (ONE / jnp.sum(e, axis=-1, keepdims=True))


def attn_fwd_kernel(group, info, qkv, ctx, s_ref, p_ref):
    row, col = positions(info[ALL_SEQS])
    for first in range(0, SEQS, group):
        some = [(i, h) for i in range(first, first + group) for h in range(HEADS)]
        xs = {i: qkv[:, i].reshape(ROWS, QKV_N) for i, _ in some}
        for n, (i, h) in enumerate(some):
            mask = (col <= row) & (col < info[pl.program_id(0) * SEQS + i])
            score = dims(heads_of(xs[i], 0, h), heads_of(xs[i], 1, h), 1, 1) * HD**-HALF
            s_ref[n] = jnp.where(mask, score, NEG)
        p_ref[...] = softmax(s_ref[...]).astype(BF)
        out = {i: [] for i in xs}
        for n, (i, h) in enumerate(some):
            out[i].append(dims(p_ref[n], heads_of(xs[i], TWO, h), 1, 0).astype(BF))
        for i, parts in out.items():
            ctx[:, i] = jnp.concatenate(parts, axis=-1).reshape(PEERS, GROUP, INNER)


def attn_bwd_steps(group, info, qkv, dctx, out, s_ref, dp_ref, p_ref, ds_ref):
    row, col = positions(info[ALL_SEQS])
    for first in range(0, SEQS, group):
        some = [(i, h) for i in range(first, first + group) for h in range(HEADS)]
        xs = {i: (qkv[:, i].reshape(ROWS, QKV_N), dctx[:, i].reshape(ROWS, INNER)) for i, _ in some}
        for n, (i, h) in enumerate(some):
            x, d = xs[i]
            mask = (col <= row) & (col < info[pl.program_id(0) * SEQS + i])
            score = dims(heads_of(x, 0, h), heads_of(x, 1, h), 1, 1) * HD**-HALF
            s_ref[n] = jnp.where(mask, score, NEG)
            dp_ref[n] = dims(heads_of(d, 0, h), heads_of(x, TWO, h), 1, 1).astype(BF)
        p = softmax(s_ref[...])
        dp = dp_ref[...].astype(F32)
        p_ref[...] = p.astype(BF)
        ds = p * (dp - jnp.sum(dp * p, axis=-1, keepdims=True))
        ds_ref[...] = (ds * HD**-HALF).astype(BF)
        grads = {i: ([], [], []) for i in xs}
        for n, (i, h) in enumerate(some):
            x, d = xs[i]
            dq, dk, dv = grads[i]
            dq.append(dims(ds_ref[n], heads_of(x, 1, h), 1, 0).astype(BF))
            dk.append(dims(ds_ref[n], heads_of(x, 0, h), 0, 0).astype(BF))
            dv.append(dims(p_ref[n], heads_of(d, 0, h), 0, 0).astype(BF))
        for i, parts in grads.items():
            out[:, i] = jnp.concatenate(sum(parts, []), axis=-1).reshape(PEERS, GROUP, QKV_N)


def seq_spec(n):
    per_half = PEERS // SEQS
    return pl.BlockSpec((None, PEERS, SEQS, GROUP, n), lambda i, info: (lax.div(i, per_half), 0, lax.rem(i, per_half), 0, 0))


def by_seq(a):
    return a.reshape(TWO, PEERS, PEERS, GROUP, a.shape[-1])


def seq_shape(n):
    return jax.ShapeDtypeStruct((TWO, PEERS, PEERS, GROUP, n), BF)


def attn_tiles(group, *types):
    return [pltpu.VMEM((group * HEADS, ROWS, ROWS), t) for t in types]


def attn_fwd(info, qkv, group):
    grid_spec = pltpu.PrefetchScalarGridSpec(
        num_scalar_prefetch=1, grid=(ALL_SEQS // SEQS,), in_specs=[seq_spec(QKV_N)], out_specs=seq_spec(INNER), scratch_shapes=attn_tiles(group, F32, BF)
    )
    out = pl.pallas_call(partial(attn_fwd_kernel, group), name="attn_fwd", out_shape=seq_shape(INNER), grid_spec=grid_spec)(info, by_seq(qkv))
    return out.reshape(TWO, PEERS, ROWS, INNER)


def stacking(puts, stacks):
    used = sorted({p[1] for p in puts})
    first = [next(p for p in puts if p[1] == k) for k in used]
    shapes = [jax.ShapeDtypeStruct((p[3],) + p[0].shape, p[0].dtype) for p in first]
    given = [k for k in used if stacks[k] is not None]
    dma = pltpu.SemaphoreType.DMA
    scratch = [pltpu.VMEM(p[0].shape, p[0].dtype) for p in puts] + [dma((len(puts),)), dma((len(puts),))]
    return used, shapes, given, scratch


def attn_bwd(info, qkv, dctx, puts, stacks, group):
    used, shapes, given, scratch = stacking(puts, stacks)
    m = len(puts)

    def kernel(info, qkv, dctx, *refs):
        grads, refs = refs[:m], refs[m + len(given) :]
        out, outs, refs = refs[0], refs[1 : 1 + len(used)], refs[1 + len(used) :]
        bounce, load_sem, put_sem, tiles = refs[:m], refs[m], refs[m + 1], refs[m + TWO :]
        step = pl.program_id(0)

        def load(i):
            return Pieces(grads[i], bounce[i], load_sem.at[i], PEERS)

        def put(i):
            return Pieces(bounce[i], outs[used.index(puts[i][1])].at[puts[i][TWO]], put_sem.at[i], PEERS)

        @pl.when(step == 0)
        def _():
            for i in range(m):
                load(i).start()

        for at, some in ((1, range(m // TWO)), (TWO, range(m // TWO, m))):

            @pl.when(step == at)
            def _(some=some):
                for i in some:
                    load(i).wait()
                    put(i).start()

        attn_bwd_steps(group, info, qkv, dctx, out, *tiles)

        @pl.when(step == ALL_SEQS // SEQS - 1)
        def _():
            for i in range(m):
                put(i).wait()

    hbm = pl.BlockSpec(memory_space=ANY)
    grid_spec = pltpu.PrefetchScalarGridSpec(
        num_scalar_prefetch=1,
        grid=(ALL_SEQS // SEQS,),
        in_specs=[seq_spec(QKV_N), seq_spec(INNER)] + [hbm] * (m + len(given)),
        out_specs=[seq_spec(QKV_N)] + [hbm] * len(used),
        scratch_shapes=scratch + attn_tiles(group, F32, BF, BF, BF),
    )
    res = pl.pallas_call(
        kernel,
        name="attn_bwd",
        out_shape=[seq_shape(QKV_N)] + shapes,
        grid_spec=grid_spec,
        input_output_aliases={3 + m + j: 1 + used.index(k) for j, k in enumerate(given)},
        compiler_params=pltpu.CompilerParams(vmem_limit_bytes=VMEM_LIMIT),
    )(info, by_seq(qkv), by_seq(dctx), *[p[0] for p in puts], *[stacks[k] for k in given])
    for k, a in zip(used, res[1:]):
        stacks[k] = a
    return res[0].reshape(TWO, PEERS, ROWS, QKV_N)


def put_last(puts, stacks):
    used, shapes, given, scratch = stacking(puts, stacks)
    m = len(puts)

    def kernel(*refs):
        grads, refs = refs[:m], refs[m + len(given) :]
        outs, refs = refs[: len(used)], refs[len(used) :]
        bounce, load_sem, put_sem = refs[:m], refs[m], refs[m + 1]
        loads = [Pieces(grads[i], bounce[i], load_sem.at[i], PEERS).start() for i in range(m)]
        stores = []
        for i, p in enumerate(puts):
            loads[i].wait()
            stores.append(Pieces(bounce[i], outs[used.index(p[1])].at[p[TWO]], put_sem.at[i], PEERS).start())
        for c in stores:
            c.wait()

    hbm = pl.BlockSpec(memory_space=ANY)
    res = pl.pallas_call(
        kernel,
        name="put_last",
        out_shape=shapes,
        in_specs=[hbm] * (m + len(given)),
        out_specs=[hbm] * len(used),
        scratch_shapes=scratch,
        input_output_aliases={m + j: used.index(k) for j, k in enumerate(given)},
        compiler_params=pltpu.CompilerParams(vmem_limit_bytes=VMEM_LIMIT),
    )(*[p[0] for p in puts], *[stacks[k] for k in given])
    for k, a in zip(used, res):
        stacks[k] = a


def group_body(x_loc, dy_loc, len_loc, wqkv, wout, wup, bup, wdown, vec):
    n = wqkv.shape[0]
    ids = iter(range(ROWS))
    shape = x_loc.shape
    x = x_loc.reshape(TWO, ROWS, D)
    dy = dy_loc.reshape(TWO, ROWS, D)
    wq = jnp.transpose(wqkv, (0, 2, 3, 4, 1)).reshape(n, QKV_N, D)
    wo = wout.reshape(n, INNER, D)
    info = jnp.concatenate([len_loc, lax.axis_index(TP).reshape(1).astype(jnp.int32)])

    def flat(a):
        return a.reshape(TOK, a.shape[-1])

    def row(layer, i, bias=None):
        return SimpleNamespace(gain=(layer, i), shift=(layer, i + 1), bias=bias)

    ln2, bias1, bias2 = TWO, 4, 5
    saved = [SimpleNamespace() for _ in range(n)]
    (r,) = fused("first", next(ids), FIRST, config(N_FIRST, dict(in0=x, wb=wq, vec=vec), row(0, 0), ag=(QKV, 0)))
    s = saved[0]
    s.x, s.a, s.qkv = x, r.full, r.res
    for l in range(n):
        s = saved[l]
        s.ctx = attn_fwd(info, s.qkv, SEQS)
        arrays = dict(lhs1=s.ctx, wa=wo, wb=wup, in0=s.x, vec=vec, b_up=bup)
        stages = [config(N_LN, arrays, row(l, ln2, (l, bias1)), rs=(l, INNER, False), ag=(UP, l))]
        kind, taken = MID, (("lhs1", "res"), ("in0", "out0"))
        arrays = dict(wa=wdown, vec=vec)
        if l + 1 < n:
            arrays.update(wb=wq)
            stages.append(config(N_LN, arrays, row(l + 1, 0, (l, bias2)), rs=(l, FF, False), ag=(QKV, l + 1), taken=taken))
        else:
            kind = TOP
            arrays.update(src=dy)
            stages.append(config(N_RES, arrays, row(0, 0, (l, bias2)), rs=(l, FF, False), ag=(DACT, l), taken=taken + (("slope", "slope"),)))
        r, z = fused(f"fwd_{l}", next(ids), kind, *stages)
        s.hid, s.act, s.slope, s.m_t, s.act_t = r.out0, r.res, r.slope, r.full_t, r.res_t
        if l + 1 < n:
            s = saved[l + 1]
            s.x, s.a, s.qkv = z.out0, z.full, z.res
    y, d_cur, d_full, d_pre = z.out0, z.out1, z.full, z.res
    g_bup, rows, puts, stacks = [z.bup], [], [(y.reshape(KT, D), 4, 0, 1)], [None] * 6
    mlp_plans = ((3, 1, 0, 6, 1, 0, 2, 0, 2, 2, 3, 0, 2), (3, 1, 0, 5, 1, 0, 2, 0, 2, 2, 3, 0, 2), (3, 1, 0, 5, 1, 0, 2, 0, 2, 2, 3, 0, 2))
    attn_plans = ((8, 5), (4, 2, 0, 6, 2, 0, 1, 1, 1, 1, 2, 1, 1), (3, 2, 0, 7, 2, 0, 1, 1, 1, 1, 3, 1, 1))
    for l in reversed(range(n)):
        s = saved[l]
        arrays = dict(lhs1=d_pre, wa=wup, wb=wo, in0=s.hid, in1=d_cur, vec=vec, f0l=s.act_t, f0r=flat(d_full), f1l=s.m_t, f1r=flat(d_pre))
        common = dict(fills=((FF, D, TWO), (D, FF, 1)), bm=BM + BM, flat_t=True, plan=mlp_plans[l])
        (r,) = fused(f"d_mlp_{l}", next(ids), MID, config(N_BWD2, arrays, row(l, ln2), rs=(l, FF, True), ag=(DCTX, l), **common))
        d_hid, d_attn, v3 = r.out0, r.full, r.vo
        puts += [(r.g0, 3, l, n), (r.g1, TWO, l, n)]
        d_qkv = attn_bwd(info, s.qkv, r.res, puts, stacks, TWO if l else 1)
        arrays = dict(lhs1=d_qkv, wa=wq, in0=s.x, in1=d_hid, vec=vec, f0l=flat(s.ctx), f0r=flat(d_attn), f1l=flat(d_qkv), f1r=flat(s.a))
        common = dict(rs=(l, QKV_N, False), fills=((INNER, D, 1), (QKV_N, D, 3)), plan=attn_plans[l])
        if l:
            arrays.update(wb=wdown, slope=saved[l - 1].slope)
            common.update(ag=(DACT, l - 1))
        else:
            arrays.update({f"row_a{i}": rows[n - 1 - i][0] for i in range(1, n)}, row_b0=v3, **{f"row_b{i}": rows[n - 1 - i][1] for i in range(1, n)})
            common.update(layers=n)
        (r,) = fused(f"d_attn_{l}", next(ids), MID if l else LAST, config(N_BWD1, arrays, row(l, 0), **common))
        if l:
            g_bup.append(r.bup)
            d_full, d_pre = r.full, r.res
        puts = [(r.g0, 1, l, n), (r.g1, 0, l, n)]
        rows.append((r.vo, v3))
        d_cur = r.out0
    put_last(puts + [(d_cur.reshape(KT, D), 5, 0, 1)], stacks)
    g_qkv = jnp.transpose(stacks[0].reshape(n, 3, HEADS, HD, D), (0, 4, 1, 2, 3))
    g_out = stacks[1].reshape(n, HEADS, HD, D)
    return stacks[4].reshape(shape), stacks[5].reshape(shape), g_qkv, g_out, stacks[2], jnp.concatenate(g_bup[::-1]), stacks[3], r.row_o


def solution(mesh):
    act_spec = P(DP, TP, None)
    in_specs = (act_spec, act_spec, P(DP), P(None, None, None, TP, None), P(None, TP, None, None), P(None, None, TP), P(None, TP), P(None, TP, None), P())
    out_specs = (act_spec, act_spec, P(DP, None, None, TP, None), P(DP, TP, None, None), P(DP, None, TP), P(DP, TP), P(DP, TP, None), P(DP, None, None))
    return jax.shard_map(group_body, mesh=mesh, in_specs=in_specs, out_specs=out_specs, check_vma=False)
```

```python
from functools import partial
from types import SimpleNamespace

import jax
import jax.numpy as jnp
from jax import lax
from jax.experimental import pallas as pl
from jax.experimental.pallas import tpu as pltpu
from jax.sharding import PartitionSpec as P

TP, DP = "tp", "dp"
D, FF, INNER, QKV_N = 3072, 1536, 384, 1152
ROWS, HALF_ROWS, GROUP = 128, 64, 16
LANES, SUBL = 128, 8
A, B = HALVES = range(2)
PEERS = 8
TOK = len(HALVES) * PEERS * ROWS
HEADS, HD = 4, 96
SEQS, ALL_SEQS = 4, 16
BM, BN, KT = 384, 512, 256
BF, F32 = jnp.bfloat16, jnp.float32
ANY = pl.ANY
VMEM_LIMIT = 66_900_000
GELU_C, GELU_D = 0.7978845608028654, 0.044715
EPS, NEG = 1e-5, -1e30
ONE, TWO, HALF = 1.0, 2, 0.5
OWN, XN, YN, FAR = PAIRS = range(4)
Q_ORDER = (FAR, XN, YN, OWN)
R_X, R_Y, R_FAR = 2, 4, 6
X_FAR, Y_FAR, X_RAW, Y_RAW, X_SUM, Y_SUM, N_RS = range(4, 11)
G_CORE, G_XT, G_XB, G_YB, G_YT, G_FT, G_FB, G_C3, G_C5, G_C7, N_AG = range(11)
CROSSING = {XN: G_C3, YN: G_C5, FAR: G_C7}
FIRST, MID, TOP, LAST = range(4)
N_FIRST, N_LN, N_RES, N_BWD2, N_BWD1 = range(5)
QKV, UP, DACT, DCTX = range(4)
WIDTH = (QKV_N, FF, FF, INNER)
PER = 6
ALL = 1 << 20


def dims(lhs, rhs, lc, rc):
    return lax.dot_general(lhs, rhs, (((lc,), (rc,)), ((), ())), preferred_element_type=F32)


def peers():
    me = lax.axis_index(TP)
    dp = lax.axis_index(DP)

    def flip(bit):
        return me + bit - TWO * bit * lax.rem(lax.div(me, bit), TWO)

    return [(dp, flip(1 << k)) for k in range(3)]


def say_here(devices):
    for dev in devices:
        pl.semaphore_signal(pltpu.get_barrier_semaphore(), inc=1, device_id=dev, device_id_type=pl.DeviceIdType.MESH)


def await_peers(n=3):
    pl.semaphore_wait(pltpu.get_barrier_semaphore(), n)


def remote(src, dst, send, recv, dev):
    return pltpu.make_async_remote_copy(src_ref=src, dst_ref=dst, send_sem=send, recv_sem=recv, device_id=dev, device_id_type=pl.DeviceIdType.MESH)


class Pieces:
    def __init__(self, src, dst, sem, n):
        self.src, self.dst, self.sem, self.n = src, dst, sem, n

    def start(self):
        src, dst = self.src, self.dst
        step = src.shape[-2] // self.n
        for i in range(self.n):
            at = pl.ds(i * step, step)
            if len(src.shape) == 3:
                for j in range(src.shape[0]):
                    pltpu.make_async_copy(src.at[j, at], dst.at[j, at], self.sem).start()
            else:
                pltpu.make_async_copy(src.at[at], dst.at[at], self.sem).start()
        return self

    def wait(self):
        pltpu.make_async_copy(self.src, self.dst, self.sem).wait()


def call(name, cid, body, ins, outs, scratch, small):
    names = [list(vars(a)) for a in (ins, outs, scratch)]

    def kernel(*refs):
        body(SimpleNamespace(**dict(zip(sum(names, []), refs))))

    def spec(n):
        return pl.BlockSpec(memory_space=pltpu.VMEM if n in small else ANY)

    res = pl.pallas_call(
        kernel,
        name=name,
        out_shape=list(vars(outs).values()),
        in_specs=[spec(n) for n in names[0]],
        out_specs=[spec(n) for n in names[1]],
        scratch_shapes=list(vars(scratch).values()),
        compiler_params=pltpu.CompilerParams(vmem_limit_bytes=VMEM_LIMIT, collective_id=cid, has_side_effects=True),
    )(*vars(ins).values())
    return SimpleNamespace(**dict(zip(names[1], res)))


def config(norm, arrays, vec, rs=None, ag=None, fills=(), bm=BM, flat_t=False, plan=(), taken=(), layers=0):
    return SimpleNamespace(norm=norm, arrays=arrays, vec=vec, rs=rs, ag=ag, fills=fills, bm=bm, flat_t=flat_t, plan=plan, taken=dict(taken), layers=layers)


def declare(c):
    outs, sc = SimpleNamespace(), SimpleNamespace()
    dma = pltpu.SemaphoreType.DMA
    n_in = TWO if c.norm in (N_BWD2, N_BWD1) else 1
    n_acc = {N_BWD2: 4, N_BWD1: TWO}.get(c.norm, 0)
    shard = jax.ShapeDtypeStruct((TWO, ROWS, D), F32)
    if c.norm != N_FIRST:
        outs.out0 = shard
        sc.nout = pltpu.VMEM((ROWS, D), F32)
    if c.norm == N_RES:
        outs.out1 = shard
        sc.nout1 = pltpu.VMEM((ROWS, D), F32)
    sc.nin = pltpu.VMEM((n_in, ROWS, D), F32)
    sc.nsem = dma((n_in + TWO,))
    if n_acc:
        outs.vo = jax.ShapeDtypeStruct((SUBL, D), F32)
        sc.acc = pltpu.VMEM((n_acc, SUBL, D), F32)
    if c.rs:
        k1 = c.rs[1]
        tile1 = 1024
        tiles1 = D // tile1
        halves = (TWO, ROWS, D)
        sc.w1 = pltpu.VMEM((D, k1) if c.rs[2] else (k1, D), BF)
        sc.lhs = pltpu.VMEM((TWO, TWO, ROWS, k1), BF)
        sc.own = pltpu.VMEM((TWO, len(PAIRS), ROWS, D), BF)
        sc.snd = pltpu.VMEM((len(PAIRS), ROWS, D), BF)
        sc.drx = pltpu.VMEM((TWO, len(PAIRS), ROWS, D), BF)
        sc.hx = pltpu.VMEM((TWO, HALF_ROWS, D), BF)
        sc.hy = pltpu.VMEM((TWO, HALF_ROWS, D), BF)
        sc.rx = pltpu.VMEM(halves, BF)
        sc.ry = pltpu.VMEM(halves, BF)
        sc.w1_sem = dma((tiles1,))
        sc.lhs_sem = dma((TWO,))
        sc.rs_send = dma((TWO, N_RS))
        sc.rs_recv = dma((TWO, N_RS))
        sc.far_send = dma((tiles1, len(PAIRS)))
        sc.far_recv = dma((tiles1, len(PAIRS)))
    if c.ag:
        what = c.ag[0]
        n2 = WIDTH[what]
        outs.full = jax.ShapeDtypeStruct((TWO, PEERS, ROWS, D), BF)
        outs.res = jax.ShapeDtypeStruct((TWO, PEERS, ROWS, n2), BF)
        pairs_of = (TWO, TWO, ROWS, n2)
        sc.w2 = pltpu.VMEM((D, n2) if what == UP else (n2, D), BF)
        sc.g = pltpu.VMEM((TWO, ROWS, D), BF)
        sc.agin = pltpu.VMEM((TWO, TWO, ROWS, D), BF)
        sc.last = pltpu.VMEM((TWO, ROWS, D), BF)
        sc.w2_sem = dma
        sc.g_sem = dma((TWO,))
        sc.agin_sem = dma((TWO,))
        sc.last_sem = dma((TWO,))
        sc.ag_send = dma((TWO, N_AG))
        sc.ag_recv = dma((TWO, N_AG))
        sc.res_st = pltpu.VMEM(pairs_of, BF)
        sc.res_sem = dma((TWO,))
        if what == UP:
            outs.slope = jax.ShapeDtypeStruct((TWO, PEERS, ROWS, n2), F32)
            outs.full_t = jax.ShapeDtypeStruct((D, TOK), BF)
            outs.res_t = jax.ShapeDtypeStruct((n2, TOK), BF)
            sc.full_ts = pltpu.VMEM((D, KT), BF)
            sc.res_ts = pltpu.VMEM((n2, KT), BF)
            sc.t_sem = dma((TWO,))
        if what == DACT:
            outs.bup = jax.ShapeDtypeStruct((1, n2), F32)
            sc.bacc = pltpu.VMEM((SUBL, n2), F32)
        if what in (UP, DACT):
            sc.slope_st = pltpu.VMEM(pairs_of, F32)
            sc.slope_sem = dma((TWO,))
    if c.fills:
        slots = TWO if c.flat_t else max(f[2] for f in c.fills)
        sc.f_at = pltpu.VMEM((slots, c.bm, TOK), BF)
        ahead = 3 if c.flat_t or not c.ag else TWO
        sc.f_rhs = pltpu.VMEM((ahead, TOK, BN), BF)
        sc.f_out = pltpu.VMEM((TWO, c.bm, BN), BF)
        if not c.flat_t:
            sc.f_lhs = pltpu.VMEM((TOK, c.bm), BF)
        sc.fl_sem = dma((slots,))
        sc.fr_sem = dma((ahead,))
        sc.fo_sem = dma((TWO,))
        for i, f in enumerate(c.fills):
            setattr(outs, f"g{i}", jax.ShapeDtypeStruct(f[:TWO], BF))
    if c.layers:
        outs.row_o = jax.ShapeDtypeStruct((c.layers, PER, D), F32)
        rows = -(-PER * c.layers // SUBL) * SUBL
        for k, n in (("e", rows), ("l", SUBL)):
            half = (n, D // TWO)
            parts = dict(v=pltpu.VMEM((n, D), F32), a=pltpu.VMEM((n, D), F32), t=pltpu.VMEM((n, D), F32), s=pltpu.VMEM((3,) + half, F32), b=pltpu.VMEM((TWO,) + half, F32))
            parts.update(send=dma((4,)), recv=dma((4,)))
            for p, x in parts.items():
                setattr(sc, k + p, x)
    return outs, sc


def stage(c, r):
    norm, vec, rs, ag, fills, bm, flat_t, plan = c.norm, c.vec, c.rs, c.ag, c.fills, c.bm, c.flat_t, c.plan
    n_in = TWO if norm in (N_BWD2, N_BWD1) else 1
    n_acc = {N_BWD2: 4, N_BWD1: TWO}.get(norm, 0)
    if rs:
        k1 = rs[1]
        tile1 = 1024
        tiles1 = D // tile1
    if ag:
        what = ag[0]
        n2 = WIDTH[what]
    core, px, py = peers()
    waiting = [1] if c.first else []
    late = () if c.first else (4, 5)

    def await_once():
        while waiting:
            waiting.pop()
            await_peers()

    def begin(src, dst, sem, n=4):
        return Pieces(src, dst, sem, n).start()

    def norm_load(h):
        some = (r.in0, r.in1) if n_in == TWO else (r.in0,)
        return [begin(x.at[h], r.nin.at[i], r.nsem.at[i]) for i, x in enumerate(some)]

    def vrow(row):
        return r.vec[row[0], pl.ds(row[1], 1), :]

    out_copy = []

    def mean(x):
        return jnp.sum(x, axis=-1, keepdims=True) * (ONE / D)

    def norm_half(h, loads):
        for c in loads:
            c.wait()
        while out_copy:
            out_copy.pop().wait()

        def rows(i, carry):
            at = pl.ds(pl.multiple_of(i * GROUP, GROUP), GROUP)
            x = r.nin[0, at, :]
            if rs:
                o = r.own[h, OWN, at, :].astype(F32) + r.rx[h, at, :].astype(F32) + r.ry[h, at, :].astype(F32)
                o = o.astype(BF).astype(F32)
            if norm in (N_LN, N_RES):
                x = x + o + vrow(vec.bias)
                r.nout[at, :] = x
            if norm == N_RES:
                r.nout1[at, :] = r.g[h, at, :].astype(F32)
                return carry
            cen = x - mean(x)
            rstd = lax.rsqrt(mean(cen * cen) + EPS)
            if norm in (N_FIRST, N_LN):
                r.g[h, at, :] = (cen * rstd * vrow(vec.gain) + vrow(vec.shift)).astype(BF)
                return carry
            xh = cen * rstd
            dxh = o * vrow(vec.gain)
            base = r.nin[1, at, :]
            res = base + rstd * (dxh - mean(dxh) - xh * mean(dxh * xh))
            r.nout[at, :] = res
            if ag:
                r.g[h, at, :] = res.astype(BF)
            sums = [o * xh, o] + ([res, base] if norm == N_BWD2 else [])
            for j, v in enumerate(sums):
                r.acc[j] += v[:SUBL] + v[SUBL:]
            return carry

        lax.fori_loop(0, ROWS // GROUP, rows, 0)
        if norm != N_FIRST:
            out_copy.append(begin(r.nout, r.out0.at[h], r.nsem.at[n_in]))
        if norm == N_RES:
            out_copy.append(begin(r.nout1, r.out1.at[h], r.nsem.at[n_in + 1]))

    top, bot = pl.ds(0, HALF_ROWS), pl.ds(HALF_ROWS, HALF_ROWS)
    if rs:
        seq = [(h, q) for h in HALVES for q in Q_ORDER]
        lhs_loads, rs_copy, far_copy, w1_loads = {}, {}, {}, []
        own = r.own

        def w1_load():
            for n in range(tiles1):
                at = pl.ds(n * tile1, tile1)
                src, dst = r.wa.at[rs[0]], r.w1
                src, dst = (src.at[at], dst.at[at]) if rs[2] else (src.at[:, at], dst.at[:, at])
                w1_loads.append(begin(src, dst, r.w1_sem.at[n]))

        def lhs_load(i):
            h, q = seq[i]
            s = i % TWO
            lhs_loads[i] = begin(r.lhs1.at[h, pl.ds(TWO * q, TWO)], r.lhs.at[s], r.lhs_sem.at[s])

        def lhs_late():
            for i in late:
                lhs_load(i)

        def rs_start(h, j, src, dst, dev):
            c = remote(src, dst, r.rs_send.at[h, j], r.rs_recv.at[h, j], dev)
            c.start()
            rs_copy[h, j] = c

        def far_start(n, j, src, dst, dev):
            c = remote(src, dst, r.far_send.at[n, j], r.far_recv.at[n, j], dev)
            c.start()
            far_copy[n, j] = c

        def add_into(dst, src, n, at_cols=slice(None)):
            def rows(i, carry):
                at = pl.ds(pl.multiple_of(i * GROUP, GROUP), GROUP)
                dst[at, at_cols] = (dst[at, at_cols].astype(F32) + src[at, at_cols].astype(F32)).astype(BF)
                return carry

            lax.fori_loop(0, n // GROUP, rows, 0)

        def far_merge(n, send):
            cols = pl.ds(n * tile1, tile1)
            far_copy[n, 0].wait_recv()
            add_into(own.at[A, FAR], r.drx.at[A, FAR], ROWS, cols)
            if send:
                far_sends(n)

        def far_sends(n):
            cols = pl.ds(n * tile1, tile1)
            far_start(n, 1, own.at[A, FAR, top, cols], r.hx.at[A, :, cols], px)
            far_start(n, 2, own.at[A, FAR, bot, cols], r.hy.at[A, :, cols], py)

        def product_in(i, between=None, send=True):
            h, q = seq[i]
            s = i % TWO
            lhs_loads[i].wait()
            if i == len(PAIRS):
                for n in range(tiles1):
                    far_copy[n, 0].wait_send()
            elif h == B:
                rs_copy[A, q].wait_send()

            def tile(n, carry):
                at = pl.ds(pl.multiple_of(n * tile1, tile1), tile1)
                x = r.lhs[s].reshape(TWO * ROWS, k1)
                y = dims(x, r.w1[at, :], 1, 1) if rs[2] else dims(x, r.w1[:, at], 1, 0)
                y = y.astype(BF)
                own[h, q, :, at] = y[:ROWS]
                r.snd[q, :, at] = y[ROWS:]
                return carry

            if i == 0:
                for n in range(tiles1):
                    cols = pl.ds(n * tile1, tile1)
                    w1_loads[n].wait()
                    tile(n, 0)
                    if n == 0:
                        await_once()
                    far_start(n, 0, r.snd.at[FAR, :, cols], r.drx.at[A, FAR, :, cols], core)
                    if n:
                        far_merge(n - 1, send)
            else:
                tile(0, 0)
                if between:
                    between()
                lax.fori_loop(1, tiles1, tile, 0)
            if i + TWO < len(seq) and i + TWO not in late:
                lhs_load(i + TWO)
            if i:
                rs_start(h, q, r.snd.at[q], r.drx.at[h, q], core)

        def merge(h, q):
            rs_copy[h, q].wait_recv()
            add_into(own.at[h, q], r.drx.at[h, q], ROWS)

        def first_sends(h, q):
            if q == FAR:
                rs_start(h, X_FAR, own.at[h, q, top], r.hx.at[h], px)
                rs_start(h, Y_FAR, own.at[h, q, bot], r.hy.at[h], py)
            if q == XN:
                rs_start(h, X_RAW, own.at[h, q, top], r.rx.at[h, top], px)
            if q == YN:
                rs_start(h, Y_RAW, own.at[h, q, bot], r.ry.at[h, bot], py)

        def far_wait(h, j):
            if h == A:
                for n in range(tiles1):
                    far_copy[n, 1 + j].wait_recv()
            else:
                rs_copy[h, X_FAR + j].wait_recv()

        def third_sends(h):
            far_wait(h, 1)
            add_into(own.at[h, XN, bot], r.hy.at[h], HALF_ROWS)
            rs_start(h, X_SUM, own.at[h, XN, bot], r.rx.at[h, bot], px)
            far_wait(h, 0)
            add_into(own.at[h, YN, top], r.hx.at[h], HALF_ROWS)
            rs_start(h, Y_SUM, own.at[h, YN, top], r.ry.at[h, top], py)

        def rs_done(h):
            for j in (X_RAW, Y_RAW, X_SUM, Y_SUM):
                rs_copy[h, j].wait_recv()

        def step(i, send=True):
            def between():
                h, q = seq[i - 1]
                if i == 1:
                    far_merge(tiles1 - 1, send)
                    return
                merge(h, q)
                if send:
                    first_sends(h, q)

            product_in(i, between if i % len(PAIRS) else None, send)

    if ag:
        full = r.full
        ag_copy, g_copy, ready_loads, res_out, w2_copy, last_copy = {}, {}, {}, {}, [], []

        def w2_load():
            w2_copy.append(begin(r.wb.at[ag[1]], r.w2, r.w2_sem, PEERS))

        def ag_start(h, j, src, dst, dev):
            c = remote(src, dst, r.ag_send.at[h, j], r.ag_recv.at[h, j], dev)
            c.start()
            ag_copy[h, j] = c

        def own_sends(h):
            g = r.g
            ag_start(h, G_XT, g.at[h, top], full.at[h, R_X, top], px)
            ag_start(h, G_YB, g.at[h, bot], full.at[h, R_Y, bot], py)
            ag_start(h, G_XB, g.at[h, bot], full.at[h, R_X, bot], px)
            ag_start(h, G_YT, g.at[h, top], full.at[h, R_Y, top], py)
            ag_start(h, G_CORE, g.at[h], full.at[h, 1], core)
            g_copy[h] = begin(g.at[h], full.at[h, 0], r.g_sem.at[h])

        def far_place(h, other):
            return full.at[h, R_FAR + other] if h == A else r.last.at[other]

        def forward(h):
            ag_copy[h, G_XT].wait_recv()
            ag_start(h, G_FT, full.at[h, R_X, top], far_place(h, 0).at[top], py)
            ag_copy[h, G_YB].wait_recv()
            ag_start(h, G_FB, full.at[h, R_Y, bot], far_place(h, 0).at[bot], px)

        def cross(h):
            ag_copy[h, G_XB].wait_recv()
            ag_start(h, G_C3, full.at[h, R_X], full.at[h, R_X + 1], core)
            ag_copy[h, G_YT].wait_recv()
            ag_start(h, G_C5, full.at[h, R_Y], full.at[h, R_Y + 1], core)

        def cross_far(h):
            ag_copy[h, G_FT].wait_recv()
            ag_copy[h, G_FB].wait_recv()
            ag_start(h, G_C7, far_place(h, 0), far_place(h, 1), core)
            if h == B:
                last_copy.append(begin(r.last.at[0], full.at[h, R_FAR], r.last_sem.at[0]))

        def ready(h, q):
            s = (len(PAIRS) * h + (OWN, XN, YN, FAR).index(q)) % TWO
            pair = pl.ds(TWO * q, TWO)
            loads = []
            if what == DACT:
                loads.append(begin(r.slope.at[h, pair], r.slope_st.at[s], r.slope_sem.at[s]))
            if q == OWN:
                g_copy.pop(h).wait()
                ag_copy[h, G_CORE].wait_recv()
            else:
                ag_copy[h, CROSSING[q]].wait_recv()
            if (h, q) == (B, FAR):
                last_copy.append(begin(r.last.at[1], full.at[h, R_FAR + 1], r.last_sem.at[1]))
            else:
                loads.append(begin(full.at[h, pair], r.agin.at[s], r.agin_sem.at[s]))
            ready_loads[h, q] = (s, loads)

        flipped = {}

        def flip(src, stage, dst, i):
            if i in flipped:
                flipped[i].wait()

            def block(k, carry):
                at = pl.ds(pl.multiple_of(k * KT, KT), KT)
                stage[at, :] = src[:, :, at].reshape(KT, KT).T
                return carry

            lax.fori_loop(0, stage.shape[0] // KT, block, 0)
            flipped[i] = begin(stage, dst, r.t_sem.at[i])

        to_flip = []

        def flip_all():
            while to_flip:
                flip(*to_flip.pop(0))

        def product(h, q):
            if (h, q) not in ready_loads:
                ready(h, q)
            s, loads = ready_loads.pop((h, q))
            pair = pl.ds(TWO * q, TWO)
            while w2_copy:
                w2_copy.pop().wait()
            for c in res_out.pop(s, ()):
                c.wait()
            for c in loads:
                c.wait()
            nt = BM if what in (QKV, DCTX) else BN

            def tile(n, carry):
                at = pl.ds(pl.multiple_of(n * nt, nt), nt)
                x = r.last[...] if (h, q) == (B, FAR) else r.agin[s]
                x = x.reshape(TWO * ROWS, D)
                y = dims(x, r.w2[:, at], 1, 0) if what == UP else dims(x, r.w2[at, :], 1, 1)
                if what == UP:
                    u = y + r.b_up[pl.ds(ag[1], 1), at]
                    t = jnp.tanh(GELU_C * (u + GELU_D * (u * u * u)))
                    slope = HALF * (ONE + t) + (HALF * GELU_C) * u * (ONE - t * t) * (ONE + (3 * GELU_D) * (u * u))
                    r.slope_st[s, :, :, at] = slope.reshape(TWO, ROWS, nt)
                    y = u * (HALF * (ONE + t))
                if what == DACT:
                    y = y.astype(BF).astype(F32) * r.slope_st[s, :, :, at].reshape(TWO * ROWS, nt)
                    r.bacc[:, at] += jnp.sum(y.reshape(-1, SUBL, nt), axis=0)
                r.res_st[s, :, :, at] = y.astype(BF).reshape(TWO, ROWS, nt)
                return carry

            if n2 == nt:
                tile(0, 0)
            else:
                lax.fori_loop(0, n2 // nt, tile, 0)
            res_out[s] = [begin(r.res_st.at[s], r.res.at[h, pair], r.res_sem.at[s])]
            if what == UP:
                res_out[s].append(begin(r.slope_st.at[s], r.slope.at[h, pair], r.slope_sem.at[s]))
                cols = pl.ds((h * PEERS + TWO * q) * ROWS, KT)
                gathered = r.last if (h, q) == (B, FAR) else r.agin.at[s]
                to_flip.append((gathered, r.full_ts, r.full_t.at[:, cols], 0))
                to_flip.append((r.res_st.at[s], r.res_ts, r.res_t.at[:, cols], 1))

    jobs = []
    if fills:
        refs = [[getattr(r, k) for k in (f"f{i}l", f"f{i}r", f"g{i}")] for i in range(len(fills))]
        jobs = [SimpleNamespace(lhs=f[0], rhs=f[1], out=f[2], blocks=c[0] // bm // c[2], tiles=c[1] // BN, sub=c[2], done=0) for f, c in zip(refs, fills)]
        slots = r.f_rhs.shape[0]
        for j in jobs:
            j.fetches = j.tiles if j.tiles <= slots else j.blocks * j.tiles

    def lhs_copy(j, k):
        at = pl.ds(pl.multiple_of(k * bm, bm), bm)
        if flat_t:
            s = lax.rem(k, TWO)
            return Pieces(j.lhs.at[at], r.f_at.at[s], r.fl_sem.at[s], PEERS)
        return Pieces(j.lhs.at[:, at], r.f_lhs, r.fl_sem.at[0], PEERS)

    def rhs_copy(j, v):
        s = lax.rem(v, slots)
        return Pieces(j.rhs.at[:, pl.ds(pl.multiple_of(lax.rem(v, j.tiles) * BN, BN), BN)], r.f_rhs.at[s], r.fr_sem.at[s], PEERS)

    def put_copy(j, u):
        s, v = lax.rem(u, TWO), lax.div(u, j.sub)
        row = lax.div(v, j.tiles) * j.sub + lax.rem(u, j.sub)
        dst = j.out.at[pl.ds(pl.multiple_of(row * bm, bm), bm), pl.ds(pl.multiple_of(lax.rem(v, j.tiles) * BN, BN), BN)]
        return Pieces(r.f_out.at[s], dst, r.fo_sem.at[s], 3)

    def job_begin(j):
        lhs_copy(j, jnp.int32(0)).start()
        if flat_t:
            lhs_copy(j, jnp.int32(1)).start()
        for v in range(slots - 1):
            rhs_copy(j, jnp.int32(v)).start()

    def fill(n):
        while n > 0 and jobs:
            j = jobs[0]
            rhs_all = j.blocks * j.tiles
            count = rhs_all * j.sub

            def unit(u, carry):
                v, b, s = lax.div(u, j.sub), lax.rem(u, j.sub), lax.rem(u, TWO)
                vs, t = lax.rem(v, slots), lax.rem(v, j.tiles)
                k = lax.div(v, j.tiles) * j.sub + b

                @pl.when(t == 0)
                def _():
                    lhs_copy(j, k).wait()
                    if flat_t:
                        return
                    for i in range(TOK // KT):
                        r.f_at[b, :, i * KT : (i + 1) * KT] = r.f_lhs[i * KT : (i + 1) * KT, :].T

                    @pl.when(k + 1 < j.blocks * j.sub)
                    def _():
                        lhs_copy(j, k + 1).start()

                @pl.when((b == 0) & (v < j.fetches))
                def _():
                    rhs_copy(j, v).wait()

                    @pl.when(v + (slots - 1) < j.fetches)
                    def _():
                        rhs_copy(j, v + (slots - 1)).start()

                @pl.when(u >= TWO)
                def _():
                    put_copy(j, u - TWO).wait()

                r.f_out[s] = dims(r.f_at[lax.rem(k, TWO) if flat_t else b], r.f_rhs[vs], 1, 0).astype(BF)
                put_copy(j, u).start()
                if flat_t:

                    @pl.when((t == j.tiles - 1) & (k + TWO < j.blocks * j.sub))
                    def _():
                        lhs_copy(j, k + TWO).start()

                return carry

            upto = min(count, j.done + n)
            n -= upto - j.done
            lax.fori_loop(j.done, upto, unit, 0)
            j.done = upto
            if upto == count:
                for u in (count - TWO, count - 1):
                    put_copy(j, jnp.int32(u)).wait()
                jobs.pop(0)
                if jobs:
                    job_begin(jobs[0])

    steps = list(plan)

    def fill_next():
        if steps:
            fill(steps.pop(0))

    def prologue():
        if rs:
            lhs_load(0)
            w1_load()
            lhs_load(1)
        if ag:
            w2_load()
        if jobs:
            job_begin(jobs[0])

    def clear():
        for j in range(n_acc):
            r.acc[j] = jnp.zeros((SUBL, D), F32)
        if ag and what == DACT:
            r.bacc[...] = jnp.zeros((SUBL, n2), F32)

    def rs_sent():
        for (h, j), x in rs_copy.items():
            if h == B or j > 3:
                x.wait_send()
        for (n, j), x in far_copy.items():
            if j:
                x.wait_send()
        rs_copy.clear()
        far_copy.clear()

    def rows_out():
        while out_copy:
            out_copy.pop().wait()

    def res_done():
        for s in list(res_out):
            for x in res_out.pop(s):
                x.wait()

    def end():
        for j in range(n_acc):
            r.vo[pl.ds(j, 1), :] = jnp.sum(r.acc[j], axis=0, keepdims=True)
        if n_acc:
            r.vo[n_acc:, :] = jnp.zeros((SUBL - n_acc, D), F32)
        if ag and what == DACT:
            r.bup[...] = jnp.sum(r.bacc[...], axis=0, keepdims=True)
        rows_out()
        if rs:
            rs_sent()
        if ag:
            for x in ag_copy.values():
                x.wait_send()
            res_done()
            for x in last_copy + list(flipped.values()):
                x.wait()

    return SimpleNamespace(**locals())


SHARED = ("own", "snd", "drx", "hx", "hy", "rx", "ry", "nin", "nout", "agin")


def fused(name, cid, kind, *stages):
    ins, outs, scratch, small, views = SimpleNamespace(), SimpleNamespace(), SimpleNamespace(), [], []
    shared = SHARED + (("res_st", "slope_st") if kind == TOP else ("g", "last"))
    for i, c in enumerate(stages):
        c.first = i == 0
        c_outs, c_sc = declare(c)
        view = {}
        for group, names in ((ins, c.arrays), (outs, vars(c_outs)), (scratch, vars(c_sc))):
            for n, x in names.items():
                view[n] = f"{n}{0 if group is scratch and n in shared else i}"
                setattr(group, view[n], x)
                if group is not scratch and (n in ("vec", "b_up", "vo", "bup") or n.startswith("row_")):
                    small.append(view[n])
        view.update({n: f"{prev}{i - 1}" for n, prev in c.taken.items()})
        views.append(view)
    if kind == TOP:
        del scratch.w21
        views[1]["w2"] = views[1]["w1"]
    elif len(stages) > 1:
        del scratch.w10
        views[0]["w1"] = views[1]["w2"]

    def body(refs):
        refs = vars(refs)
        st = [stage(c, SimpleNamespace(**{n: refs[x] for n, x in v.items()})) for c, v in zip(stages, views)]
        if kind == MID and len(st) > 1:
            st[0].r.w1 = st[0].r.w1.at[pl.ds(0, stages[0].rs[1])]
        say_here(peers())
        PROGRAMS[kind](*st)

    res = call(name, cid, body, ins, outs, scratch, small)
    return [SimpleNamespace(**{n: getattr(res, x) for n, x in v.items() if hasattr(res, x) and n not in c.taken}) for c, v in zip(stages, views)]


def both_halves(s, loads):
    for i in range(len(PAIRS)):
        s.step(i)
    s.merge(A, OWN)
    s.third_sends(A)
    second_half(s, loads)


def second_half(s, loads):
    for i in range(len(PAIRS), len(s.seq)):
        s.step(i)
    s.merge(B, OWN)
    s.fill_next()
    s.rs_done(A)
    s.norm_half(A, loads)


def products(s, h):
    s.cross(h)
    s.fill_next()
    s.ready(h, XN)
    s.ready(h, YN)
    s.product(h, XN)
    if h == A:
        s.flip_all()
    s.product(h, YN)
    if h == A:
        s.flip_all()
    s.fill_next()
    s.cross_far(h)


def first_program(s):
    s.prologue()
    loads = s.norm_load(A)
    s.norm_half(A, loads)
    loads = s.norm_load(B)
    s.await_once()
    s.own_sends(A)
    s.norm_half(B, loads)
    s.product(A, OWN)
    s.forward(A)
    s.own_sends(B)
    s.ready(B, OWN)
    s.product(B, OWN)
    products(s, A)
    s.product(A, FAR)
    s.forward(B)
    products(s, B)
    s.product(B, FAR)
    s.end()


def sum_steps(v, a, t, s, b, send, recv):
    core, px, py = peers()
    half = D // TWO
    mine = pl.ds(pl.multiple_of(lax.rem(lax.axis_index(TP), TWO) * half, half), half)
    copies = []

    def go(src, dst, i, dev):
        x = remote(src, dst, send.at[i], recv.at[i], dev)
        x.start()
        copies.append(x)

    def one():
        go(v, a, 0, core)

    def two():
        copies.pop().wait()
        s[0] = v[:, mine] + a[:, mine]
        go(s.at[0], b.at[0], 1, px)

    def three():
        copies.pop().wait()
        s[1] = s[0] + b[0]
        go(s.at[1], b.at[1], TWO, py)

    def four():
        copies.pop().wait()
        s[TWO] = s[1] + b[1]
        t[:, mine] = s[TWO]
        go(s.at[TWO], t.at[:, mine], 3, core)

    def five():
        copies.pop().wait()

    return one, two, three, four, five


def last_program(s):
    r = s.r
    s.prologue()
    loads = s.norm_load(A)
    s.clear()
    layers = range(s.c.layers)
    r.ev[...] = jnp.zeros(r.ev.shape, F32)
    for l in layers:
        at = PER * l
        if l:
            r.ev[at : at + TWO, :] = getattr(r, f"row_a{l}")[:TWO, :]
        r.ev[at + TWO : at + PER, :] = getattr(r, f"row_b{l}")[: PER - TWO, :]
    early = sum_steps(r.ev, r.ea, r.et, r.es, r.eb, r.esend, r.erecv)
    late = sum_steps(r.lv, r.la, r.lt, r.ls, r.lb, r.lsend, r.lrecv)
    for i in range(len(PAIRS)):
        s.step(i)
        early[i]()
    s.merge(A, OWN)
    s.third_sends(A)
    second_half(s, loads)
    early[-1]()
    loads = s.norm_load(B)
    s.fill_next()
    s.third_sends(B)
    s.fill(ALL)
    s.rs_done(B)
    s.norm_half(B, loads)
    r.lv[...] = jnp.zeros(r.lv.shape, F32)
    for j in range(TWO):
        r.lv[pl.ds(j, 1), :] = jnp.sum(r.acc[j], axis=0, keepdims=True)
    for x in late:
        x()
    for l in layers:
        r.row_o[l] = r.et[PER * l : PER * (l + 1), :]
    r.row_o[0, :TWO, :] = r.lt[:TWO, :]
    s.end()


def to_forward(s, next_loads=None):
    loads = s.norm_load(B)
    s.fill_next()
    s.third_sends(B)
    s.own_sends(A)
    s.fill_next()
    s.product(A, OWN)
    s.flip_all()
    s.fill_next()
    s.rs_done(B)
    s.norm_half(B, loads)
    if next_loads:
        next_loads()
    s.fill_next()
    s.forward(A)
    s.own_sends(B)
    s.fill_next()
    s.product(B, OWN)
    s.flip_all()
    s.fill_next()
    products(s, A)
    s.fill_next()
    s.product(A, FAR)
    s.flip_all()
    s.forward(B)


def to_end(s):
    s.fill_next()
    products(s, B)
    s.fill(ALL)
    s.flip_all()
    s.product(B, FAR)
    s.flip_all()
    s.end()


def mid_program(s, z=None):
    s.prologue()
    loads = s.norm_load(A)
    s.clear()
    both_halves(s, loads)
    if z is None:
        to_forward(s)
        to_end(s)
        return

    def next_loads():
        z.w1_load()
        z.w2_load()

    to_forward(s, next_loads)
    s.res_done()
    s.rows_out()
    s.rs_sent()
    z.lhs_load(0)
    z.lhs_load(1)
    loads = z.norm_load(A)
    z.step(0)
    z.step(1)
    s.cross(B)
    z.step(TWO)
    z.step(3)
    s.ready(B, XN)
    s.ready(B, YN)
    z.merge(A, OWN)
    s.cross_far(B)
    s.product(B, XN)
    s.product(B, YN)
    s.flip_all()
    s.product(B, FAR)
    z.third_sends(A)
    s.flip_all()
    s.res_done()
    z.lhs_late()
    for i in range(len(PAIRS), len(z.seq)):
        z.step(i)
    z.merge(B, OWN)
    z.rs_done(A)
    s.end()
    z.norm_half(A, loads)
    to_forward(z)
    to_end(z)


def top_program(s, z):
    s.prologue()
    loads = s.norm_load(A)
    z.clear()
    both_halves(s, loads)
    srcs = []

    def next_loads():
        z.w1_load()
        srcs.extend(z.begin(z.r.src.at[h], z.r.g.at[h], z.r.g_sem.at[h]) for h in HALVES)

    to_forward(s, next_loads)
    for x in srcs:
        x.wait()
    z.own_sends(A)
    s.res_done()
    s.rows_out()
    s.rs_sent()
    z.lhs_load(0)
    z.lhs_load(1)
    loads = z.norm_load(A)
    z.step(0, False)
    z.step(1, False)
    s.cross(B)
    z.step(TWO, False)
    z.step(3, False)
    s.ready(B, XN)
    s.ready(B, YN)
    z.merge(A, OWN)
    s.cross_far(B)
    s.product(B, XN)
    s.product(B, YN)
    s.flip_all()
    z.forward(A)
    s.product(B, FAR)
    s.flip_all()
    s.end()
    z.own_sends(B)
    z.lhs_late()
    z.product(A, OWN)
    z.ready(B, OWN)
    z.cross(A)
    z.product(B, OWN)
    z.ready(A, XN)
    z.ready(A, YN)
    z.product(A, XN)
    z.product(A, YN)
    z.forward(B)
    z.cross_far(A)
    for n in range(z.tiles1):
        z.far_sends(n)
    z.first_sends(A, XN)
    z.first_sends(A, YN)
    z.product_in(4)
    z.product(A, FAR)
    z.cross(B)
    z.step(5, False)
    z.ready(B, XN)
    z.ready(B, YN)
    z.product(B, XN)
    z.cross_far(B)
    z.product(B, YN)
    z.third_sends(A)
    z.first_sends(B, FAR)
    z.merge(B, XN)
    z.first_sends(B, XN)
    z.product_in(6)
    z.merge(B, YN)
    z.first_sends(B, YN)
    z.product_in(7)
    z.merge(B, OWN)
    z.rs_done(A)
    z.norm_half(A, loads)
    loads = z.norm_load(B)
    z.product(B, FAR)
    z.third_sends(B)
    z.rs_done(B)
    z.norm_half(B, loads)
    z.end()


PROGRAMS = (first_program, mid_program, top_program, last_program)


def positions(me):
    def pos(axis):
        i = lax.broadcasted_iota(jnp.int32, (ROWS, ROWS), axis)
        return lax.bitwise_xor(lax.div(i, GROUP), me) * GROUP + lax.rem(i, GROUP)

    return pos(0), pos(1)


def heads_of(x, part, h):
    at = part * INNER + h * HD
    return x[:, at : at + HD]


def softmax(s):
    e = jnp.exp(s - jnp.max(s, axis=-1, keepdims=True))
    return e * (ONE / jnp.sum(e, axis=-1, keepdims=True))


def attn_fwd_kernel(group, info, qkv, ctx, s_ref, p_ref):
    row, col = positions(info[ALL_SEQS])
    for first in range(0, SEQS, group):
        some = [(i, h) for i in range(first, first + group) for h in range(HEADS)]
        xs = {i: qkv[:, i].reshape(ROWS, QKV_N) for i, _ in some}
        for n, (i, h) in enumerate(some):
            mask = (col <= row) & (col < info[pl.program_id(0) * SEQS + i])
            score = dims(heads_of(xs[i], 0, h), heads_of(xs[i], 1, h), 1, 1) * HD**-HALF
            s_ref[n] = jnp.where(mask, score, NEG)
        p_ref[...] = softmax(s_ref[...]).astype(BF)
        out = {i: [] for i in xs}
        for n, (i, h) in enumerate(some):
            out[i].append(dims(p_ref[n], heads_of(xs[i], TWO, h), 1, 0).astype(BF))
        for i, parts in out.items():
            ctx[:, i] = jnp.concatenate(parts, axis=-1).reshape(PEERS, GROUP, INNER)


def attn_bwd_steps(group, info, qkv, dctx, out, s_ref, dp_ref, p_ref, ds_ref):
    row, col = positions(info[ALL_SEQS])
    for first in range(0, SEQS, group):
        some = [(i, h) for i in range(first, first + group) for h in range(HEADS)]
        xs = {i: (qkv[:, i].reshape(ROWS, QKV_N), dctx[:, i].reshape(ROWS, INNER)) for i, _ in some}
        for n, (i, h) in enumerate(some):
            x, d = xs[i]
            mask = (col <= row) & (col < info[pl.program_id(0) * SEQS + i])
            score = dims(heads_of(x, 0, h), heads_of(x, 1, h), 1, 1) * HD**-HALF
            s_ref[n] = jnp.where(mask, score, NEG)
            dp_ref[n] = dims(heads_of(d, 0, h), heads_of(x, TWO, h), 1, 1).astype(BF)
        p = softmax(s_ref[...])
        dp = dp_ref[...].astype(F32)
        p_ref[...] = p.astype(BF)
        ds = p * (dp - jnp.sum(dp * p, axis=-1, keepdims=True))
        ds_ref[...] = (ds * HD**-HALF).astype(BF)
        grads = {i: ([], [], []) for i in xs}
        for n, (i, h) in enumerate(some):
            x, d = xs[i]
            dq, dk, dv = grads[i]
            dq.append(dims(ds_ref[n], heads_of(x, 1, h), 1, 0).astype(BF))
            dk.append(dims(ds_ref[n], heads_of(x, 0, h), 0, 0).astype(BF))
            dv.append(dims(p_ref[n], heads_of(d, 0, h), 0, 0).astype(BF))
        for i, parts in grads.items():
            out[:, i] = jnp.concatenate(sum(parts, []), axis=-1).reshape(PEERS, GROUP, QKV_N)


def seq_spec(n):
    per_half = PEERS // SEQS
    return pl.BlockSpec((None, PEERS, SEQS, GROUP, n), lambda i, info: (lax.div(i, per_half), 0, lax.rem(i, per_half), 0, 0))


def by_seq(a):
    return a.reshape(TWO, PEERS, PEERS, GROUP, a.shape[-1])


def seq_shape(n):
    return jax.ShapeDtypeStruct((TWO, PEERS, PEERS, GROUP, n), BF)


def attn_tiles(group, *types):
    return [pltpu.VMEM((group * HEADS, ROWS, ROWS), t) for t in types]


def attn_fwd(info, qkv, group):
    grid_spec = pltpu.PrefetchScalarGridSpec(
        num_scalar_prefetch=1, grid=(ALL_SEQS // SEQS,), in_specs=[seq_spec(QKV_N)], out_specs=seq_spec(INNER), scratch_shapes=attn_tiles(group, F32, BF)
    )
    out = pl.pallas_call(partial(attn_fwd_kernel, group), name="attn_fwd", out_shape=seq_shape(INNER), grid_spec=grid_spec)(info, by_seq(qkv))
    return out.reshape(TWO, PEERS, ROWS, INNER)


def stacking(puts, stacks):
    used = sorted({p[1] for p in puts})
    first = [next(p for p in puts if p[1] == k) for k in used]
    shapes = [jax.ShapeDtypeStruct((p[3],) + p[0].shape, p[0].dtype) for p in first]
    given = [k for k in used if stacks[k] is not None]
    dma = pltpu.SemaphoreType.DMA
    scratch = [pltpu.VMEM(p[0].shape, p[0].dtype) for p in puts] + [dma((len(puts),)), dma((len(puts),))]
    return used, shapes, given, scratch


def attn_bwd(info, qkv, dctx, puts, stacks, group):
    used, shapes, given, scratch = stacking(puts, stacks)
    m = len(puts)

    def kernel(info, qkv, dctx, *refs):
        grads, refs = refs[:m], refs[m + len(given) :]
        out, outs, refs = refs[0], refs[1 : 1 + len(used)], refs[1 + len(used) :]
        bounce, load_sem, put_sem, tiles = refs[:m], refs[m], refs[m + 1], refs[m + TWO :]
        step = pl.program_id(0)

        def load(i):
            return Pieces(grads[i], bounce[i], load_sem.at[i], PEERS)

        def put(i):
            return Pieces(bounce[i], outs[used.index(puts[i][1])].at[puts[i][TWO]], put_sem.at[i], PEERS)

        @pl.when(step == 0)
        def _():
            for i in range(m):
                load(i).start()

        for at, some in ((1, range(m // TWO)), (TWO, range(m // TWO, m))):

            @pl.when(step == at)
            def _(some=some):
                for i in some:
                    load(i).wait()
                    put(i).start()

        attn_bwd_steps(group, info, qkv, dctx, out, *tiles)

        @pl.when(step == ALL_SEQS // SEQS - 1)
        def _():
            for i in range(m):
                put(i).wait()

    hbm = pl.BlockSpec(memory_space=ANY)
    grid_spec = pltpu.PrefetchScalarGridSpec(
        num_scalar_prefetch=1,
        grid=(ALL_SEQS // SEQS,),
        in_specs=[seq_spec(QKV_N), seq_spec(INNER)] + [hbm] * (m + len(given)),
        out_specs=[seq_spec(QKV_N)] + [hbm] * len(used),
        scratch_shapes=scratch + attn_tiles(group, F32, BF, BF, BF),
    )
    res = pl.pallas_call(
        kernel,
        name="attn_bwd",
        out_shape=[seq_shape(QKV_N)] + shapes,
        grid_spec=grid_spec,
        input_output_aliases={3 + m + j: 1 + used.index(k) for j, k in enumerate(given)},
        compiler_params=pltpu.CompilerParams(vmem_limit_bytes=VMEM_LIMIT),
    )(info, by_seq(qkv), by_seq(dctx), *[p[0] for p in puts], *[stacks[k] for k in given])
    for k, a in zip(used, res[1:]):
        stacks[k] = a
    return res[0].reshape(TWO, PEERS, ROWS, QKV_N)


def put_last(puts, stacks, lhs, rhs, k, layer):
    used, shapes, given, scratch = stacking(puts, stacks)
    m, n, wide = len(puts), lhs.shape[-1], rhs.shape[-1]
    skip = m + TWO + len(given)
    tiles, ahead = wide // BN, 3

    def kernel(*refs):
        grads, lhs_ref, rhs_ref, refs = refs[:m], refs[m], refs[m + 1], refs[skip + 1 :]
        outs, goal, refs = refs[: len(used)], refs[len(used)], refs[len(used) + 1 :]
        bounce, load_sem, put_sem, refs = refs[:m], refs[m], refs[m + 1], refs[m + TWO :]
        f_lhs, f_at, f_rhs, f_out, l_sem, r_sem, o_sem = refs

        def right(t):
            return Pieces(rhs_ref.at[:, pl.ds(t * BN, BN)], f_rhs.at[t % ahead], r_sem.at[t % ahead], PEERS)

        def store(t):
            return Pieces(f_out.at[t % TWO], goal.at[layer, :, pl.ds(t * BN, BN)], o_sem.at[t % TWO], ahead)

        left = Pieces(lhs_ref, f_lhs, l_sem, PEERS).start()
        for t in range(ahead - 1):
            right(t).start()
        loads = [Pieces(grads[i], bounce[i], load_sem.at[i], PEERS).start() for i in range(m)]
        stores = []
        left.wait()
        for i in range(TOK // KT):
            f_at[:, i * KT : (i + 1) * KT] = f_lhs[i * KT : (i + 1) * KT, :].T
        for t in range(tiles):
            right(t).wait()
            if t + ahead - 1 < tiles:
                right(t + ahead - 1).start()
            if t >= TWO:
                store(t - TWO).wait()
            f_out[t % TWO] = dims(f_at[...], f_rhs[t % ahead], 1, 0).astype(BF)
            store(t).start()
            if t < m:
                loads[t].wait()
                stores.append(Pieces(bounce[t], outs[used.index(puts[t][1])].at[puts[t][TWO]], put_sem.at[t], PEERS).start())
        for t in range(tiles - TWO, tiles):
            store(t).wait()
        for c in stores:
            c.wait()

    hbm = pl.BlockSpec(memory_space=ANY)
    dma = pltpu.SemaphoreType.DMA
    old = stacks[k]
    aliases = {m + TWO + j: used.index(g) for j, g in enumerate(given)}
    *res, stacks[k] = pl.pallas_call(
        kernel,
        name="put_last",
        out_shape=shapes + [jax.ShapeDtypeStruct(old.shape, old.dtype)],
        in_specs=[hbm] * (skip + 1),
        out_specs=[hbm] * (len(used) + 1),
        scratch_shapes=scratch
        + [pltpu.VMEM(x, BF) for x in ((TOK, n), (n, TOK), (ahead, TOK, BN), (TWO, n, BN))]
        + [dma, dma((ahead,)), dma((TWO,))],
        input_output_aliases={**aliases, skip: len(used)},
        compiler_params=pltpu.CompilerParams(vmem_limit_bytes=VMEM_LIMIT),
    )(*[p[0] for p in puts], lhs, rhs, *[stacks[g] for g in given], old)
    for g, a in zip(used, res):
        stacks[g] = a


def group_body(x_loc, dy_loc, len_loc, wqkv, wout, wup, bup, wdown, vec):
    n = wqkv.shape[0]
    ids = iter(range(ROWS))
    shape = x_loc.shape
    x = x_loc.reshape(TWO, ROWS, D)
    dy = dy_loc.reshape(TWO, ROWS, D)
    wq = jnp.transpose(wqkv, (0, 2, 3, 4, 1)).reshape(n, QKV_N, D)
    wo = wout.reshape(n, INNER, D)
    info = jnp.concatenate([len_loc, lax.axis_index(TP).reshape(1).astype(jnp.int32)])

    def flat(a):
        return a.reshape(TOK, a.shape[-1])

    def row(layer, i, bias=None):
        return SimpleNamespace(gain=(layer, i), shift=(layer, i + 1), bias=bias)

    ln2, bias1, bias2 = TWO, 4, 5
    saved = [SimpleNamespace() for _ in range(n)]
    (r,) = fused("first", next(ids), FIRST, config(N_FIRST, dict(in0=x, wb=wq, vec=vec), row(0, 0), ag=(QKV, 0)))
    s = saved[0]
    s.x, s.a, s.qkv = x, r.full, r.res
    for l in range(n):
        s = saved[l]
        s.ctx = attn_fwd(info, s.qkv, SEQS)
        arrays = dict(lhs1=s.ctx, wa=wo, wb=wup, in0=s.x, vec=vec, b_up=bup)
        stages = [config(N_LN, arrays, row(l, ln2, (l, bias1)), rs=(l, INNER, False), ag=(UP, l))]
        kind, taken = MID, (("lhs1", "res"), ("in0", "out0"))
        arrays = dict(wa=wdown, vec=vec)
        if l + 1 < n:
            arrays.update(wb=wq)
            stages.append(config(N_LN, arrays, row(l + 1, 0, (l, bias2)), rs=(l, FF, False), ag=(QKV, l + 1), taken=taken))
        else:
            kind = TOP
            arrays.update(src=dy)
            stages.append(config(N_RES, arrays, row(0, 0, (l, bias2)), rs=(l, FF, False), ag=(DACT, l), taken=taken + (("slope", "slope"),)))
        r, z = fused(f"fwd_{l}", next(ids), kind, *stages)
        s.hid, s.act, s.slope, s.m_t, s.act_t = r.out0, r.res, r.slope, r.full_t, r.res_t
        if l + 1 < n:
            s = saved[l + 1]
            s.x, s.a, s.qkv = z.out0, z.full, z.res
    y, d_cur, d_full, d_pre = z.out0, z.out1, z.full, z.res
    g_bup, rows, puts, stacks = [z.bup], [], [(y.reshape(KT, D), 4, 0, 1)], [None] * 6
    mlp_plan = (3, 1, 0, 7, 1, 0, TWO, 0, TWO, TWO, 3, 0, TWO)
    attn_plan = (3, TWO, 0, 7, TWO, 0, 1, 1, 1, 1, 3, 1, 1)
    for l in reversed(range(n)):
        s = saved[l]
        arrays = dict(lhs1=d_pre, wa=wup, wb=wo, in0=s.hid, in1=d_cur, vec=vec, f0l=s.act_t, f0r=flat(d_full), f1l=s.m_t, f1r=flat(d_pre))
        common = dict(fills=((FF, D, TWO), (D, FF, 1)), bm=BM + BM, flat_t=True, plan=mlp_plan)
        (r,) = fused(f"d_mlp_{l}", next(ids), MID, config(N_BWD2, arrays, row(l, ln2), rs=(l, FF, True), ag=(DCTX, l), **common))
        d_hid, d_attn, v3 = r.out0, r.full, r.vo
        puts += [(r.g0, 3, l, n), (r.g1, TWO, l, n)]
        d_qkv = attn_bwd(info, s.qkv, r.res, puts, stacks, TWO if l else 1)
        arrays = dict(lhs1=d_qkv, wa=wq, in0=s.x, in1=d_hid, vec=vec, f0l=flat(d_qkv), f0r=flat(s.a))
        fills = ((QKV_N, D, 3), (INNER, D, 1))
        common = dict(rs=(l, QKV_N, False), fills=fills if l else fills[:1], plan=attn_plan if l else (6, 4))
        if l:
            arrays.update(f1l=flat(s.ctx), f1r=flat(d_attn))
            arrays.update(wb=wdown, slope=saved[l - 1].slope)
            common.update(ag=(DACT, l - 1))
        else:
            arrays.update({f"row_a{i}": rows[n - 1 - i][0] for i in range(1, n)}, row_b0=v3, **{f"row_b{i}": rows[n - 1 - i][1] for i in range(1, n)})
            common.update(layers=n)
        (r,) = fused(f"d_attn_{l}", next(ids), MID if l else LAST, config(N_BWD1, arrays, row(l, 0), **common))
        if l:
            g_bup.append(r.bup)
            d_full, d_pre = r.full, r.res
        puts = [(r.g0, 0, l, n)] + ([(r.g1, 1, l, n)] if l else [])
        rows.append((r.vo, v3))
        d_cur = r.out0
    put_last(puts + [(d_cur.reshape(KT, D), 5, 0, 1)], stacks, flat(s.ctx), flat(d_attn), 1, 0)
    g_qkv = jnp.transpose(stacks[0].reshape(n, 3, HEADS, HD, D), (0, 4, 1, 2, 3))
    g_out = stacks[1].reshape(n, HEADS, HD, D)
    return stacks[4].reshape(shape), stacks[5].reshape(shape), g_qkv, g_out, stacks[2], jnp.concatenate(g_bup[::-1]), stacks[3], r.row_o


def solution(mesh):
    act_spec = P(DP, TP, None)
    in_specs = (act_spec, act_spec, P(DP), P(None, None, None, TP, None), P(None, TP, None, None), P(None, None, TP), P(None, TP), P(None, TP, None), P())
    out_specs = (act_spec, act_spec, P(DP, None, None, TP, None), P(DP, TP, None, None), P(DP, None, TP), P(DP, TP), P(DP, TP, None), P(DP, None, None))
    return jax.shard_map(group_body, mesh=mesh, in_specs=in_specs, out_specs=out_specs, check_vma=False)
```
